32 devices in a mesh: shard: 2 (over core), ctx: 4 (over y, x), tp: 4 (over z).
Axes of the slice: x: 2, y: 2, z: 4, core: 2. Of those that a mesh axis runs over, the one named last changes fastest.
Arguments:
- layer_input: bfloat16 [8, 1024, 2048], P('shard', 'ctx'), may hold values from -6 to 6
- output_gradient: bfloat16 [8, 1024, 2048], P('shard', 'ctx'), may hold values from -6 to 6
- picture_piece_starts: int32 [8, 2], P('shard'), may hold values from 0 to 768, as said below
- sequence_adapter_index: int32 [8], P('shard'), may hold values from 0 to 7
- attention_norm_gain: float32 [2048], replicated, may hold values from 0.5 to 1.5
- attention_norm_bias: float32 [2048], replicated, may hold values from -1 to 1
- feedforward_norm_gain: float32 [2048], replicated, may hold values from 0.5 to 1.5
- feedforward_norm_bias: float32 [2048], replicated, may hold values from -1 to 1
- query_key_value_weight: bfloat16 [2048, 3, 2048], P('shard', None, 'tp'), may hold values from -0.125 to 0.125
- attention_output_weight: bfloat16 [2048, 2048], P('tp', 'shard'), may hold values from -0.375 to 0.375
- up_projection_weight: bfloat16 [2048, 8192], P('shard', 'tp'), may hold values from -0.125 to 0.125
- down_projection_weight: bfloat16 [8192, 2048], P('tp', 'shard'), may hold values from -0.09375 to 0.09375
- adapter_projection_first: bfloat16 [8, 2048, 16], replicated, may hold values from -0.125 to 0.125
- adapter_projection_second: bfloat16 [8, 16, 3, 2048], P(None, None, None, 'tp'), may hold values from -0.75 to 0.75
- adapter_heads_first: bfloat16 [8, 2048, 16], P(None, 'tp'), may hold values from -0.375 to 0.375
- adapter_heads_second: bfloat16 [8, 16, 2048], replicated, may hold values from -0.75 to 0.75
- adapter_up_first: bfloat16 [8, 2048, 16], replicated, may hold values from -0.125 to 0.125
- adapter_up_second: bfloat16 [8, 16, 8192], P(None, None, 'tp'), may hold values from -0.75 to 0.75
- adapter_down_first: bfloat16 [8, 8192, 16], P(None, 'tp'), may hold values from -0.09375 to 0.09375
- adapter_down_second: bfloat16 [8, 16, 2048], replicated, may hold values from -0.75 to 0.75
Outputs:
- layer_out: bfloat16 [8, 1024, 2048], P('shard', 'ctx')
- input_grad: bfloat16 [8, 1024, 2048], P('shard', 'ctx')
- qkv_in_grad: float32 [8, 2048, 16], replicated
- qkv_out_grad: float32 [8, 16, 3, 2048], P(None, None, None, 'tp')
- heads_in_grad: float32 [8, 2048, 16], P(None, 'tp')
- heads_out_grad: float32 [8, 16, 2048], replicated
- up_in_grad: float32 [8, 2048, 16], replicated
- up_out_grad: float32 [8, 16, 8192], P(None, None, 'tp')
- down_in_grad: float32 [8, 8192, 16], P(None, 'tp')
- down_out_grad: float32 [8, 16, 2048], replicated
The draws below stay inside these ranges and needn't reach their ends.
Inputs may be any that keep to these rules, and one draw needn't show every extreme that they name: `picture_piece_starts`: piece c of a sequence starts within positions c * 512 to (c + 1) * 512 - 256, so pieces never meet; in some sequence a piece starts at 0, in some sequence a piece ends at 1024.
All inputs are finite; a program needn't handle non-finite values.
Results may differ from the reference program's by a relative error of at most 0.019.
Values may be sent and summed in bfloat16 or wider, within the bound.
A program may use at most 320 MiB of HBM per device.

```python
import jax
import jax.numpy as jnp
from jax import lax

MODEL_DIM = 2048
H = 16
HD = 128
HIDDEN_UNITS = 8192
ADAPTER_COUNT = 8
ADAPTER_RANK = 16
PIC = 256
PICS = 2
LEN = 1024
SEQS = 8


def draw_picture_piece_starts(key, part):
    span = LEN // PICS - PIC + 1
    first_key, second_key, third_key = jax.random.split(key, 3)
    offsets = jax.random.randint(first_key, (SEQS, PICS), 0, span)
    low_row = jax.random.randint(second_key, (), 0, SEQS)
    high_row = jax.random.randint(third_key, (), 0, SEQS)
    seq_ids = jnp.arange(SEQS, dtype=jnp.int32)[:, None]
    piece_ids = jnp.arange(PICS, dtype=jnp.int32)[None, :]
    offsets = jnp.where((seq_ids == low_row) & (piece_ids == 0), 0, offsets)
    offsets = jnp.where((seq_ids == high_row) & (piece_ids == PICS - 1), span - 1, offsets)
    return (piece_ids * (LEN // PICS) + offsets).astype(jnp.int32)


def plant(values, rng, least, top_value):
    longest = values.shape.index(max(values.shape))
    spots = []
    for shift in (0, 1):
        where = [jax.random.randint(jax.random.fold_in(rng, axis), (), 0, length) for axis, length in enumerate(values.shape)]
        where[longest] = (where[longest] + shift) % values.shape[longest]
        spots.append(tuple(where))
    return values.at[spots[0]].set(least).at[spots[1]].set(top_value)


def levels(key, dims, cuts, least, top_value):
    gain = 1.0
    for dim, blocks in cuts:
        steps = jax.random.uniform(jax.random.fold_in(jax.random.fold_in(key, 6), dim), (blocks,), jnp.float32, least / len(cuts), top_value / len(cuts))
        gain = gain * jnp.repeat(jnp.exp(steps), dims[dim] // blocks).reshape((-1,) + (1,) * (len(dims) - 1 - dim))
    return gain


def normal_values(rng, shape, scale, bound, pieces=(), held_as=jnp.bfloat16):
    values = scale * jax.random.normal(rng, shape, jnp.float32)
    if pieces:
        values = values * levels(rng, shape, pieces, -0.22, 0.18)
    return jnp.clip(values, -bound, bound).astype(held_as)


def setup_inputs(seed: int = 0) -> dict:
    key_list = jax.random.split(jax.random.key(seed), 21)
    return {
        "layer_input": normal_values(key_list[0], (SEQS, LEN, MODEL_DIM), 1.0, 6.0, ((0, 2), (1, 4))),
        "output_gradient": normal_values(key_list[1], (SEQS, LEN, MODEL_DIM), 1.0, 6.0, ((0, 2), (1, 4))),
        "picture_piece_starts": draw_picture_piece_starts(jax.random.fold_in(key_list[20], 71), 0),
        "sequence_adapter_index": plant(jax.random.randint(key_list[3], (SEQS,), 0, ADAPTER_COUNT), jax.random.fold_in(key_list[3], 1), 0, ADAPTER_COUNT - 1).astype(jnp.int32),
        "attention_norm_gain": jnp.clip(1.0 + 0.1 * jax.random.normal(key_list[4], (MODEL_DIM,), jnp.float32), 0.5, 1.5),
        "attention_norm_bias": normal_values(key_list[5], (MODEL_DIM,), 0.2, 1.0, (), jnp.float32),
        "feedforward_norm_gain": jnp.clip(1.0 + 0.1 * jax.random.normal(key_list[6], (MODEL_DIM,), jnp.float32), 0.5, 1.5),
        "feedforward_norm_bias": normal_values(key_list[7], (MODEL_DIM,), 0.2, 1.0, (), jnp.float32),
        "query_key_value_weight": normal_values(key_list[8], (MODEL_DIM, 3, MODEL_DIM), MODEL_DIM ** -0.5, 0.125, ((0, 2), (2, 4))),
        "attention_output_weight": normal_values(key_list[9], (MODEL_DIM, MODEL_DIM), (MODEL_DIM // 8) ** -0.5, 0.375, ((0, 4), (1, 2))),
        "up_projection_weight": normal_values(key_list[10], (MODEL_DIM, HIDDEN_UNITS), MODEL_DIM ** -0.5, 0.125, ((0, 2), (1, 4))),
        "down_projection_weight": normal_values(key_list[11], (HIDDEN_UNITS, MODEL_DIM), (HIDDEN_UNITS // 2) ** -0.5, 0.09375, ((0, 4), (1, 2))),
        "adapter_projection_first": normal_values(key_list[12], (ADAPTER_COUNT, MODEL_DIM, ADAPTER_RANK), MODEL_DIM ** -0.5, 0.125),
        "adapter_projection_second": normal_values(key_list[13], (ADAPTER_COUNT, ADAPTER_RANK, 3, MODEL_DIM), (4 * ADAPTER_RANK) ** -0.5, 0.75, ((3, 4),)),
        "adapter_heads_first": normal_values(key_list[14], (ADAPTER_COUNT, MODEL_DIM, ADAPTER_RANK), (MODEL_DIM // 8) ** -0.5, 0.375, ((1, 4),)),
        "adapter_heads_second": normal_values(key_list[15], (ADAPTER_COUNT, ADAPTER_RANK, MODEL_DIM), (4 * ADAPTER_RANK) ** -0.5, 0.75),
        "adapter_up_first": normal_values(key_list[16], (ADAPTER_COUNT, MODEL_DIM, ADAPTER_RANK), MODEL_DIM ** -0.5, 0.125),
        "adapter_up_second": normal_values(key_list[17], (ADAPTER_COUNT, ADAPTER_RANK, HIDDEN_UNITS), (4 * ADAPTER_RANK) ** -0.5, 0.75, ((2, 4),)),
        "adapter_down_first": normal_values(key_list[18], (ADAPTER_COUNT, HIDDEN_UNITS, ADAPTER_RANK), (HIDDEN_UNITS // 2) ** -0.5, 0.09375, ((1, 4),)),
        "adapter_down_second": normal_values(key_list[19], (ADAPTER_COUNT, ADAPTER_RANK, MODEL_DIM), (4 * ADAPTER_RANK) ** -0.5, 0.75),
    }


NORM_EPS = 1e-05
HIGH = lax.Precision.HIGHEST

@jax.custom_vjp
def low(v):
    return lax.optimization_barrier(v.astype(jnp.bfloat16)).astype(jnp.float32)

@jax.custom_vjp
def low_back(v):
    return v

def low_keep(v):
    return (low(v), None)

def low_pass(kept, grad):
    return (grad,)

def back_keep(v):
    return (v, None)

def back_low(kept, grad):
    return (low(grad),)
low.defvjp(low_keep, low_pass)
low_back.defvjp(back_keep, back_low)

def matmul(left_mat, right_mat):
    return jnp.dot(left_mat, right_mat, precision=HIGH, preferred_element_type=jnp.float32)

def layer_norm(inputs, gains, biases):
    average = lax.optimization_barrier(jnp.mean(inputs, axis=-1, keepdims=True))
    centred = inputs - average
    spread = lax.optimization_barrier(jnp.mean(centred * centred, axis=-1, keepdims=True))
    return centred * lax.rsqrt(spread + NORM_EPS) * gains + biases

def gelu_tanh(inputs):
    return 0.5 * inputs * (1.0 + jnp.tanh(0.7978845608028654 * (inputs + 0.044715 * inputs * inputs * inputs)))

def flattened_first(adapter_mat):
    adapter_tables, inner_dim, rank_width = adapter_mat.shape
    return jnp.transpose(adapter_mat, (1, 0, 2)).reshape(inner_dim, adapter_tables * rank_width)

def flattened_second(adapter_mat):
    return adapter_mat.reshape(adapter_mat.shape[0] * adapter_mat.shape[1], -1)

def piece_labels(starts, positions):
    inside = (positions[None, :] >= starts[:, None]) & (positions[None, :] < starts[:, None] + PIC)
    labels = jnp.arange(1, PICS + 1, dtype=jnp.int32)
    return lax.optimization_barrier(jnp.sum(jnp.where(inside, labels[:, None], 0), axis=0)).astype(jnp.int32)

def attention(queries, key_rows, value_rows, starts):
    positions = jnp.arange(LEN, dtype=jnp.int32)
    labels_all = piece_labels(starts, positions)
    slopes = jnp.exp2(-8.0 * (jnp.arange(H, dtype=jnp.float32) + 1.0) / H)
    block_len = min(512, LEN)
    block_count = LEN // block_len

    def one_block(element):
        query_block, offset = element
        query_pos = offset + jnp.arange(block_len, dtype=jnp.int32)
        query_labels = lax.dynamic_slice_in_dim(labels_all, offset, block_len)
        logits = jnp.einsum('qhd,khd->hqk', query_block, key_rows, precision=HIGH) * HD ** (-0.5)
        distance = jnp.abs(query_pos[:, None] - positions[None, :]).astype(jnp.float32)
        logits = low_back(logits - slopes[:, None, None] * distance[None])
        visible_mask = (positions[None, :] <= query_pos[:, None]) | (query_labels[:, None] == labels_all[None, :]) & (query_labels[:, None] > 0)
        exponent = jnp.where(visible_mask[None], jnp.exp(logits), 0.0)
        totals = lax.optimization_barrier(jnp.sum(exponent, axis=-1))
        weighted = low_back(jnp.einsum('hqk,khd->qhd', low(exponent), value_rows, precision=HIGH))
        return weighted / jnp.transpose(totals)[:, :, None]
    offsets = jnp.arange(block_count, dtype=jnp.int32) * block_len
    blocks_out = lax.map(jax.checkpoint(one_block), (queries.reshape(block_count, block_len, H, HD), offsets))
    return blocks_out.reshape(LEN, H * HD)

def layer_pass(tokens, adapter_matrices, frozen, starts, adapter_id):
    qkv_in, qkv_out, heads_in, heads_out, up_in, up_out, down_in, down_out = adapter_matrices
    gain_one, bias_one, gain_two, bias_two, qkv_full, heads_full, up_full, down_full = frozen
    columns = jnp.arange(ADAPTER_COUNT * ADAPTER_RANK, dtype=jnp.int32) // ADAPTER_RANK
    select = (columns == adapter_id).astype(jnp.float32)[None, :]
    first_act = low(layer_norm(tokens, gain_one, bias_one))
    first_low = low(low_back(matmul(first_act, flattened_first(qkv_in)) * select))
    projected = low(low_back(matmul(first_act, qkv_full) + matmul(first_low, flattened_second(qkv_out))))
    queries = projected[:, :MODEL_DIM].reshape(LEN, H, HD)
    key_rows = projected[:, MODEL_DIM:2 * MODEL_DIM].reshape(LEN, H, HD)
    value_rows = projected[:, 2 * MODEL_DIM:].reshape(LEN, H, HD)
    heads_raw = attention(queries, key_rows, value_rows, starts)
    heads_act = low(low_back(heads_raw))
    heads_low = low(low_back(matmul(heads_act, flattened_first(heads_in)) * select))
    middle = tokens + low_back(matmul(heads_act, heads_full) + matmul(heads_low, flattened_second(heads_out)))
    second_act = low(layer_norm(middle, gain_two, bias_two))
    up_low = low(low_back(matmul(second_act, flattened_first(up_in)) * select))
    hidden = low_back(matmul(second_act, up_full) + matmul(up_low, flattened_second(up_out)))
    activated = low(gelu_tanh(hidden))
    down_low = low(low_back(matmul(activated, flattened_first(down_in)) * select))
    return middle + low_back(matmul(activated, down_full) + matmul(down_low, flattened_second(down_out)))

def reference(layer_input, output_gradient, picture_piece_starts, sequence_adapter_index, attention_norm_gain, attention_norm_bias, feedforward_norm_gain, feedforward_norm_bias, query_key_value_weight, attention_output_weight, up_projection_weight, down_projection_weight, adapter_projection_first, adapter_projection_second, adapter_heads_first, adapter_heads_second, adapter_up_first, adapter_up_second, adapter_down_first, adapter_down_second):
    frozen = (attention_norm_gain.astype(jnp.float32), attention_norm_bias.astype(jnp.float32), feedforward_norm_gain.astype(jnp.float32), feedforward_norm_bias.astype(jnp.float32), query_key_value_weight.astype(jnp.float32).reshape(MODEL_DIM, 3 * MODEL_DIM), attention_output_weight.astype(jnp.float32), up_projection_weight.astype(jnp.float32), down_projection_weight.astype(jnp.float32))
    adapter_matrices = (adapter_projection_first.astype(jnp.float32), adapter_projection_second.astype(jnp.float32), adapter_heads_first.astype(jnp.float32), adapter_heads_second.astype(jnp.float32), adapter_up_first.astype(jnp.float32), adapter_up_second.astype(jnp.float32), adapter_down_first.astype(jnp.float32), adapter_down_second.astype(jnp.float32))

    def per_sequence(grad_sums, element):
        tokens, grads_back, starts, adapter_id = element

        def forward(token_rows, mats):
            return layer_pass(token_rows, mats, frozen, starts, adapter_id)
        result, pullback = jax.vjp(forward, tokens.astype(jnp.float32), adapter_matrices)
        grad_tokens, grad_mats = pullback(grads_back.astype(jnp.float32))
        grad_sums = jax.tree.map(lambda first, second: first + second, grad_sums, grad_mats)
        return (grad_sums, (result.astype(jnp.bfloat16), grad_tokens.astype(jnp.bfloat16)))
    zero_init = jax.tree.map(jnp.zeros_like, adapter_matrices)
    grad_sums, (layer_outs, input_grads) = lax.scan(per_sequence, zero_init, (layer_input, output_gradient, picture_piece_starts, sequence_adapter_index))
    return (layer_outs, input_grads, grad_sums[0], grad_sums[1], grad_sums[2], grad_sums[3], grad_sums[4], grad_sums[5], grad_sums[6], grad_sums[7])
```

```python
import jax
import jax.numpy as jnp
from jax import lax
from jax.sharding import PartitionSpec as P

HD = 128
PIC = 256


NORM_EPS = 1e-05


def layer_norm(inputs, gains, biases):
    average = jnp.mean(inputs, axis=-1, keepdims=True)
    centred = inputs - average
    spread = jnp.mean(centred * centred, axis=-1, keepdims=True)
    return centred * lax.rsqrt(spread + NORM_EPS) * gains + biases


def gelu_tanh(inputs):
    return (
        0.5
        * inputs
        * (1.0 + jnp.tanh(0.7978845608028654 * (inputs + 0.044715 * inputs * inputs * inputs)))
    )


def flattened_first(adapter_mat):
    adapter_tables, inner_dim, rank_width = adapter_mat.shape
    return jnp.transpose(adapter_mat, (1, 0, 2)).reshape(inner_dim, adapter_tables * rank_width)


def flattened_second(adapter_mat):
    return adapter_mat.reshape(adapter_mat.shape[0] * adapter_mat.shape[1], -1)


def unflat_in(grad_flat, adapter_tables):
    inner_dim = grad_flat.shape[0]
    return jnp.transpose(grad_flat.reshape(inner_dim, adapter_tables, -1), (1, 0, 2))


def matmul(left_mat, right_mat):
    return jnp.dot(left_mat, right_mat, preferred_element_type=jnp.float32)


def matmul_tn(left_mat, right_mat):
    return lax.dot_general(
        left_mat, right_mat, (((0,), (0,)), ((), ())), preferred_element_type=jnp.float32
    )


def matmul_nt(left_mat, right_mat):
    return lax.dot_general(
        left_mat, right_mat, (((1,), (1,)), ((), ())), preferred_element_type=jnp.float32
    )


def piece_labels(starts, positions):
    inside = (positions[None, None, :] >= starts[:, :, None]) & (
        positions[None, None, :] < starts[:, :, None] + PIC
    )
    labels = jnp.arange(1, starts.shape[1] + 1, dtype=jnp.int32)
    return jnp.sum(jnp.where(inside, labels[None, :, None], 0), axis=1)


def visible(query_pos, key_pos, query_labels, key_labels):
    causal = key_pos[None, None, :] <= query_pos[None, :, None]
    shared = (query_labels[:, :, None] == key_labels[:, None, :]) & (query_labels[:, :, None] > 0)
    return causal | shared


def exponents(queries, key_rows, query_pos, key_pos, visible_mask, slopes):
    score_scale = queries.shape[-1] ** (-0.5)
    logits = (
        jnp.einsum("sqhd,skhd->shqk", queries, key_rows, preferred_element_type=jnp.float32)
        * score_scale
    )
    distance = jnp.abs(query_pos[:, None] - key_pos[None, :]).astype(jnp.float32)
    logits = logits - slopes[None, :, None, None] * distance[None, None]
    return jnp.where(visible_mask[:, None], jnp.exp(logits), 0.0)


def block_grads(
    queries, scaled_grad, row_delta, key_rows, value_rows, query_pos, key_pos, visible_mask, slopes
):
    score_scale = queries.shape[-1] ** (-0.5)
    exponent = exponents(queries, key_rows, query_pos, key_pos, visible_mask, slopes)
    products_gv = jnp.einsum(
        "sqhd,skhd->shqk", scaled_grad, value_rows, preferred_element_type=jnp.float32
    )
    grad_logits = (
        exponent * (products_gv - jnp.transpose(row_delta, (0, 2, 1))[..., None])
    ).astype(jnp.bfloat16)
    grad_queries = (
        jnp.einsum("shqk,skhd->sqhd", grad_logits, key_rows, preferred_element_type=jnp.float32)
        * score_scale
    )
    grad_keyrows = (
        jnp.einsum("shqk,sqhd->skhd", grad_logits, queries, preferred_element_type=jnp.float32)
        * score_scale
    )
    grad_valrows = jnp.einsum(
        "shqk,sqhd->skhd",
        exponent.astype(jnp.bfloat16),
        scaled_grad,
        preferred_element_type=jnp.float32,
    )
    return (grad_queries, grad_keyrows, grad_valrows)


def tp_rows(rows_array, tp_count):
    chunk = rows_array.shape[0] // tp_count
    return lax.dynamic_slice_in_dim(rows_array, lax.axis_index("tp") * chunk, chunk, axis=0)


def scatter_rows(partials):
    widths = [part.shape[1] for part in partials]
    joined = lax.psum_scatter(
        jnp.concatenate(partials, axis=1), "tp", scatter_dimension=0, tiled=True
    )
    return split_columns(joined, widths)


def gather_rows(rows_here):
    widths = [part.shape[1] for part in rows_here]
    joined = lax.all_gather(jnp.concatenate(rows_here, axis=1), "tp", axis=0, tiled=True)
    return split_columns(joined, widths)


def split_columns(joined, widths):
    parts, offset = [], 0
    for width in widths:
        parts.append(joined[:, offset : offset + width])
        offset += width
    return tuple(parts)


def body(
    layer_input,
    output_gradient,
    picture_piece_starts,
    sequence_adapter_index,
    attention_norm_gain,
    attention_norm_bias,
    feedforward_norm_gain,
    feedforward_norm_bias,
    query_key_value_weight,
    attention_output_weight,
    up_projection_weight,
    down_projection_weight,
    adapter_projection_first,
    adapter_projection_second,
    adapter_heads_first,
    adapter_heads_second,
    adapter_up_first,
    adapter_up_second,
    adapter_down_first,
    adapter_down_second,
):
    seq_here, local_len, model_width = layer_input.shape
    tok_rows = seq_here * local_len
    tp_count = lax.axis_size("tp")
    adapter_tables = adapter_projection_first.shape[0]
    rank_width = adapter_projection_first.shape[2]
    head_width = HD
    device_heads = adapter_projection_second.shape[-1] // head_width
    local_width = device_heads * head_width
    columns = jnp.arange(adapter_tables * rank_width, dtype=jnp.int32) // rank_width
    chosen = (sequence_adapter_index[:, None] == columns[None, :]).astype(jnp.float32)
    select = jnp.broadcast_to(
        chosen[:, None, :], (seq_here, local_len, adapter_tables * rank_width)
    ).reshape(tok_rows, adapter_tables * rank_width)
    select_here = tp_rows(select, tp_count)
    head_ids = lax.axis_index("tp") * device_heads + jnp.arange(device_heads, dtype=jnp.int32)
    slopes = jnp.exp2(
        -8.0 * (head_ids.astype(jnp.float32) + 1.0) / (device_heads * tp_count)
    )
    here_pos = lax.axis_index("ctx") * local_len + jnp.arange(local_len, dtype=jnp.int32)
    here_labels = piece_labels(picture_piece_starts, here_pos)
    heads_full = lax.all_gather(
        lax.all_gather(attention_output_weight, "tp", axis=0, tiled=True),
        "shard",
        axis=1,
        tiled=True,
    )
    heads_first_all = lax.all_gather(adapter_heads_first, "tp", axis=1, tiled=True)
    projection_first_flattened = flattened_first(adapter_projection_first)
    projection_second_flattened = flattened_second(adapter_projection_second)
    heads_first_flattened = flattened_first(adapter_heads_first)
    heads_first_all_flattened = flattened_first(heads_first_all)
    heads_second_flattened = flattened_second(adapter_heads_second)
    up_first_flattened = flattened_first(adapter_up_first)
    up_second_flattened = flattened_second(adapter_up_second)
    down_first_flattened = flattened_first(adapter_down_first)
    down_second_flattened = flattened_second(adapter_down_second)
    residual = layer_input.reshape(tok_rows, model_width).astype(jnp.float32)
    residual_here = tp_rows(residual, tp_count)
    first_norm = layer_norm(residual, attention_norm_gain, attention_norm_bias)
    first_act = first_norm.astype(jnp.bfloat16)
    _, first_back_full = jax.vjp(
        lambda inputs: layer_norm(inputs, attention_norm_gain, attention_norm_bias), residual_here
    )
    gathered_rows = (
        lax.all_gather(query_key_value_weight, "shard", axis=0, tiled=True),
        lax.all_gather(up_projection_weight, "shard", axis=0, tiled=True),
    )
    qkv_full = gathered_rows[0].reshape(model_width, 3 * local_width)
    up_full = gathered_rows[1]
    down_full = lax.all_gather(down_projection_weight, "shard", axis=1, tiled=True)
    first_low = (matmul(first_act, projection_first_flattened) * select).astype(jnp.bfloat16)
    projected = (
        matmul(first_act, qkv_full) + matmul(first_low, projection_second_flattened)
    ).astype(jnp.bfloat16)
    queries_flat = projected[:, :local_width].reshape(seq_here, local_len, local_width)
    queries = queries_flat.reshape(seq_here, local_len, device_heads, head_width)
    key_rows = projected[:, local_width : 2 * local_width].reshape(seq_here, local_len, local_width)
    value_rows = projected[:, 2 * local_width :].reshape(seq_here, local_len, local_width)
    pieces = (
        lax.all_gather(key_rows, "ctx", axis=1, tiled=True),
        lax.all_gather(value_rows, "ctx", axis=1, tiled=True),
    )
    piece_len = pieces[0].shape[1]
    key_pos = jnp.arange(piece_len, dtype=jnp.int32)
    key_labels = piece_labels(picture_piece_starts, key_pos)
    visible_mask = visible(here_pos, key_pos, here_labels, key_labels)
    piece_keys = pieces[0].reshape(seq_here, piece_len, device_heads, head_width)
    piece_values = pieces[1].reshape(seq_here, piece_len, device_heads, head_width)
    exponent = exponents(queries, piece_keys, here_pos, key_pos, visible_mask, slopes)
    weighted = jnp.einsum(
        "shqk,skhd->sqhd",
        exponent.astype(jnp.bfloat16),
        piece_values,
        preferred_element_type=jnp.float32,
    )
    weighted, totals = (weighted, jnp.sum(exponent, axis=-1))
    per_total = jnp.transpose(totals, (0, 2, 1))[..., None]
    heads_raw = weighted / per_total
    heads_act = heads_raw.reshape(tok_rows, local_width).astype(jnp.bfloat16)
    heads_act_here = lax.all_to_all(heads_act, "tp", 0, 1, tiled=True)
    attn_here = matmul(heads_act_here, heads_full)
    heads_low_here = (matmul(heads_act_here, heads_first_all_flattened) * select_here).astype(
        jnp.bfloat16
    )
    middle_here = residual_here + attn_here + matmul(heads_low_here, heads_second_flattened)
    second_norm, second_back = jax.vjp(
        lambda inputs: layer_norm(inputs, feedforward_norm_gain, feedforward_norm_bias), middle_here
    )
    second_act_here = second_norm.astype(jnp.bfloat16)
    (second_act,) = gather_rows((second_act_here,))
    up_low = (matmul(second_act, up_first_flattened) * select).astype(jnp.bfloat16)
    hidden = matmul(second_act, up_full) + matmul(up_low, up_second_flattened)
    activated, gelu_back = jax.vjp(gelu_tanh, hidden)
    activated = activated.astype(jnp.bfloat16)
    down_part = matmul(activated, down_full)
    down_low_part = matmul(activated, down_first_flattened)
    ffn_here, ffn_low_here = scatter_rows((down_part, down_low_part))
    down_low_here = (ffn_low_here * select_here).astype(jnp.bfloat16)
    result_here = (middle_here + ffn_here + matmul(down_low_here, down_second_flattened)).astype(
        jnp.bfloat16
    )
    result_rows, down_low = gather_rows((result_here, down_low_here))
    layer_out = result_rows.reshape(layer_input.shape)
    grad_top_low = output_gradient.reshape(tok_rows, model_width)
    grad_top_here = tp_rows(grad_top_low, tp_count).astype(jnp.float32)
    down_back = (matmul_nt(grad_top_low, down_second_flattened) * select).astype(jnp.bfloat16)
    grad_down_in = matmul_tn(activated, down_back)
    grad_activated = matmul_nt(grad_top_low, down_full) + matmul_nt(down_back, down_first_flattened)
    grad_hidden = gelu_back(grad_activated)[0].astype(jnp.bfloat16)
    up_second_gradient = matmul_tn(up_low, grad_hidden)
    ffn_back_part = matmul_nt(grad_hidden, up_full)
    ffn_back_low = matmul_nt(grad_hidden, up_second_flattened)
    back_here, back_low_here = scatter_rows((ffn_back_part, ffn_back_low))
    up_back_here = (back_low_here * select_here).astype(jnp.bfloat16)
    grad_second = back_here + matmul_nt(up_back_here, up_first_flattened)
    grad_middle_here = grad_top_here + second_back(grad_second)[0]
    grad_middle_low_here = grad_middle_here.astype(jnp.bfloat16)
    heads_back_here = (matmul_nt(grad_middle_low_here, heads_second_flattened) * select_here).astype(
        jnp.bfloat16
    )
    up_back, heads_back = gather_rows((up_back_here, heads_back_here))
    down_second_gradient = matmul_tn(down_low, grad_top_low)
    grad_up_in = matmul_tn(second_act, up_back)
    heads_second_gradient = matmul_tn(heads_low_here, grad_middle_low_here)
    grad_heads_in = matmul_tn(heads_act, heads_back)
    grad_heads_here = (
        matmul_nt(grad_middle_low_here, heads_full)
        + matmul_nt(heads_back_here, heads_first_all_flattened)
    ).astype(jnp.bfloat16)
    grad_heads = lax.all_to_all(grad_heads_here, "tp", 1, 0, tiled=True)
    grad_heads_wide = grad_heads.reshape(seq_here, local_len, device_heads, head_width).astype(
        jnp.float32
    )
    scaled_grad = (grad_heads_wide / per_total).astype(jnp.bfloat16)
    row_delta = jnp.sum(grad_heads_wide * heads_raw, axis=-1) / per_total[..., 0]
    grad_queries, grad_keyrows, grad_valrows = block_grads(
        queries,
        scaled_grad,
        row_delta,
        piece_keys,
        piece_values,
        here_pos,
        key_pos,
        visible_mask,
        slopes,
    )
    grad_keys_all, grad_values_all = (
        lax.psum_scatter(grad_keyrows, "ctx", scatter_dimension=1, tiled=True),
        lax.psum_scatter(grad_valrows, "ctx", scatter_dimension=1, tiled=True),
    )
    grad_projected = jnp.concatenate(
        [
            grad_queries.reshape(tok_rows, local_width),
            grad_keys_all.reshape(tok_rows, local_width),
            grad_values_all.reshape(tok_rows, local_width),
        ],
        axis=1,
    ).astype(jnp.bfloat16)
    projection_second_gradient = matmul_tn(first_low, grad_projected)
    attn_back_part = matmul_nt(grad_projected, qkv_full)
    attn_back_low = matmul_nt(grad_projected, projection_second_flattened)
    first_here, first_low_here = scatter_rows((attn_back_part, attn_back_low))
    qkv_back_here = (first_low_here * select_here).astype(jnp.bfloat16)
    grad_first = first_here + matmul_nt(qkv_back_here, projection_first_flattened)
    input_here = (grad_middle_here + first_back_full(grad_first)[0]).astype(jnp.bfloat16)
    input_rows, qkv_back = gather_rows((input_here, qkv_back_here))
    input_grad = input_rows.reshape(layer_input.shape)
    grad_qkv_in = matmul_tn(first_act, qkv_back)
    heads_second_total = lax.psum(heads_second_gradient, "tp")
    adapter_terms = (
        unflat_in(grad_qkv_in, adapter_tables),
        projection_second_gradient.reshape(adapter_projection_second.shape),
        unflat_in(grad_heads_in, adapter_tables),
        heads_second_total.reshape(adapter_heads_second.shape),
        unflat_in(grad_up_in, adapter_tables),
        up_second_gradient.reshape(adapter_up_second.shape),
        unflat_in(grad_down_in, adapter_tables),
        down_second_gradient.reshape(adapter_down_second.shape),
    )
    summed = lax.psum(adapter_terms, ("shard", "ctx"))
    return (
        layer_out,
        input_grad,
        summed[0],
        summed[1],
        summed[2],
        summed[3],
        summed[4],
        summed[5],
        summed[6],
        summed[7],
    )


def solution(mesh):
    placed = (
        P("shard", "ctx", None),
        P("shard", "ctx", None),
        P("shard", None),
        P("shard"),
        P(),
        P(),
        P(),
        P(),
        P("shard", None, "tp"),
        P("tp", "shard"),
        P("shard", "tp"),
        P("tp", "shard"),
        P(),
        P(None, None, None, "tp"),
        P(None, "tp", None),
        P(),
        P(),
        P(None, None, "tp"),
        P(None, "tp", None),
        P(),
    )
    return jax.shard_map(
        body,
        mesh=mesh,
        in_specs=placed,
        out_specs=(
            P("shard", "ctx", None),
            P("shard", "ctx", None),
            P(),
            P(None, None, None, "tp"),
            P(None, "tp", None),
            P(),
            P(),
            P(None, None, "tp"),
            P(None, "tp", None),
            P(),
        ),
        check_vma=False,
    )
```

```python
import jax
import jax.numpy as jnp
from jax import lax
from jax.sharding import PartitionSpec as P

HD = 128
PIC = 256


NORM_EPS = 1e-05


def layer_norm(inputs, gains, biases):
    average = jnp.mean(inputs, axis=-1, keepdims=True)
    centred = inputs - average
    spread = jnp.mean(centred * centred, axis=-1, keepdims=True)
    return centred * lax.rsqrt(spread + NORM_EPS) * gains + biases


def gelu_tanh(inputs):
    return (
        0.5
        * inputs
        * (1.0 + jnp.tanh(0.7978845608028654 * (inputs + 0.044715 * inputs * inputs * inputs)))
    )


def flattened_first(adapter_mat):
    adapter_tables, inner_dim, rank_width = adapter_mat.shape
    return jnp.transpose(adapter_mat, (1, 0, 2)).reshape(inner_dim, adapter_tables * rank_width)


def flattened_second(adapter_mat):
    return adapter_mat.reshape(adapter_mat.shape[0] * adapter_mat.shape[1], -1)


def unflat_in(grad_flat, adapter_tables):
    inner_dim = grad_flat.shape[0]
    return jnp.transpose(grad_flat.reshape(inner_dim, adapter_tables, -1), (1, 0, 2))


def matmul(left_mat, right_mat):
    return jnp.dot(left_mat, right_mat, preferred_element_type=jnp.float32)


def matmul_tn(left_mat, right_mat):
    return lax.dot_general(
        left_mat, right_mat, (((0,), (0,)), ((), ())), preferred_element_type=jnp.float32
    )


def matmul_nt(left_mat, right_mat):
    return lax.dot_general(
        left_mat, right_mat, (((1,), (1,)), ((), ())), preferred_element_type=jnp.float32
    )


def piece_labels(starts, positions):
    inside = (positions[None, None, :] >= starts[:, :, None]) & (
        positions[None, None, :] < starts[:, :, None] + PIC
    )
    labels = jnp.arange(1, starts.shape[1] + 1, dtype=jnp.int32)
    return jnp.sum(jnp.where(inside, labels[None, :, None], 0), axis=1)


def visible(query_pos, key_pos, query_labels, key_labels):
    causal = key_pos[None, None, :] <= query_pos[None, :, None]
    shared = (query_labels[:, :, None] == key_labels[:, None, :]) & (query_labels[:, :, None] > 0)
    return causal | shared


def exponents(queries, key_rows, query_pos, key_pos, visible_mask, slopes):
    score_scale = queries.shape[-1] ** (-0.5)
    logits = (
        jnp.einsum("sqhd,skhd->shqk", queries, key_rows, preferred_element_type=jnp.float32)
        * score_scale
    )
    distance = jnp.abs(query_pos[:, None] - key_pos[None, :]).astype(jnp.float32)
    logits = logits - slopes[None, :, None, None] * distance[None, None]
    return jnp.where(visible_mask[:, None], jnp.exp(logits), 0.0)


def block_grads(
    queries, scaled_grad, row_delta, key_rows, value_rows, query_pos, key_pos, visible_mask, slopes
):
    score_scale = queries.shape[-1] ** (-0.5)
    exponent = exponents(queries, key_rows, query_pos, key_pos, visible_mask, slopes)
    products_gv = jnp.einsum(
        "sqhd,skhd->shqk", scaled_grad, value_rows, preferred_element_type=jnp.float32
    )
    grad_logits = (
        exponent * (products_gv - jnp.transpose(row_delta, (0, 2, 1))[..., None])
    ).astype(jnp.bfloat16)
    grad_queries = (
        jnp.einsum("shqk,skhd->sqhd", grad_logits, key_rows, preferred_element_type=jnp.float32)
        * score_scale
    )
    grad_keyrows = (
        jnp.einsum("shqk,sqhd->skhd", grad_logits, queries, preferred_element_type=jnp.float32)
        * score_scale
    )
    grad_valrows = jnp.einsum(
        "shqk,sqhd->skhd",
        exponent.astype(jnp.bfloat16),
        scaled_grad,
        preferred_element_type=jnp.float32,
    )
    return (grad_queries, grad_keyrows, grad_valrows)


def tp_rows(rows_array, tp_count):
    chunk = rows_array.shape[0] // tp_count
    return lax.dynamic_slice_in_dim(rows_array, lax.axis_index("tp") * chunk, chunk, axis=0)


def scatter_rows(partials):
    widths = [part.shape[1] for part in partials]
    joined = lax.psum_scatter(
        jnp.concatenate(partials, axis=1).astype(jnp.bfloat16),
        "tp",
        scatter_dimension=0,
        tiled=True,
    )
    return split_columns(joined.astype(jnp.float32), widths)


def gather_rows(rows_here):
    widths = [part.shape[1] for part in rows_here]
    joined = lax.all_gather(jnp.concatenate(rows_here, axis=1), "tp", axis=0, tiled=True)
    return split_columns(joined, widths)


def split_columns(joined, widths):
    parts, offset = [], 0
    for width in widths:
        parts.append(joined[:, offset : offset + width])
        offset += width
    return tuple(parts)


def body(
    layer_input,
    output_gradient,
    picture_piece_starts,
    sequence_adapter_index,
    attention_norm_gain,
    attention_norm_bias,
    feedforward_norm_gain,
    feedforward_norm_bias,
    query_key_value_weight,
    attention_output_weight,
    up_projection_weight,
    down_projection_weight,
    adapter_projection_first,
    adapter_projection_second,
    adapter_heads_first,
    adapter_heads_second,
    adapter_up_first,
    adapter_up_second,
    adapter_down_first,
    adapter_down_second,
):
    seq_here, local_len, model_width = layer_input.shape
    tok_rows = seq_here * local_len
    tp_count = lax.axis_size("tp")
    adapter_tables = adapter_projection_first.shape[0]
    rank_width = adapter_projection_first.shape[2]
    head_width = HD
    device_heads = adapter_projection_second.shape[-1] // head_width
    local_width = device_heads * head_width
    columns = jnp.arange(adapter_tables * rank_width, dtype=jnp.int32) // rank_width
    chosen = (sequence_adapter_index[:, None] == columns[None, :]).astype(jnp.float32)
    select = jnp.broadcast_to(
        chosen[:, None, :], (seq_here, local_len, adapter_tables * rank_width)
    ).reshape(tok_rows, adapter_tables * rank_width)
    select_here = tp_rows(select, tp_count)
    head_ids = lax.axis_index("tp") * device_heads + jnp.arange(device_heads, dtype=jnp.int32)
    slopes = jnp.exp2(
        -8.0 * (head_ids.astype(jnp.float32) + 1.0) / (device_heads * tp_count)
    )
    here_pos = lax.axis_index("ctx") * local_len + jnp.arange(local_len, dtype=jnp.int32)
    here_labels = piece_labels(picture_piece_starts, here_pos)
    heads_full = lax.all_gather(
        lax.all_gather(attention_output_weight, "tp", axis=0, tiled=True),
        "shard",
        axis=1,
        tiled=True,
    )
    heads_first_all = lax.all_gather(adapter_heads_first, "tp", axis=1, tiled=True)
    projection_first_flattened = flattened_first(adapter_projection_first)
    projection_second_flattened = flattened_second(adapter_projection_second)
    heads_first_flattened = flattened_first(adapter_heads_first)
    heads_first_all_flattened = flattened_first(heads_first_all)
    heads_second_flattened = flattened_second(adapter_heads_second)
    up_first_flattened = flattened_first(adapter_up_first)
    up_second_flattened = flattened_second(adapter_up_second)
    down_first_flattened = flattened_first(adapter_down_first)
    down_second_flattened = flattened_second(adapter_down_second)
    residual = layer_input.reshape(tok_rows, model_width).astype(jnp.float32)
    residual_here = tp_rows(residual, tp_count)
    first_norm = layer_norm(residual, attention_norm_gain, attention_norm_bias)
    first_act = first_norm.astype(jnp.bfloat16)
    _, first_back_full = jax.vjp(
        lambda inputs: layer_norm(inputs, attention_norm_gain, attention_norm_bias), residual_here
    )
    gathered_rows = (
        lax.all_gather(query_key_value_weight, "shard", axis=0, tiled=True),
        lax.all_gather(up_projection_weight, "shard", axis=0, tiled=True),
    )
    qkv_full = gathered_rows[0].reshape(model_width, 3 * local_width)
    up_full = gathered_rows[1]
    down_full = lax.all_gather(down_projection_weight, "shard", axis=1, tiled=True)
    first_low = (matmul(first_act, projection_first_flattened) * select).astype(jnp.bfloat16)
    projected = (
        matmul(first_act, qkv_full) + matmul(first_low, projection_second_flattened)
    ).astype(jnp.bfloat16)
    queries_flat = projected[:, :local_width].reshape(seq_here, local_len, local_width)
    queries = queries_flat.reshape(seq_here, local_len, device_heads, head_width)
    key_rows = projected[:, local_width : 2 * local_width].reshape(seq_here, local_len, local_width)
    value_rows = projected[:, 2 * local_width :].reshape(seq_here, local_len, local_width)
    pieces = (
        lax.all_gather(key_rows, "ctx", axis=1, tiled=True),
        lax.all_gather(value_rows, "ctx", axis=1, tiled=True),
    )
    piece_len = pieces[0].shape[1]
    key_pos = jnp.arange(piece_len, dtype=jnp.int32)
    key_labels = piece_labels(picture_piece_starts, key_pos)
    visible_mask = visible(here_pos, key_pos, here_labels, key_labels)
    piece_keys = pieces[0].reshape(seq_here, piece_len, device_heads, head_width)
    piece_values = pieces[1].reshape(seq_here, piece_len, device_heads, head_width)
    exponent = exponents(queries, piece_keys, here_pos, key_pos, visible_mask, slopes)
    weighted = jnp.einsum(
        "shqk,skhd->sqhd",
        exponent.astype(jnp.bfloat16),
        piece_values,
        preferred_element_type=jnp.float32,
    )
    weighted, totals = (weighted, jnp.sum(exponent, axis=-1))
    per_total = jnp.transpose(totals, (0, 2, 1))[..., None]
    heads_raw = weighted / per_total
    heads_act = heads_raw.reshape(tok_rows, local_width).astype(jnp.bfloat16)
    heads_act_here = lax.all_to_all(heads_act, "tp", 0, 1, tiled=True)
    attn_here = matmul(heads_act_here, heads_full)
    heads_low_here = (matmul(heads_act_here, heads_first_all_flattened) * select_here).astype(
        jnp.bfloat16
    )
    middle_here = residual_here + attn_here + matmul(heads_low_here, heads_second_flattened)
    second_norm, second_back = jax.vjp(
        lambda inputs: layer_norm(inputs, feedforward_norm_gain, feedforward_norm_bias), middle_here
    )
    second_act_here = second_norm.astype(jnp.bfloat16)
    (second_act,) = gather_rows((second_act_here,))
    up_low = (matmul(second_act, up_first_flattened) * select).astype(jnp.bfloat16)
    hidden = matmul(second_act, up_full) + matmul(up_low, up_second_flattened)
    activated, gelu_back = jax.vjp(gelu_tanh, hidden)
    activated = activated.astype(jnp.bfloat16)
    down_part = matmul(activated, down_full)
    down_low_part = matmul(activated, down_first_flattened)
    ffn_here, ffn_low_here = scatter_rows((down_part, down_low_part))
    down_low_here = (ffn_low_here * select_here).astype(jnp.bfloat16)
    result_here = (middle_here + ffn_here + matmul(down_low_here, down_second_flattened)).astype(
        jnp.bfloat16
    )
    result_rows, down_low = gather_rows((result_here, down_low_here))
    layer_out = result_rows.reshape(layer_input.shape)
    grad_top_low = output_gradient.reshape(tok_rows, model_width)
    grad_top_here = tp_rows(grad_top_low, tp_count).astype(jnp.float32)
    down_back = (matmul_nt(grad_top_low, down_second_flattened) * select).astype(jnp.bfloat16)
    grad_down_in = matmul_tn(activated, down_back)
    grad_activated = matmul_nt(grad_top_low, down_full) + matmul_nt(down_back, down_first_flattened)
    grad_hidden = gelu_back(grad_activated)[0].astype(jnp.bfloat16)
    up_second_gradient = matmul_tn(up_low, grad_hidden)
    ffn_back_part = matmul_nt(grad_hidden, up_full)
    ffn_back_low = matmul_nt(grad_hidden, up_second_flattened)
    back_here, back_low_here = scatter_rows((ffn_back_part, ffn_back_low))
    up_back_here = (back_low_here * select_here).astype(jnp.bfloat16)
    grad_second = back_here + matmul_nt(up_back_here, up_first_flattened)
    grad_middle_here = grad_top_here + second_back(grad_second)[0]
    grad_middle_low_here = grad_middle_here.astype(jnp.bfloat16)
    heads_back_here = (matmul_nt(grad_middle_low_here, heads_second_flattened) * select_here).astype(
        jnp.bfloat16
    )
    up_back, heads_back = gather_rows((up_back_here, heads_back_here))
    down_second_gradient = matmul_tn(down_low, grad_top_low)
    grad_up_in = matmul_tn(second_act, up_back)
    heads_second_gradient = matmul_tn(heads_low_here, grad_middle_low_here)
    grad_heads_in = matmul_tn(heads_act, heads_back)
    grad_heads_here = (
        matmul_nt(grad_middle_low_here, heads_full)
        + matmul_nt(heads_back_here, heads_first_all_flattened)
    ).astype(jnp.bfloat16)
    grad_heads = lax.all_to_all(grad_heads_here, "tp", 1, 0, tiled=True)
    grad_heads_wide = grad_heads.reshape(seq_here, local_len, device_heads, head_width).astype(
        jnp.float32
    )
    scaled_grad = (grad_heads_wide / per_total).astype(jnp.bfloat16)
    row_delta = jnp.sum(grad_heads_wide * heads_raw, axis=-1) / per_total[..., 0]
    grad_queries, grad_keyrows, grad_valrows = block_grads(
        queries,
        scaled_grad,
        row_delta,
        piece_keys,
        piece_values,
        here_pos,
        key_pos,
        visible_mask,
        slopes,
    )
    grad_keys_all, grad_values_all = (
        lax.psum_scatter(grad_keyrows, "ctx", scatter_dimension=1, tiled=True),
        lax.psum_scatter(grad_valrows, "ctx", scatter_dimension=1, tiled=True),
    )
    grad_projected = jnp.concatenate(
        [
            grad_queries.reshape(tok_rows, local_width),
            grad_keys_all.reshape(tok_rows, local_width),
            grad_values_all.reshape(tok_rows, local_width),
        ],
        axis=1,
    ).astype(jnp.bfloat16)
    projection_second_gradient = matmul_tn(first_low, grad_projected)
    attn_back_part = matmul_nt(grad_projected, qkv_full)
    attn_back_low = matmul_nt(grad_projected, projection_second_flattened)
    first_here, first_low_here = scatter_rows((attn_back_part, attn_back_low))
    qkv_back_here = (first_low_here * select_here).astype(jnp.bfloat16)
    grad_first = first_here + matmul_nt(qkv_back_here, projection_first_flattened)
    input_here = (grad_middle_here + first_back_full(grad_first)[0]).astype(jnp.bfloat16)
    input_rows, qkv_back = gather_rows((input_here, qkv_back_here))
    input_grad = input_rows.reshape(layer_input.shape)
    grad_qkv_in = matmul_tn(first_act, qkv_back)
    heads_second_total = lax.psum(heads_second_gradient, "tp")
    adapter_terms = (
        unflat_in(grad_qkv_in, adapter_tables),
        projection_second_gradient.reshape(adapter_projection_second.shape),
        unflat_in(grad_heads_in, adapter_tables),
        heads_second_total.reshape(adapter_heads_second.shape),
        unflat_in(grad_up_in, adapter_tables),
        up_second_gradient.reshape(adapter_up_second.shape),
        unflat_in(grad_down_in, adapter_tables),
        down_second_gradient.reshape(adapter_down_second.shape),
    )
    summed = lax.psum(adapter_terms, ("shard", "ctx"))
    return (
        layer_out,
        input_grad,
        summed[0],
        summed[1],
        summed[2],
        summed[3],
        summed[4],
        summed[5],
        summed[6],
        summed[7],
    )


def solution(mesh):
    placed = (
        P("shard", "ctx", None),
        P("shard", "ctx", None),
        P("shard", None),
        P("shard"),
        P(),
        P(),
        P(),
        P(),
        P("shard", None, "tp"),
        P("tp", "shard"),
        P("shard", "tp"),
        P("tp", "shard"),
        P(),
        P(None, None, None, "tp"),
        P(None, "tp", None),
        P(),
        P(),
        P(None, None, "tp"),
        P(None, "tp", None),
        P(),
    )
    return jax.shard_map(
        body,
        mesh=mesh,
        in_specs=placed,
        out_specs=(
            P("shard", "ctx", None),
            P("shard", "ctx", None),
            P(),
            P(None, None, None, "tp"),
            P(None, "tp", None),
            P(),
            P(),
            P(None, None, "tp"),
            P(None, "tp", None),
            P(),
        ),
        check_vma=False,
    )
```

```python
import jax
import jax.numpy as jnp
from jax import lax
from jax.sharding import PartitionSpec as P

HD = 128
PIC = 256


NORM_EPS = 1e-05


def layer_norm(inputs, gains, biases):
    average = jnp.mean(inputs, axis=-1, keepdims=True)
    centred = inputs - average
    spread = jnp.mean(centred * centred, axis=-1, keepdims=True)
    return centred * lax.rsqrt(spread + NORM_EPS) * gains + biases


def gelu_tanh(inputs):
    return (
        0.5
        * inputs
        * (1.0 + jnp.tanh(0.7978845608028654 * (inputs + 0.044715 * inputs * inputs * inputs)))
    )


def flattened_first(adapter_mat):
    adapter_tables, inner_dim, rank_width = adapter_mat.shape
    return jnp.transpose(adapter_mat, (1, 0, 2)).reshape(inner_dim, adapter_tables * rank_width)


def flattened_second(adapter_mat):
    return adapter_mat.reshape(adapter_mat.shape[0] * adapter_mat.shape[1], -1)


def unflat_in(grad_flat, adapter_tables):
    inner_dim = grad_flat.shape[0]
    return jnp.transpose(grad_flat.reshape(inner_dim, adapter_tables, -1), (1, 0, 2))


def matmul(left_mat, right_mat):
    return jnp.dot(left_mat, right_mat, preferred_element_type=jnp.float32)


def matmul_tn(left_mat, right_mat):
    return lax.dot_general(
        left_mat, right_mat, (((0,), (0,)), ((), ())), preferred_element_type=jnp.float32
    )


def matmul_nt(left_mat, right_mat):
    return lax.dot_general(
        left_mat, right_mat, (((1,), (1,)), ((), ())), preferred_element_type=jnp.float32
    )


def piece_labels(starts, positions):
    inside = (positions[None, None, :] >= starts[:, :, None]) & (
        positions[None, None, :] < starts[:, :, None] + PIC
    )
    labels = jnp.arange(1, starts.shape[1] + 1, dtype=jnp.int32)
    return jnp.sum(jnp.where(inside, labels[None, :, None], 0), axis=1)


def visible(query_pos, key_pos, query_labels, key_labels):
    causal = key_pos[None, None, :] <= query_pos[None, :, None]
    shared = (query_labels[:, :, None] == key_labels[:, None, :]) & (query_labels[:, :, None] > 0)
    return causal | shared


def exponents(queries, key_rows, query_pos, key_pos, visible_mask, slopes):
    score_scale = queries.shape[-1] ** (-0.5)
    logits = (
        jnp.einsum("sqhd,skhd->shqk", queries, key_rows, preferred_element_type=jnp.float32)
        * score_scale
    )
    distance = jnp.abs(query_pos[:, None] - key_pos[None, :]).astype(jnp.float32)
    logits = logits - slopes[None, :, None, None] * distance[None, None]
    return jnp.where(visible_mask[:, None], jnp.exp(logits), 0.0)


def block_grads(
    queries, scaled_grad, row_delta, key_rows, value_rows, query_pos, key_pos, visible_mask, slopes
):
    score_scale = queries.shape[-1] ** (-0.5)
    exponent = exponents(queries, key_rows, query_pos, key_pos, visible_mask, slopes)
    products_gv = jnp.einsum(
        "sqhd,skhd->shqk", scaled_grad, value_rows, preferred_element_type=jnp.float32
    )
    grad_logits = (
        exponent * (products_gv - jnp.transpose(row_delta, (0, 2, 1))[..., None])
    ).astype(jnp.bfloat16)
    grad_queries = (
        jnp.einsum("shqk,skhd->sqhd", grad_logits, key_rows, preferred_element_type=jnp.float32)
        * score_scale
    )
    grad_keyrows = (
        jnp.einsum("shqk,sqhd->skhd", grad_logits, queries, preferred_element_type=jnp.float32)
        * score_scale
    )
    grad_valrows = jnp.einsum(
        "shqk,sqhd->skhd",
        exponent.astype(jnp.bfloat16),
        scaled_grad,
        preferred_element_type=jnp.float32,
    )
    return (grad_queries, grad_keyrows, grad_valrows)


def partner_swaps(block, axis_name, axis_count):
    received = [block]
    for offset in range(1, axis_count):
        pairs = [(index, index ^ offset) for index in range(axis_count)]
        received.append(lax.ppermute(block, axis_name, pairs))
    return received


def pair_gather(block, axis_name, axis):
    if lax.axis_size(axis_name) != 2:
        return lax.all_gather(block, axis_name, axis=axis, tiled=True)
    other = lax.ppermute(block, axis_name, [(0, 1), (1, 0)])
    first = lax.axis_index(axis_name) == 0
    low = jnp.where(first, block, other)
    high = jnp.where(first, other, block)
    return jnp.concatenate([low, high], axis=axis)


def tp_rows(rows_array, tp_count):
    chunk = rows_array.shape[0] // tp_count
    return lax.dynamic_slice_in_dim(rows_array, lax.axis_index("tp") * chunk, chunk, axis=0)


def scatter_rows(partials):
    widths = [part.shape[1] for part in partials]
    joined = lax.psum_scatter(
        jnp.concatenate(partials, axis=1).astype(jnp.bfloat16),
        "tp",
        scatter_dimension=0,
        tiled=True,
    )
    return split_columns(joined.astype(jnp.float32), widths)


def gather_rows(rows_here):
    widths = [part.shape[1] for part in rows_here]
    joined = lax.all_gather(jnp.concatenate(rows_here, axis=1), "tp", axis=0, tiled=True)
    return split_columns(joined, widths)


def split_columns(joined, widths):
    parts, offset = [], 0
    for width in widths:
        parts.append(joined[:, offset : offset + width])
        offset += width
    return tuple(parts)


def body(
    layer_input,
    output_gradient,
    picture_piece_starts,
    sequence_adapter_index,
    attention_norm_gain,
    attention_norm_bias,
    feedforward_norm_gain,
    feedforward_norm_bias,
    query_key_value_weight,
    attention_output_weight,
    up_projection_weight,
    down_projection_weight,
    adapter_projection_first,
    adapter_projection_second,
    adapter_heads_first,
    adapter_heads_second,
    adapter_up_first,
    adapter_up_second,
    adapter_down_first,
    adapter_down_second,
):
    seq_here, local_len, model_width = layer_input.shape
    tok_rows = seq_here * local_len
    tp_count = lax.axis_size("tp")
    adapter_tables = adapter_projection_first.shape[0]
    rank_width = adapter_projection_first.shape[2]
    head_width = HD
    device_heads = adapter_projection_second.shape[-1] // head_width
    local_width = device_heads * head_width
    columns = jnp.arange(adapter_tables * rank_width, dtype=jnp.int32) // rank_width
    chosen = (sequence_adapter_index[:, None] == columns[None, :]).astype(jnp.float32)
    select = jnp.broadcast_to(
        chosen[:, None, :], (seq_here, local_len, adapter_tables * rank_width)
    ).reshape(tok_rows, adapter_tables * rank_width)
    select_here = tp_rows(select, tp_count)
    head_ids = lax.axis_index("tp") * device_heads + jnp.arange(device_heads, dtype=jnp.int32)
    slopes = jnp.exp2(
        -8.0 * (head_ids.astype(jnp.float32) + 1.0) / (device_heads * tp_count)
    )
    here_pos = lax.axis_index("ctx") * local_len + jnp.arange(local_len, dtype=jnp.int32)
    here_labels = piece_labels(picture_piece_starts, here_pos)
    heads_full = pair_gather(
        lax.all_gather(attention_output_weight, "tp", axis=0, tiled=True), "shard", 1
    )
    heads_first_all = lax.all_gather(adapter_heads_first, "tp", axis=1, tiled=True)
    projection_first_flattened = flattened_first(adapter_projection_first)
    projection_second_flattened = flattened_second(adapter_projection_second)
    heads_first_flattened = flattened_first(adapter_heads_first)
    heads_first_all_flattened = flattened_first(heads_first_all)
    heads_second_flattened = flattened_second(adapter_heads_second)
    up_first_flattened = flattened_first(adapter_up_first)
    up_second_flattened = flattened_second(adapter_up_second)
    down_first_flattened = flattened_first(adapter_down_first)
    down_second_flattened = flattened_second(adapter_down_second)
    residual = layer_input.reshape(tok_rows, model_width).astype(jnp.float32)
    residual_here = tp_rows(residual, tp_count)
    first_norm = layer_norm(residual, attention_norm_gain, attention_norm_bias)
    first_act = first_norm.astype(jnp.bfloat16)
    _, first_back_full = jax.vjp(
        lambda inputs: layer_norm(inputs, attention_norm_gain, attention_norm_bias), residual_here
    )
    gathered_rows = (
        pair_gather(query_key_value_weight, "shard", 0),
        pair_gather(up_projection_weight, "shard", 0),
    )
    qkv_full = gathered_rows[0].reshape(model_width, 3 * local_width)
    up_full = gathered_rows[1]
    down_full = pair_gather(down_projection_weight, "shard", 1)
    first_low = (matmul(first_act, projection_first_flattened) * select).astype(jnp.bfloat16)
    projected = (
        matmul(first_act, qkv_full) + matmul(first_low, projection_second_flattened)
    ).astype(jnp.bfloat16)
    queries_flat = projected[:, :local_width].reshape(seq_here, local_len, local_width)
    queries = queries_flat.reshape(seq_here, local_len, device_heads, head_width)
    key_rows = projected[:, local_width : 2 * local_width].reshape(seq_here, local_len, local_width)
    value_rows = projected[:, 2 * local_width :].reshape(seq_here, local_len, local_width)
    ctx_count = lax.axis_size("ctx")
    ctx_here = lax.axis_index("ctx")
    blocks = partner_swaps(
        jnp.concatenate([key_rows, value_rows], axis=2), "ctx", ctx_count
    )
    pieces = jnp.concatenate(blocks, axis=1)
    piece_len = pieces.shape[1]
    key_pos = jnp.concatenate(
        [
            (ctx_here ^ offset) * local_len + jnp.arange(local_len, dtype=jnp.int32)
            for offset in range(ctx_count)
        ]
    )
    key_labels = piece_labels(picture_piece_starts, key_pos)
    visible_mask = visible(here_pos, key_pos, here_labels, key_labels)
    piece_keys = pieces[:, :, :local_width].reshape(seq_here, piece_len, device_heads, head_width)
    piece_values = pieces[:, :, local_width:].reshape(
        seq_here, piece_len, device_heads, head_width
    )
    exponent = exponents(queries, piece_keys, here_pos, key_pos, visible_mask, slopes)
    weighted = jnp.einsum(
        "shqk,skhd->sqhd",
        exponent.astype(jnp.bfloat16),
        piece_values,
        preferred_element_type=jnp.float32,
    )
    weighted, totals = (weighted, jnp.sum(exponent, axis=-1))
    per_total = jnp.transpose(totals, (0, 2, 1))[..., None]
    heads_raw = weighted / per_total
    heads_act = heads_raw.reshape(tok_rows, local_width).astype(jnp.bfloat16)
    heads_act_here = lax.all_to_all(heads_act, "tp", 0, 1, tiled=True)
    attn_here = matmul(heads_act_here, heads_full)
    heads_low_here = (matmul(heads_act_here, heads_first_all_flattened) * select_here).astype(
        jnp.bfloat16
    )
    middle_here = residual_here + attn_here + matmul(heads_low_here, heads_second_flattened)
    second_norm, second_back = jax.vjp(
        lambda inputs: layer_norm(inputs, feedforward_norm_gain, feedforward_norm_bias), middle_here
    )
    second_act_here = second_norm.astype(jnp.bfloat16)
    (second_act,) = gather_rows((second_act_here,))
    up_low = (matmul(second_act, up_first_flattened) * select).astype(jnp.bfloat16)
    hidden = matmul(second_act, up_full) + matmul(up_low, up_second_flattened)
    activated, gelu_back = jax.vjp(gelu_tanh, hidden)
    activated = activated.astype(jnp.bfloat16)
    down_part = matmul(activated, down_full)
    down_low_part = matmul(activated, down_first_flattened)
    ffn_here, ffn_low_here = scatter_rows((down_part, down_low_part))
    down_low_here = (ffn_low_here * select_here).astype(jnp.bfloat16)
    result_here = (middle_here + ffn_here + matmul(down_low_here, down_second_flattened)).astype(
        jnp.bfloat16
    )
    result_rows, down_low = gather_rows((result_here, down_low_here))
    layer_out = result_rows.reshape(layer_input.shape)
    grad_top_low = output_gradient.reshape(tok_rows, model_width)
    grad_top_here = tp_rows(grad_top_low, tp_count).astype(jnp.float32)
    down_back = (matmul_nt(grad_top_low, down_second_flattened) * select).astype(jnp.bfloat16)
    grad_down_in = matmul_tn(activated, down_back)
    grad_activated = matmul_nt(grad_top_low, down_full) + matmul_nt(down_back, down_first_flattened)
    grad_hidden = gelu_back(grad_activated)[0].astype(jnp.bfloat16)
    up_second_gradient = matmul_tn(up_low, grad_hidden)
    ffn_back_part = matmul_nt(grad_hidden, up_full)
    ffn_back_low = matmul_nt(grad_hidden, up_second_flattened)
    back_here, back_low_here = scatter_rows((ffn_back_part, ffn_back_low))
    up_back_here = (back_low_here * select_here).astype(jnp.bfloat16)
    grad_second = back_here + matmul_nt(up_back_here, up_first_flattened)
    grad_middle_here = grad_top_here + second_back(grad_second)[0]
    grad_middle_low_here = grad_middle_here.astype(jnp.bfloat16)
    heads_back_here = (matmul_nt(grad_middle_low_here, heads_second_flattened) * select_here).astype(
        jnp.bfloat16
    )
    up_back, heads_back = gather_rows((up_back_here, heads_back_here))
    down_second_gradient = matmul_tn(down_low, grad_top_low)
    grad_up_in = matmul_tn(second_act, up_back)
    heads_second_gradient = matmul_tn(heads_low_here, grad_middle_low_here)
    grad_heads_in = matmul_tn(heads_act, heads_back)
    grad_heads_here = (
        matmul_nt(grad_middle_low_here, heads_full)
        + matmul_nt(heads_back_here, heads_first_all_flattened)
    ).astype(jnp.bfloat16)
    grad_heads = lax.all_to_all(grad_heads_here, "tp", 1, 0, tiled=True)
    grad_heads_wide = grad_heads.reshape(seq_here, local_len, device_heads, head_width).astype(
        jnp.float32
    )
    scaled_grad = (grad_heads_wide / per_total).astype(jnp.bfloat16)
    row_delta = jnp.sum(grad_heads_wide * heads_raw, axis=-1) / per_total[..., 0]
    grad_queries, grad_keyrows, grad_valrows = block_grads(
        queries,
        scaled_grad,
        row_delta,
        piece_keys,
        piece_values,
        here_pos,
        key_pos,
        visible_mask,
        slopes,
    )
    grad_kv = jnp.concatenate(
        [
            grad_keyrows.reshape(seq_here, ctx_count, local_len, local_width),
            grad_valrows.reshape(seq_here, ctx_count, local_len, local_width),
        ],
        axis=3,
    )
    grad_kv_here = grad_kv[:, 0]
    for offset in range(1, ctx_count):
        pairs = [(index, index ^ offset) for index in range(ctx_count)]
        grad_kv_here = grad_kv_here + lax.ppermute(grad_kv[:, offset], "ctx", pairs)
    grad_keys_all = grad_kv_here[:, :, :local_width]
    grad_values_all = grad_kv_here[:, :, local_width:]
    grad_projected = jnp.concatenate(
        [
            grad_queries.reshape(tok_rows, local_width),
            grad_keys_all.reshape(tok_rows, local_width),
            grad_values_all.reshape(tok_rows, local_width),
        ],
        axis=1,
    ).astype(jnp.bfloat16)
    projection_second_gradient = matmul_tn(first_low, grad_projected)
    attn_back_part = matmul_nt(grad_projected, qkv_full)
    attn_back_low = matmul_nt(grad_projected, projection_second_flattened)
    first_here, first_low_here = scatter_rows((attn_back_part, attn_back_low))
    qkv_back_here = (first_low_here * select_here).astype(jnp.bfloat16)
    grad_first = first_here + matmul_nt(qkv_back_here, projection_first_flattened)
    input_here = (grad_middle_here + first_back_full(grad_first)[0]).astype(jnp.bfloat16)
    input_rows, qkv_back = gather_rows((input_here, qkv_back_here))
    input_grad = input_rows.reshape(layer_input.shape)
    grad_qkv_in = matmul_tn(first_act, qkv_back)
    heads_second_total = lax.psum(heads_second_gradient, "tp")
    adapter_terms = (
        unflat_in(grad_qkv_in, adapter_tables),
        projection_second_gradient.reshape(adapter_projection_second.shape),
        unflat_in(grad_heads_in, adapter_tables),
        heads_second_total.reshape(adapter_heads_second.shape),
        unflat_in(grad_up_in, adapter_tables),
        up_second_gradient.reshape(adapter_up_second.shape),
        unflat_in(grad_down_in, adapter_tables),
        down_second_gradient.reshape(adapter_down_second.shape),
    )
    summed = lax.psum(adapter_terms, ("shard", "ctx"))
    return (
        layer_out,
        input_grad,
        summed[0],
        summed[1],
        summed[2],
        summed[3],
        summed[4],
        summed[5],
        summed[6],
        summed[7],
    )


def solution(mesh):
    placed = (
        P("shard", "ctx", None),
        P("shard", "ctx", None),
        P("shard", None),
        P("shard"),
        P(),
        P(),
        P(),
        P(),
        P("shard", None, "tp"),
        P("tp", "shard"),
        P("shard", "tp"),
        P("tp", "shard"),
        P(),
        P(None, None, None, "tp"),
        P(None, "tp", None),
        P(),
        P(),
        P(None, None, "tp"),
        P(None, "tp", None),
        P(),
    )
    return jax.shard_map(
        body,
        mesh=mesh,
        in_specs=placed,
        out_specs=(
            P("shard", "ctx", None),
            P("shard", "ctx", None),
            P(),
            P(None, None, None, "tp"),
            P(None, "tp", None),
            P(),
            P(),
            P(None, None, "tp"),
            P(None, "tp", None),
            P(),
        ),
        check_vma=False,
    )
```

```python
import jax
import jax.numpy as jnp
from jax import lax
from jax.sharding import PartitionSpec as P

HD = 128
PIC = 256


NORM_EPS = 1e-05


def layer_norm(inputs, gains, biases):
    average = jnp.mean(inputs, axis=-1, keepdims=True)
    centred = inputs - average
    spread = jnp.mean(centred * centred, axis=-1, keepdims=True)
    return centred * lax.rsqrt(spread + NORM_EPS) * gains + biases


def gelu_tanh(inputs):
    return (
        0.5
        * inputs
        * (1.0 + jnp.tanh(0.7978845608028654 * (inputs + 0.044715 * inputs * inputs * inputs)))
    )


def flattened_first(adapter_mat):
    adapter_tables, inner_dim, rank_width = adapter_mat.shape
    return jnp.transpose(adapter_mat, (1, 0, 2)).reshape(inner_dim, adapter_tables * rank_width)


def flattened_second(adapter_mat):
    return adapter_mat.reshape(adapter_mat.shape[0] * adapter_mat.shape[1], -1)


def unflat_in(grad_flat, adapter_tables):
    inner_dim = grad_flat.shape[0]
    return jnp.transpose(grad_flat.reshape(inner_dim, adapter_tables, -1), (1, 0, 2))


def matmul(left_mat, right_mat):
    return jnp.dot(left_mat, right_mat, preferred_element_type=jnp.float32)


def matmul_tn(left_mat, right_mat):
    return lax.dot_general(
        left_mat, right_mat, (((0,), (0,)), ((), ())), preferred_element_type=jnp.float32
    )


def matmul_nt(left_mat, right_mat):
    return lax.dot_general(
        left_mat, right_mat, (((1,), (1,)), ((), ())), preferred_element_type=jnp.float32
    )


def piece_labels(starts, positions):
    inside = (positions[None, None, :] >= starts[:, :, None]) & (
        positions[None, None, :] < starts[:, :, None] + PIC
    )
    labels = jnp.arange(1, starts.shape[1] + 1, dtype=jnp.int32)
    return jnp.sum(jnp.where(inside, labels[None, :, None], 0), axis=1)


def visible(query_pos, key_pos, query_labels, key_labels):
    causal = key_pos[None, None, :] <= query_pos[None, :, None]
    shared = (query_labels[:, :, None] == key_labels[:, None, :]) & (query_labels[:, :, None] > 0)
    return causal | shared


def exponents(queries, key_rows, query_pos, key_pos, visible_mask, slopes):
    score_scale = queries.shape[-1] ** (-0.5)
    logits = (
        jnp.einsum("sqhd,skhd->shqk", queries, key_rows, preferred_element_type=jnp.float32)
        * score_scale
    )
    distance = jnp.abs(query_pos[:, None] - key_pos[None, :]).astype(jnp.float32)
    logits = logits - slopes[None, :, None, None] * distance[None, None]
    return jnp.where(visible_mask[:, None], jnp.exp(logits), 0.0)


def block_grads(
    queries, scaled_grad, row_delta, key_rows, value_rows, query_pos, key_pos, visible_mask, slopes
):
    score_scale = queries.shape[-1] ** (-0.5)
    exponent = exponents(queries, key_rows, query_pos, key_pos, visible_mask, slopes)
    products_gv = jnp.einsum(
        "sqhd,skhd->shqk", scaled_grad, value_rows, preferred_element_type=jnp.float32
    )
    grad_logits = (
        exponent * (products_gv - jnp.transpose(row_delta, (0, 2, 1))[..., None])
    ).astype(jnp.bfloat16)
    grad_queries = (
        jnp.einsum("shqk,skhd->sqhd", grad_logits, key_rows, preferred_element_type=jnp.float32)
        * score_scale
    )
    grad_keyrows = (
        jnp.einsum("shqk,sqhd->skhd", grad_logits, queries, preferred_element_type=jnp.float32)
        * score_scale
    )
    grad_valrows = jnp.einsum(
        "shqk,sqhd->skhd",
        exponent.astype(jnp.bfloat16),
        scaled_grad,
        preferred_element_type=jnp.float32,
    )
    return (grad_queries, grad_keyrows, grad_valrows)


def partner_swaps(block, axis_name, axis_count):
    received = [block]
    for offset in range(1, axis_count):
        pairs = [(index, index ^ offset) for index in range(axis_count)]
        received.append(lax.ppermute(block, axis_name, pairs))
    return received


def pair_gather(block, axis_name, axis):
    if lax.axis_size(axis_name) != 2:
        return lax.all_gather(block, axis_name, axis=axis, tiled=True)
    other = lax.ppermute(block, axis_name, [(0, 1), (1, 0)])
    first = lax.axis_index(axis_name) == 0
    low = jnp.where(first, block, other)
    high = jnp.where(first, other, block)
    return jnp.concatenate([low, high], axis=axis)


def tp_rows(rows_array, tp_count):
    chunk = rows_array.shape[0] // tp_count
    return lax.dynamic_slice_in_dim(rows_array, lax.axis_index("tp") * chunk, chunk, axis=0)


def scatter_rows(partials):
    widths = [part.shape[1] for part in partials]
    joined = lax.psum_scatter(
        jnp.concatenate(partials, axis=1).astype(jnp.bfloat16),
        "tp",
        scatter_dimension=0,
        tiled=True,
    )
    return split_columns(joined.astype(jnp.float32), widths)


def gather_rows(rows_here):
    widths = [part.shape[1] for part in rows_here]
    joined = lax.all_gather(jnp.concatenate(rows_here, axis=1), "tp", axis=0, tiled=True)
    return split_columns(joined, widths)


def split_columns(joined, widths):
    parts, offset = [], 0
    for width in widths:
        parts.append(joined[:, offset : offset + width])
        offset += width
    return tuple(parts)


def layer_body(
    layer_input,
    output_gradient,
    picture_piece_starts,
    sequence_adapter_index,
    attention_norm_gain,
    attention_norm_bias,
    feedforward_norm_gain,
    feedforward_norm_bias,
    query_key_value_weight,
    attention_output_weight,
    up_projection_weight,
    down_projection_weight,
    adapter_projection_first,
    adapter_projection_second,
    adapter_heads_first,
    adapter_heads_second,
    adapter_up_first,
    adapter_up_second,
    adapter_down_first,
    adapter_down_second,
):
    seq_here, local_len, model_width = layer_input.shape
    tok_rows = seq_here * local_len
    tp_count = lax.axis_size("tp")
    adapter_tables = adapter_projection_first.shape[0]
    rank_width = adapter_projection_first.shape[2]
    head_width = HD
    device_heads = adapter_projection_second.shape[-1] // head_width
    local_width = device_heads * head_width
    columns = jnp.arange(adapter_tables * rank_width, dtype=jnp.int32) // rank_width
    chosen = (sequence_adapter_index[:, None] == columns[None, :]).astype(jnp.float32)
    select = jnp.broadcast_to(
        chosen[:, None, :], (seq_here, local_len, adapter_tables * rank_width)
    ).reshape(tok_rows, adapter_tables * rank_width)
    select_here = tp_rows(select, tp_count)
    head_ids = lax.axis_index("tp") * device_heads + jnp.arange(device_heads, dtype=jnp.int32)
    slopes = jnp.exp2(
        -8.0 * (head_ids.astype(jnp.float32) + 1.0) / (device_heads * tp_count)
    )
    here_pos = lax.axis_index("ctx") * local_len + jnp.arange(local_len, dtype=jnp.int32)
    here_labels = piece_labels(picture_piece_starts, here_pos)
    heads_first_local = flattened_first(adapter_heads_first)
    heads_pair = lax.all_gather(
        jnp.concatenate([attention_output_weight, heads_first_local], axis=1),
        "tp",
        axis=0,
        tiled=True,
    )
    out_cols = attention_output_weight.shape[1]
    heads_full = pair_gather(heads_pair[:, :out_cols], "shard", 1)
    heads_first_all_flattened = heads_pair[:, out_cols:]
    projection_first_flattened = flattened_first(adapter_projection_first)
    projection_second_flattened = flattened_second(adapter_projection_second)
    heads_first_flattened = flattened_first(adapter_heads_first)
    heads_second_flattened = flattened_second(adapter_heads_second)
    up_first_flattened = flattened_first(adapter_up_first)
    up_second_flattened = flattened_second(adapter_up_second)
    down_first_flattened = flattened_first(adapter_down_first)
    down_second_flattened = flattened_second(adapter_down_second)
    residual = layer_input.reshape(tok_rows, model_width).astype(jnp.float32)
    residual_here = tp_rows(residual, tp_count)
    first_norm = layer_norm(residual, attention_norm_gain, attention_norm_bias)
    first_act = first_norm.astype(jnp.bfloat16)
    _, first_back_full = jax.vjp(
        lambda inputs: layer_norm(inputs, attention_norm_gain, attention_norm_bias), residual_here
    )
    gathered_rows = (
        pair_gather(query_key_value_weight, "shard", 0),
        pair_gather(up_projection_weight, "shard", 0),
    )
    qkv_full = gathered_rows[0].reshape(model_width, 3 * local_width)
    up_full = gathered_rows[1]
    down_full = pair_gather(down_projection_weight, "shard", 1)
    first_low = (matmul(first_act, projection_first_flattened) * select).astype(jnp.bfloat16)
    projected = (
        matmul(first_act, qkv_full) + matmul(first_low, projection_second_flattened)
    ).astype(jnp.bfloat16)
    queries_flat = projected[:, :local_width].reshape(seq_here, local_len, local_width)
    queries = queries_flat.reshape(seq_here, local_len, device_heads, head_width)
    key_rows = projected[:, local_width : 2 * local_width].reshape(seq_here, local_len, local_width)
    value_rows = projected[:, 2 * local_width :].reshape(seq_here, local_len, local_width)
    ctx_count = lax.axis_size("ctx")
    ctx_here = lax.axis_index("ctx")
    blocks = partner_swaps(
        jnp.concatenate([key_rows, value_rows], axis=2), "ctx", ctx_count
    )
    pieces = jnp.concatenate(blocks, axis=1)
    piece_len = pieces.shape[1]
    key_pos = jnp.concatenate(
        [
            (ctx_here ^ offset) * local_len + jnp.arange(local_len, dtype=jnp.int32)
            for offset in range(ctx_count)
        ]
    )
    key_labels = piece_labels(picture_piece_starts, key_pos)
    visible_mask = visible(here_pos, key_pos, here_labels, key_labels)
    piece_keys = pieces[:, :, :local_width].reshape(seq_here, piece_len, device_heads, head_width)
    piece_values = pieces[:, :, local_width:].reshape(
        seq_here, piece_len, device_heads, head_width
    )
    exponent = exponents(queries, piece_keys, here_pos, key_pos, visible_mask, slopes)
    weighted = jnp.einsum(
        "shqk,skhd->sqhd",
        exponent.astype(jnp.bfloat16),
        piece_values,
        preferred_element_type=jnp.float32,
    )
    weighted, totals = (weighted, jnp.sum(exponent, axis=-1))
    per_total = jnp.transpose(totals, (0, 2, 1))[..., None]
    heads_raw = weighted / per_total
    heads_act = heads_raw.reshape(tok_rows, local_width).astype(jnp.bfloat16)
    heads_act_here = lax.all_to_all(heads_act, "tp", 0, 1, tiled=True)
    attn_here = matmul(heads_act_here, heads_full)
    heads_low_here = (matmul(heads_act_here, heads_first_all_flattened) * select_here).astype(
        jnp.bfloat16
    )
    middle_here = residual_here + attn_here + matmul(heads_low_here, heads_second_flattened)
    second_norm, second_back = jax.vjp(
        lambda inputs: layer_norm(inputs, feedforward_norm_gain, feedforward_norm_bias), middle_here
    )
    second_act_here = second_norm.astype(jnp.bfloat16)
    (second_act,) = gather_rows((second_act_here,))
    up_low = (matmul(second_act, up_first_flattened) * select).astype(jnp.bfloat16)
    hidden = matmul(second_act, up_full) + matmul(up_low, up_second_flattened)
    activated, gelu_back = jax.vjp(gelu_tanh, hidden)
    activated = activated.astype(jnp.bfloat16)
    down_part = matmul(activated, down_full)
    down_low_part = matmul(activated, down_first_flattened)
    ffn_here, ffn_low_here = scatter_rows((down_part, down_low_part))
    down_low_here = (ffn_low_here * select_here).astype(jnp.bfloat16)
    result_here = (middle_here + ffn_here + matmul(down_low_here, down_second_flattened)).astype(
        jnp.bfloat16
    )
    (result_rows,) = gather_rows((result_here,))
    layer_out = result_rows.reshape(layer_input.shape)
    grad_top_low = output_gradient.reshape(tok_rows, model_width)
    grad_top_here = tp_rows(grad_top_low, tp_count).astype(jnp.float32)
    down_back = (matmul_nt(grad_top_low, down_second_flattened) * select).astype(jnp.bfloat16)
    grad_down_in = matmul_tn(activated, down_back)
    grad_activated = matmul_nt(grad_top_low, down_full) + matmul_nt(down_back, down_first_flattened)
    grad_hidden = gelu_back(grad_activated)[0].astype(jnp.bfloat16)
    up_second_gradient = matmul_tn(up_low, grad_hidden)
    ffn_back_part = matmul_nt(grad_hidden, up_full)
    ffn_back_low = matmul_nt(grad_hidden, up_second_flattened)
    back_here, back_low_here = scatter_rows((ffn_back_part, ffn_back_low))
    up_back_here = (back_low_here * select_here).astype(jnp.bfloat16)
    grad_second = back_here + matmul_nt(up_back_here, up_first_flattened)
    grad_middle_here = grad_top_here + second_back(grad_second)[0]
    grad_middle_low_here = grad_middle_here.astype(jnp.bfloat16)
    heads_back_here = (matmul_nt(grad_middle_low_here, heads_second_flattened) * select_here).astype(
        jnp.bfloat16
    )
    down_second_gradient = matmul_tn(down_low_here, tp_rows(grad_top_low, tp_count))
    grad_up_in = matmul_tn(second_act_here, up_back_here)
    heads_second_gradient = matmul_tn(heads_low_here, grad_middle_low_here)
    grad_heads_in_all = matmul_tn(heads_act_here, heads_back_here)
    hidden_terms = lax.psum(
        (
            up_second_gradient.reshape(adapter_up_second.shape),
            unflat_in(grad_down_in, adapter_tables),
        ),
        ("shard", "ctx"),
    )
    token_terms = lax.psum(
        (
            grad_heads_in_all,
            unflat_in(grad_up_in, adapter_tables),
            heads_second_gradient.reshape(adapter_heads_second.shape),
            down_second_gradient.reshape(adapter_down_second.shape),
        ),
        ("shard", "ctx", "tp"),
    )
    heads_in_rows = tp_rows(token_terms[0], tp_count)
    early_terms = (
        unflat_in(heads_in_rows, adapter_tables),
        token_terms[1],
        hidden_terms[0],
        hidden_terms[1],
        token_terms[3],
    )
    heads_second_total = token_terms[2]
    grad_heads_here = (
        matmul_nt(grad_middle_low_here, heads_full)
        + matmul_nt(heads_back_here, heads_first_all_flattened)
    ).astype(jnp.bfloat16)
    grad_heads = lax.all_to_all(grad_heads_here, "tp", 1, 0, tiled=True)
    grad_heads_wide = grad_heads.reshape(seq_here, local_len, device_heads, head_width).astype(
        jnp.float32
    )
    scaled_grad = (grad_heads_wide / per_total).astype(jnp.bfloat16)
    row_delta = jnp.sum(grad_heads_wide * heads_raw, axis=-1) / per_total[..., 0]
    grad_queries, grad_keyrows, grad_valrows = block_grads(
        queries,
        scaled_grad,
        row_delta,
        piece_keys,
        piece_values,
        here_pos,
        key_pos,
        visible_mask,
        slopes,
    )
    grad_kv = jnp.concatenate(
        [
            grad_keyrows.reshape(seq_here, ctx_count, local_len, local_width),
            grad_valrows.reshape(seq_here, ctx_count, local_len, local_width),
        ],
        axis=3,
    )
    grad_kv_here = grad_kv[:, 0]
    for offset in range(1, ctx_count):
        pairs = [(index, index ^ offset) for index in range(ctx_count)]
        grad_kv_here = grad_kv_here + lax.ppermute(
            grad_kv[:, offset].astype(jnp.bfloat16), "ctx", pairs
        ).astype(jnp.float32)
    grad_keys_all = grad_kv_here[:, :, :local_width]
    grad_values_all = grad_kv_here[:, :, local_width:]
    grad_projected = jnp.concatenate(
        [
            grad_queries.reshape(tok_rows, local_width),
            grad_keys_all.reshape(tok_rows, local_width),
            grad_values_all.reshape(tok_rows, local_width),
        ],
        axis=1,
    ).astype(jnp.bfloat16)
    projection_second_gradient = matmul_tn(first_low, grad_projected)
    attn_back_part = matmul_nt(grad_projected, qkv_full)
    attn_back_low = matmul_nt(grad_projected, projection_second_flattened)
    first_here, first_low_here = scatter_rows((attn_back_part, attn_back_low))
    select_late = lax.optimization_barrier(select_here)
    qkv_back_here = (first_low_here * select_late).astype(jnp.bfloat16)
    grad_first = first_here + matmul_nt(qkv_back_here, projection_first_flattened)
    input_here = (grad_middle_here + first_back_full(grad_first)[0]).astype(jnp.bfloat16)
    input_rows, qkv_back = gather_rows((input_here, qkv_back_here))
    input_grad = input_rows.reshape(layer_input.shape)
    grad_qkv_in = matmul_tn(first_act, qkv_back)
    early_terms, late_inputs = lax.optimization_barrier(
        (
            early_terms,
            (
                unflat_in(grad_qkv_in, adapter_tables),
                projection_second_gradient.reshape(adapter_projection_second.shape),
            ),
        )
    )
    late_terms = lax.psum(late_inputs, ("shard", "ctx"))
    return (
        layer_out,
        input_grad,
        late_terms[0],
        late_terms[1],
        early_terms[0],
        heads_second_total,
        early_terms[1],
        early_terms[2],
        early_terms[3],
        early_terms[4],
    )


def solution(mesh):
    placed = (
        P("shard", "ctx", None),
        P("shard", "ctx", None),
        P("shard", None),
        P("shard"),
        P(),
        P(),
        P(),
        P(),
        P("shard", None, "tp"),
        P("tp", "shard"),
        P("shard", "tp"),
        P("tp", "shard"),
        P(),
        P(None, None, None, "tp"),
        P(None, "tp", None),
        P(),
        P(),
        P(None, None, "tp"),
        P(None, "tp", None),
        P(),
    )
    return jax.shard_map(
        layer_body,
        mesh=mesh,
        in_specs=placed,
        out_specs=(
            P("shard", "ctx", None),
            P("shard", "ctx", None),
            P(),
            P(None, None, None, "tp"),
            P(None, "tp", None),
            P(),
            P(),
            P(None, None, "tp"),
            P(None, "tp", None),
            P(),
        ),
        check_vma=False,
    )
```

```python
import jax
import jax.numpy as jnp
from jax import lax
from jax.sharding import PartitionSpec as P

HD = 128
PIC = 256


NORM_EPS = 1e-05


def layer_norm(inputs, gains, biases):
    average = jnp.mean(inputs, axis=-1, keepdims=True)
    centred = inputs - average
    spread = jnp.mean(centred * centred, axis=-1, keepdims=True)
    return centred * lax.rsqrt(spread + NORM_EPS) * gains + biases


def gelu_tanh(inputs):
    return (
        0.5
        * inputs
        * (1.0 + jnp.tanh(0.7978845608028654 * (inputs + 0.044715 * inputs * inputs * inputs)))
    )


def flattened_first(adapter_mat):
    adapter_tables, inner_dim, rank_width = adapter_mat.shape
    return jnp.transpose(adapter_mat, (1, 0, 2)).reshape(inner_dim, adapter_tables * rank_width)


def flattened_second(adapter_mat):
    return adapter_mat.reshape(adapter_mat.shape[0] * adapter_mat.shape[1], -1)


def unflat_in(grad_flat, adapter_tables):
    inner_dim = grad_flat.shape[0]
    return jnp.transpose(grad_flat.reshape(inner_dim, adapter_tables, -1), (1, 0, 2))


def matmul(left_mat, right_mat):
    return jnp.dot(left_mat, right_mat, preferred_element_type=jnp.float32)


def matmul_tn(left_mat, right_mat):
    return lax.dot_general(
        left_mat, right_mat, (((0,), (0,)), ((), ())), preferred_element_type=jnp.float32
    )


def matmul_nt(left_mat, right_mat):
    return lax.dot_general(
        left_mat, right_mat, (((1,), (1,)), ((), ())), preferred_element_type=jnp.float32
    )


def piece_labels(starts, positions):
    inside = (positions[None, None, :] >= starts[:, :, None]) & (
        positions[None, None, :] < starts[:, :, None] + PIC
    )
    labels = jnp.arange(1, starts.shape[1] + 1, dtype=jnp.int32)
    return jnp.sum(jnp.where(inside, labels[None, :, None], 0), axis=1)


def visible(query_pos, key_pos, query_labels, key_labels):
    causal = key_pos[None, None, :] <= query_pos[None, :, None]
    shared = (query_labels[:, :, None] == key_labels[:, None, :]) & (query_labels[:, :, None] > 0)
    return causal | shared


def exponents(queries, key_rows, query_pos, key_pos, visible_mask, slopes):
    score_scale = queries.shape[-1] ** (-0.5)
    logits = (
        jnp.einsum("sqhd,skhd->shqk", queries, key_rows, preferred_element_type=jnp.float32)
        * score_scale
    )
    distance = jnp.abs(query_pos[:, None] - key_pos[None, :]).astype(jnp.float32)
    logits = logits - slopes[None, :, None, None] * distance[None, None]
    return jnp.where(visible_mask[:, None], jnp.exp(logits), 0.0)


def block_grads(
    queries, scaled_grad, row_delta, key_rows, value_rows, query_pos, key_pos, visible_mask, slopes
):
    score_scale = queries.shape[-1] ** (-0.5)
    exponent = exponents(queries, key_rows, query_pos, key_pos, visible_mask, slopes)
    products_gv = jnp.einsum(
        "sqhd,skhd->shqk", scaled_grad, value_rows, preferred_element_type=jnp.float32
    )
    grad_logits = (
        exponent * (products_gv - jnp.transpose(row_delta, (0, 2, 1))[..., None])
    ).astype(jnp.bfloat16)
    grad_queries = (
        jnp.einsum("shqk,skhd->sqhd", grad_logits, key_rows, preferred_element_type=jnp.float32)
        * score_scale
    )
    grad_keyrows = (
        jnp.einsum("shqk,sqhd->skhd", grad_logits, queries, preferred_element_type=jnp.float32)
        * score_scale
    )
    grad_valrows = jnp.einsum(
        "shqk,sqhd->skhd",
        exponent.astype(jnp.bfloat16),
        scaled_grad,
        preferred_element_type=jnp.float32,
    )
    return (grad_queries, grad_keyrows, grad_valrows)


def partner_swaps(block, axis_name, axis_count):
    received = [block]
    for offset in range(1, axis_count):
        pairs = [(index, index ^ offset) for index in range(axis_count)]
        received.append(lax.ppermute(block, axis_name, pairs))
    return received


def pair_gather(block, axis_name, axis):
    if lax.axis_size(axis_name) != 2:
        return lax.all_gather(block, axis_name, axis=axis, tiled=True)
    other = lax.ppermute(block, axis_name, [(0, 1), (1, 0)])
    first = lax.axis_index(axis_name) == 0
    low = jnp.where(first, block, other)
    high = jnp.where(first, other, block)
    return jnp.concatenate([low, high], axis=axis)


def butterfly_sum(values, axis_names):
    leaves, tree = jax.tree.flatten(values)
    packed = jnp.concatenate([leaf.reshape(-1) for leaf in leaves])
    for axis_name in axis_names:
        axis_count = lax.axis_size(axis_name)
        step = 1
        while step < axis_count:
            pairs = [(index, index ^ step) for index in range(axis_count)]
            packed = packed + lax.ppermute(packed, axis_name, pairs)
            step *= 2
    parts, offset = [], 0
    for leaf in leaves:
        parts.append(packed[offset : offset + leaf.size].reshape(leaf.shape))
        offset += leaf.size
    return jax.tree.unflatten(tree, parts)


def partner_gather_rows(rows_here, axis_name):
    axis_count = lax.axis_size(axis_name)
    blocks = jnp.stack(partner_swaps(rows_here, axis_name, axis_count))
    owners = jnp.bitwise_xor(
        lax.axis_index(axis_name), jnp.arange(axis_count, dtype=jnp.int32)
    )
    ordered = jnp.take(blocks, owners, axis=0)
    return ordered.reshape(axis_count * rows_here.shape[0], *rows_here.shape[1:])


def tp_rows(rows_array, tp_count):
    chunk = rows_array.shape[0] // tp_count
    return lax.dynamic_slice_in_dim(rows_array, lax.axis_index("tp") * chunk, chunk, axis=0)


def scatter_rows(partials):
    widths = [part.shape[1] for part in partials]
    joined = lax.psum_scatter(
        jnp.concatenate(partials, axis=1).astype(jnp.bfloat16),
        "tp",
        scatter_dimension=0,
        tiled=True,
    )
    return split_columns(joined.astype(jnp.float32), widths)


def gather_rows(rows_here):
    widths = [part.shape[1] for part in rows_here]
    joined = lax.all_gather(jnp.concatenate(rows_here, axis=1), "tp", axis=0, tiled=True)
    return split_columns(joined, widths)


def split_columns(joined, widths):
    parts, offset = [], 0
    for width in widths:
        parts.append(joined[:, offset : offset + width])
        offset += width
    return tuple(parts)


def layer_body(
    layer_input,
    output_gradient,
    picture_piece_starts,
    sequence_adapter_index,
    attention_norm_gain,
    attention_norm_bias,
    feedforward_norm_gain,
    feedforward_norm_bias,
    query_key_value_weight,
    attention_output_weight,
    up_projection_weight,
    down_projection_weight,
    adapter_projection_first,
    adapter_projection_second,
    adapter_heads_first,
    adapter_heads_second,
    adapter_up_first,
    adapter_up_second,
    adapter_down_first,
    adapter_down_second,
):
    seq_here, local_len, model_width = layer_input.shape
    tok_rows = seq_here * local_len
    tp_count = lax.axis_size("tp")
    adapter_tables = adapter_projection_first.shape[0]
    rank_width = adapter_projection_first.shape[2]
    head_width = HD
    device_heads = adapter_projection_second.shape[-1] // head_width
    local_width = device_heads * head_width
    columns = jnp.arange(adapter_tables * rank_width, dtype=jnp.int32) // rank_width
    chosen = (sequence_adapter_index[:, None] == columns[None, :]).astype(jnp.float32)
    select = jnp.broadcast_to(
        chosen[:, None, :], (seq_here, local_len, adapter_tables * rank_width)
    ).reshape(tok_rows, adapter_tables * rank_width)
    select_here = tp_rows(select, tp_count)
    head_ids = lax.axis_index("tp") * device_heads + jnp.arange(device_heads, dtype=jnp.int32)
    slopes = jnp.exp2(
        -8.0 * (head_ids.astype(jnp.float32) + 1.0) / (device_heads * tp_count)
    )
    here_pos = lax.axis_index("ctx") * local_len + jnp.arange(local_len, dtype=jnp.int32)
    here_labels = piece_labels(picture_piece_starts, here_pos)
    heads_first_local = flattened_first(adapter_heads_first)
    heads_pair = lax.all_gather(
        jnp.concatenate([attention_output_weight, heads_first_local], axis=1),
        "tp",
        axis=0,
        tiled=True,
    )
    out_cols = attention_output_weight.shape[1]
    heads_full = pair_gather(heads_pair[:, :out_cols], "shard", 1)
    heads_first_all_flattened = heads_pair[:, out_cols:]
    projection_first_flattened = flattened_first(adapter_projection_first)
    projection_second_flattened = flattened_second(adapter_projection_second)
    heads_first_flattened = flattened_first(adapter_heads_first)
    heads_second_flattened = flattened_second(adapter_heads_second)
    up_first_flattened = flattened_first(adapter_up_first)
    up_second_flattened = flattened_second(adapter_up_second)
    down_first_flattened = flattened_first(adapter_down_first)
    down_second_flattened = flattened_second(adapter_down_second)
    residual = layer_input.reshape(tok_rows, model_width).astype(jnp.float32)
    residual_here = tp_rows(residual, tp_count)
    first_norm = layer_norm(residual, attention_norm_gain, attention_norm_bias)
    first_act = first_norm.astype(jnp.bfloat16)
    _, first_back_full = jax.vjp(
        lambda inputs: layer_norm(inputs, attention_norm_gain, attention_norm_bias), residual_here
    )
    gathered_rows = (
        pair_gather(query_key_value_weight, "shard", 0),
        pair_gather(up_projection_weight, "shard", 0),
    )
    qkv_full = gathered_rows[0].reshape(model_width, 3 * local_width)
    up_full = gathered_rows[1]
    down_full = pair_gather(down_projection_weight, "shard", 1)
    first_low = (matmul(first_act, projection_first_flattened) * select).astype(jnp.bfloat16)
    projected = (
        matmul(first_act, qkv_full) + matmul(first_low, projection_second_flattened)
    ).astype(jnp.bfloat16)
    queries_flat = projected[:, :local_width].reshape(seq_here, local_len, local_width)
    queries = queries_flat.reshape(seq_here, local_len, device_heads, head_width)
    key_rows = projected[:, local_width : 2 * local_width].reshape(seq_here, local_len, local_width)
    value_rows = projected[:, 2 * local_width :].reshape(seq_here, local_len, local_width)
    ctx_count = lax.axis_size("ctx")
    ctx_here = lax.axis_index("ctx")
    blocks = partner_swaps(
        jnp.concatenate([key_rows, value_rows], axis=2), "ctx", ctx_count
    )
    pieces = jnp.concatenate(blocks, axis=1)
    piece_len = pieces.shape[1]
    key_pos = jnp.concatenate(
        [
            (ctx_here ^ offset) * local_len + jnp.arange(local_len, dtype=jnp.int32)
            for offset in range(ctx_count)
        ]
    )
    key_labels = piece_labels(picture_piece_starts, key_pos)
    visible_mask = visible(here_pos, key_pos, here_labels, key_labels)
    piece_keys = pieces[:, :, :local_width].reshape(seq_here, piece_len, device_heads, head_width)
    piece_values = pieces[:, :, local_width:].reshape(
        seq_here, piece_len, device_heads, head_width
    )
    exponent = exponents(queries, piece_keys, here_pos, key_pos, visible_mask, slopes)
    weighted = jnp.einsum(
        "shqk,skhd->sqhd",
        exponent.astype(jnp.bfloat16),
        piece_values,
        preferred_element_type=jnp.float32,
    )
    weighted, totals = (weighted, jnp.sum(exponent, axis=-1))
    per_total = jnp.transpose(totals, (0, 2, 1))[..., None]
    heads_raw = weighted / per_total
    heads_act = heads_raw.reshape(tok_rows, local_width).astype(jnp.bfloat16)
    heads_act_here = lax.all_to_all(heads_act, "tp", 0, 1, tiled=True)
    attn_here = matmul(heads_act_here, heads_full)
    heads_low_here = (matmul(heads_act_here, heads_first_all_flattened) * select_here).astype(
        jnp.bfloat16
    )
    middle_here = residual_here + attn_here + matmul(heads_low_here, heads_second_flattened)
    second_norm, second_back = jax.vjp(
        lambda inputs: layer_norm(inputs, feedforward_norm_gain, feedforward_norm_bias), middle_here
    )
    second_act_here = second_norm.astype(jnp.bfloat16)
    (second_act,) = gather_rows((second_act_here,))
    up_low = (matmul(second_act, up_first_flattened) * select).astype(jnp.bfloat16)
    hidden = matmul(second_act, up_full) + matmul(up_low, up_second_flattened)
    activated, gelu_back = jax.vjp(gelu_tanh, hidden)
    activated = activated.astype(jnp.bfloat16)
    down_part = matmul(activated, down_full)
    down_low_part = matmul(activated, down_first_flattened)
    ffn_here, ffn_low_here = scatter_rows((down_part, down_low_part))
    down_low_here = (ffn_low_here * select_here).astype(jnp.bfloat16)
    result_here = (middle_here + ffn_here + matmul(down_low_here, down_second_flattened)).astype(
        jnp.bfloat16
    )
    (result_rows,) = gather_rows((result_here,))
    layer_out = result_rows.reshape(layer_input.shape)
    grad_top_low = output_gradient.reshape(tok_rows, model_width)
    grad_top_here = tp_rows(grad_top_low, tp_count).astype(jnp.float32)
    down_back = (matmul_nt(grad_top_low, down_second_flattened) * select).astype(jnp.bfloat16)
    grad_down_in = matmul_tn(activated, down_back)
    grad_activated = matmul_nt(grad_top_low, down_full) + matmul_nt(down_back, down_first_flattened)
    grad_hidden = gelu_back(grad_activated)[0].astype(jnp.bfloat16)
    up_second_gradient = matmul_tn(up_low, grad_hidden)
    ffn_back_part = matmul_nt(grad_hidden, up_full)
    ffn_back_low = matmul_nt(grad_hidden, up_second_flattened)
    back_here, back_low_here = scatter_rows((ffn_back_part, ffn_back_low))
    up_back_here = (back_low_here * select_here).astype(jnp.bfloat16)
    grad_second = back_here + matmul_nt(up_back_here, up_first_flattened)
    grad_middle_here = grad_top_here + second_back(grad_second)[0]
    grad_middle_low_here = grad_middle_here.astype(jnp.bfloat16)
    heads_back_here = (matmul_nt(grad_middle_low_here, heads_second_flattened) * select_here).astype(
        jnp.bfloat16
    )
    low_rows = partner_gather_rows(
        jnp.concatenate([down_low_here, up_back_here, heads_back_here], axis=1), "tp"
    )
    down_low, up_back, heads_back = split_columns(low_rows, [rank_width * adapter_tables] * 3)
    down_second_gradient = matmul_tn(down_low, grad_top_low)
    grad_up_in = matmul_tn(second_act, up_back)
    grad_heads_in = matmul_tn(heads_act, heads_back)
    heads_second_gradient = matmul_tn(heads_low_here, grad_middle_low_here)
    early_terms = butterfly_sum(
        (
            unflat_in(grad_heads_in, adapter_tables),
            unflat_in(grad_up_in, adapter_tables),
            up_second_gradient.reshape(adapter_up_second.shape),
            unflat_in(grad_down_in, adapter_tables),
            down_second_gradient.reshape(adapter_down_second.shape),
            butterfly_sum(heads_second_gradient, ("tp",)).reshape(
                adapter_heads_second.shape
            ),
        ),
        ("shard", "ctx"),
    )
    heads_second_total = early_terms[5]
    grad_heads_here = (
        matmul_nt(grad_middle_low_here, heads_full)
        + matmul_nt(heads_back_here, heads_first_all_flattened)
    ).astype(jnp.bfloat16)
    grad_heads = lax.all_to_all(grad_heads_here, "tp", 1, 0, tiled=True)
    grad_heads_wide = grad_heads.reshape(seq_here, local_len, device_heads, head_width).astype(
        jnp.float32
    )
    scaled_grad = (grad_heads_wide / per_total).astype(jnp.bfloat16)
    row_delta = jnp.sum(grad_heads_wide * heads_raw, axis=-1) / per_total[..., 0]
    grad_queries, grad_keyrows, grad_valrows = block_grads(
        queries,
        scaled_grad,
        row_delta,
        piece_keys,
        piece_values,
        here_pos,
        key_pos,
        visible_mask,
        slopes,
    )
    grad_kv = jnp.concatenate(
        [
            grad_keyrows.reshape(seq_here, ctx_count, local_len, local_width),
            grad_valrows.reshape(seq_here, ctx_count, local_len, local_width),
        ],
        axis=3,
    )
    grad_kv_here = grad_kv[:, 0]
    for offset in range(1, ctx_count):
        pairs = [(index, index ^ offset) for index in range(ctx_count)]
        grad_kv_here = grad_kv_here + lax.ppermute(
            grad_kv[:, offset].astype(jnp.bfloat16), "ctx", pairs
        ).astype(jnp.float32)
    grad_keys_all = grad_kv_here[:, :, :local_width]
    grad_values_all = grad_kv_here[:, :, local_width:]
    grad_projected = jnp.concatenate(
        [
            grad_queries.reshape(tok_rows, local_width),
            grad_keys_all.reshape(tok_rows, local_width),
            grad_values_all.reshape(tok_rows, local_width),
        ],
        axis=1,
    ).astype(jnp.bfloat16)
    projection_second_gradient = matmul_tn(first_low, grad_projected)
    attn_back_part = matmul_nt(grad_projected, qkv_full)
    attn_back_low = matmul_nt(grad_projected, projection_second_flattened)
    first_here, first_low_here = scatter_rows((attn_back_part, attn_back_low))
    select_late = lax.optimization_barrier(select_here)
    qkv_back_here = (first_low_here * select_late).astype(jnp.bfloat16)
    grad_first = first_here + matmul_nt(qkv_back_here, projection_first_flattened)
    input_here = (grad_middle_here + first_back_full(grad_first)[0]).astype(jnp.bfloat16)
    qkv_back = partner_gather_rows(qkv_back_here, "tp")
    (input_rows,) = gather_rows((input_here,))
    input_grad = input_rows.reshape(layer_input.shape)
    grad_qkv_in = matmul_tn(first_act, qkv_back)
    early_terms, late_inputs = lax.optimization_barrier(
        (
            early_terms,
            (
                unflat_in(grad_qkv_in, adapter_tables),
                projection_second_gradient.reshape(adapter_projection_second.shape),
            ),
        )
    )
    late_terms = butterfly_sum(late_inputs, ("shard", "ctx"))
    return (
        layer_out,
        input_grad,
        late_terms[0],
        late_terms[1],
        early_terms[0],
        heads_second_total,
        early_terms[1],
        early_terms[2],
        early_terms[3],
        early_terms[4],
    )


def solution(mesh):
    placed = (
        P("shard", "ctx", None),
        P("shard", "ctx", None),
        P("shard", None),
        P("shard"),
        P(),
        P(),
        P(),
        P(),
        P("shard", None, "tp"),
        P("tp", "shard"),
        P("shard", "tp"),
        P("tp", "shard"),
        P(),
        P(None, None, None, "tp"),
        P(None, "tp", None),
        P(),
        P(),
        P(None, None, "tp"),
        P(None, "tp", None),
        P(),
    )
    return jax.shard_map(
        layer_body,
        mesh=mesh,
        in_specs=placed,
        out_specs=(
            P("shard", "ctx", None),
            P("shard", "ctx", None),
            P(),
            P(None, None, None, "tp"),
            P(None, "tp", None),
            P(),
            P(),
            P(None, None, "tp"),
            P(None, "tp", None),
            P(),
        ),
        check_vma=False,
    )
```

```python
import jax
import jax.numpy as jnp
from jax import lax
from jax.sharding import PartitionSpec as P

HD = 128
PIC = 256


NORM_EPS = 1e-05


def layer_norm(inputs, gains, biases):
    average = jnp.mean(inputs, axis=-1, keepdims=True)
    centred = inputs - average
    spread = jnp.mean(centred * centred, axis=-1, keepdims=True)
    return centred * lax.rsqrt(spread + NORM_EPS) * gains + biases


def gelu_tanh(inputs):
    return (
        0.5
        * inputs
        * (1.0 + jnp.tanh(0.7978845608028654 * (inputs + 0.044715 * inputs * inputs * inputs)))
    )


def flattened_first(adapter_mat):
    adapter_tables, inner_dim, rank_width = adapter_mat.shape
    return jnp.transpose(adapter_mat, (1, 0, 2)).reshape(inner_dim, adapter_tables * rank_width)


def flattened_second(adapter_mat):
    return adapter_mat.reshape(adapter_mat.shape[0] * adapter_mat.shape[1], -1)


def unflat_in(grad_flat, adapter_tables):
    inner_dim = grad_flat.shape[0]
    return jnp.transpose(grad_flat.reshape(inner_dim, adapter_tables, -1), (1, 0, 2))


def matmul(left_mat, right_mat):
    return jnp.dot(left_mat, right_mat, preferred_element_type=jnp.float32)


def matmul_tn(left_mat, right_mat):
    return lax.dot_general(
        left_mat, right_mat, (((0,), (0,)), ((), ())), preferred_element_type=jnp.float32
    )


def matmul_nt(left_mat, right_mat):
    return lax.dot_general(
        left_mat, right_mat, (((1,), (1,)), ((), ())), preferred_element_type=jnp.float32
    )


def piece_labels(starts, positions):
    inside = (positions[None, None, :] >= starts[:, :, None]) & (
        positions[None, None, :] < starts[:, :, None] + PIC
    )
    labels = jnp.arange(1, starts.shape[1] + 1, dtype=jnp.int32)
    return jnp.sum(jnp.where(inside, labels[None, :, None], 0), axis=1)


def visible(query_pos, key_pos, query_labels, key_labels):
    causal = key_pos[None, None, :] <= query_pos[None, :, None]
    shared = (query_labels[:, :, None] == key_labels[:, None, :]) & (query_labels[:, :, None] > 0)
    return causal | shared


def exponents(queries, key_rows, query_pos, key_pos, visible_mask, slopes):
    score_scale = queries.shape[-1] ** (-0.5)
    logits = (
        jnp.einsum("sqhd,skhd->shqk", queries, key_rows, preferred_element_type=jnp.float32)
        * score_scale
    )
    distance = jnp.abs(query_pos[:, None] - key_pos[None, :]).astype(jnp.float32)
    logits = logits - slopes[None, :, None, None] * distance[None, None]
    return jnp.where(visible_mask[:, None], jnp.exp(logits), 0.0)


def block_grads(
    queries, scaled_grad, row_delta, key_rows, value_rows, query_pos, key_pos, visible_mask, slopes
):
    score_scale = queries.shape[-1] ** (-0.5)
    exponent = exponents(queries, key_rows, query_pos, key_pos, visible_mask, slopes)
    products_gv = jnp.einsum(
        "sqhd,skhd->shqk", scaled_grad, value_rows, preferred_element_type=jnp.float32
    )
    grad_logits = (
        exponent * (products_gv - jnp.transpose(row_delta, (0, 2, 1))[..., None])
    ).astype(jnp.bfloat16)
    grad_queries = (
        jnp.einsum("shqk,skhd->sqhd", grad_logits, key_rows, preferred_element_type=jnp.float32)
        * score_scale
    )
    grad_keyrows = (
        jnp.einsum("shqk,sqhd->skhd", grad_logits, queries, preferred_element_type=jnp.float32)
        * score_scale
    )
    grad_valrows = jnp.einsum(
        "shqk,sqhd->skhd",
        exponent.astype(jnp.bfloat16),
        scaled_grad,
        preferred_element_type=jnp.float32,
    )
    return (grad_queries, grad_keyrows, grad_valrows)


def partner_swaps(block, axis_name, axis_count):
    received = [block]
    for offset in range(1, axis_count):
        pairs = [(index, index ^ offset) for index in range(axis_count)]
        received.append(lax.ppermute(block, axis_name, pairs))
    return received


def pair_gather(block, axis_name, axis):
    if lax.axis_size(axis_name) != 2:
        return lax.all_gather(block, axis_name, axis=axis, tiled=True)
    other = lax.ppermute(block, axis_name, [(0, 1), (1, 0)])
    first = lax.axis_index(axis_name) == 0
    low = jnp.where(first, block, other)
    high = jnp.where(first, other, block)
    return jnp.concatenate([low, high], axis=axis)


def butterfly_sum(values, axis_names):
    leaves, tree = jax.tree.flatten(values)
    packed = jnp.concatenate([leaf.reshape(-1) for leaf in leaves])
    for axis_name in axis_names:
        axis_count = lax.axis_size(axis_name)
        step = 1
        while step < axis_count:
            pairs = [(index, index ^ step) for index in range(axis_count)]
            packed = packed + lax.ppermute(packed, axis_name, pairs)
            step *= 2
    parts, offset = [], 0
    for leaf in leaves:
        parts.append(packed[offset : offset + leaf.size].reshape(leaf.shape))
        offset += leaf.size
    return jax.tree.unflatten(tree, parts)


def partner_gather_rows(rows_here, axis_name):
    axis_count = lax.axis_size(axis_name)
    blocks = jnp.stack(partner_swaps(rows_here, axis_name, axis_count))
    owners = jnp.bitwise_xor(
        lax.axis_index(axis_name), jnp.arange(axis_count, dtype=jnp.int32)
    )
    ordered = jnp.take(blocks, owners, axis=0)
    return ordered.reshape(axis_count * rows_here.shape[0], *rows_here.shape[1:])


def tp_rows(rows_array, tp_count):
    chunk = rows_array.shape[0] // tp_count
    return lax.dynamic_slice_in_dim(rows_array, lax.axis_index("tp") * chunk, chunk, axis=0)


def scatter_rows(partials):
    widths = [part.shape[1] for part in partials]
    joined = lax.psum_scatter(
        jnp.concatenate(partials, axis=1).astype(jnp.bfloat16),
        "tp",
        scatter_dimension=0,
        tiled=True,
    )
    return split_columns(joined.astype(jnp.float32), widths)


def gather_rows(rows_here):
    widths = [part.shape[1] for part in rows_here]
    joined = lax.all_gather(jnp.concatenate(rows_here, axis=1), "tp", axis=0, tiled=True)
    return split_columns(joined, widths)


def split_columns(joined, widths):
    parts, offset = [], 0
    for width in widths:
        parts.append(joined[:, offset : offset + width])
        offset += width
    return tuple(parts)


def layer_body(
    layer_input,
    output_gradient,
    picture_piece_starts,
    sequence_adapter_index,
    attention_norm_gain,
    attention_norm_bias,
    feedforward_norm_gain,
    feedforward_norm_bias,
    query_key_value_weight,
    attention_output_weight,
    up_projection_weight,
    down_projection_weight,
    adapter_projection_first,
    adapter_projection_second,
    adapter_heads_first,
    adapter_heads_second,
    adapter_up_first,
    adapter_up_second,
    adapter_down_first,
    adapter_down_second,
):
    seq_here, local_len, model_width = layer_input.shape
    tok_rows = seq_here * local_len
    tp_count = lax.axis_size("tp")
    adapter_tables = adapter_projection_first.shape[0]
    rank_width = adapter_projection_first.shape[2]
    head_width = HD
    device_heads = adapter_projection_second.shape[-1] // head_width
    local_width = device_heads * head_width
    columns = jnp.arange(adapter_tables * rank_width, dtype=jnp.int32) // rank_width
    chosen = (sequence_adapter_index[:, None] == columns[None, :]).astype(jnp.float32)
    select = jnp.broadcast_to(
        chosen[:, None, :], (seq_here, local_len, adapter_tables * rank_width)
    ).reshape(tok_rows, adapter_tables * rank_width)
    select_here = tp_rows(select, tp_count)
    head_ids = lax.axis_index("tp") * device_heads + jnp.arange(device_heads, dtype=jnp.int32)
    slopes = jnp.exp2(
        -8.0 * (head_ids.astype(jnp.float32) + 1.0) / (device_heads * tp_count)
    )
    here_pos = lax.axis_index("ctx") * local_len + jnp.arange(local_len, dtype=jnp.int32)
    here_labels = piece_labels(picture_piece_starts, here_pos)
    heads_first_local = flattened_first(adapter_heads_first)
    heads_pair = lax.all_gather(
        jnp.concatenate([attention_output_weight, heads_first_local], axis=1),
        "tp",
        axis=0,
        tiled=True,
    )
    out_cols = attention_output_weight.shape[1]
    heads_full = pair_gather(heads_pair[:, :out_cols], "shard", 1)
    heads_first_all_flattened = heads_pair[:, out_cols:]
    projection_first_flattened = flattened_first(adapter_projection_first)
    projection_second_flattened = flattened_second(adapter_projection_second)
    heads_first_flattened = flattened_first(adapter_heads_first)
    heads_second_flattened = flattened_second(adapter_heads_second)
    up_first_flattened = flattened_first(adapter_up_first)
    up_second_flattened = flattened_second(adapter_up_second)
    down_first_flattened = flattened_first(adapter_down_first)
    down_second_flattened = flattened_second(adapter_down_second)
    residual = layer_input.reshape(tok_rows, model_width).astype(jnp.float32)
    residual_here = tp_rows(residual, tp_count)
    first_norm = layer_norm(residual, attention_norm_gain, attention_norm_bias)
    first_act = first_norm.astype(jnp.bfloat16)
    _, first_back_full = jax.vjp(
        lambda inputs: layer_norm(inputs, attention_norm_gain, attention_norm_bias), residual_here
    )
    gathered_rows = (
        pair_gather(query_key_value_weight, "shard", 0),
        pair_gather(up_projection_weight, "shard", 0),
    )
    qkv_full = gathered_rows[0].reshape(model_width, 3 * local_width)
    up_full = gathered_rows[1]
    down_full = pair_gather(down_projection_weight, "shard", 1)
    first_low = (matmul(first_act, projection_first_flattened) * select).astype(jnp.bfloat16)
    projected = (
        matmul(first_act, qkv_full) + matmul(first_low, projection_second_flattened)
    ).astype(jnp.bfloat16)
    queries_flat = projected[:, :local_width].reshape(seq_here, local_len, local_width)
    queries = queries_flat.reshape(seq_here, local_len, device_heads, head_width)
    key_rows = projected[:, local_width : 2 * local_width].reshape(seq_here, local_len, local_width)
    value_rows = projected[:, 2 * local_width :].reshape(seq_here, local_len, local_width)
    ctx_count = lax.axis_size("ctx")
    ctx_here = lax.axis_index("ctx")
    blocks = partner_swaps(
        jnp.concatenate([key_rows, value_rows], axis=2), "ctx", ctx_count
    )
    pieces = jnp.concatenate(blocks, axis=1)
    piece_len = pieces.shape[1]
    key_pos = jnp.concatenate(
        [
            (ctx_here ^ offset) * local_len + jnp.arange(local_len, dtype=jnp.int32)
            for offset in range(ctx_count)
        ]
    )
    key_labels = piece_labels(picture_piece_starts, key_pos)
    visible_mask = visible(here_pos, key_pos, here_labels, key_labels)
    piece_keys = pieces[:, :, :local_width].reshape(seq_here, piece_len, device_heads, head_width)
    piece_values = pieces[:, :, local_width:].reshape(
        seq_here, piece_len, device_heads, head_width
    )
    exponent = exponents(queries, piece_keys, here_pos, key_pos, visible_mask, slopes)
    weighted = jnp.einsum(
        "shqk,skhd->sqhd",
        exponent.astype(jnp.bfloat16),
        piece_values,
        preferred_element_type=jnp.float32,
    )
    weighted, totals = (weighted, jnp.sum(exponent, axis=-1))
    per_total = jnp.transpose(totals, (0, 2, 1))[..., None]
    heads_raw = weighted / per_total
    heads_act = heads_raw.reshape(tok_rows, local_width).astype(jnp.bfloat16)
    heads_act_here = lax.all_to_all(heads_act, "tp", 0, 1, tiled=True)
    attn_here = matmul(heads_act_here, heads_full)
    heads_low_here = (matmul(heads_act_here, heads_first_all_flattened) * select_here).astype(
        jnp.bfloat16
    )
    middle_here = residual_here + attn_here + matmul(heads_low_here, heads_second_flattened)
    second_norm, second_back = jax.vjp(
        lambda inputs: layer_norm(inputs, feedforward_norm_gain, feedforward_norm_bias), middle_here
    )
    second_act_here = second_norm.astype(jnp.bfloat16)
    (second_act,) = gather_rows((second_act_here,))
    up_low = (matmul(second_act, up_first_flattened) * select).astype(jnp.bfloat16)
    hidden = matmul(second_act, up_full) + matmul(up_low, up_second_flattened)
    activated, gelu_back = jax.vjp(gelu_tanh, hidden)
    activated = activated.astype(jnp.bfloat16)
    down_part = matmul(activated, down_full)
    down_low_part = matmul(activated, down_first_flattened)
    ffn_here, ffn_low_here = scatter_rows((down_part, down_low_part))
    down_low_here = (ffn_low_here * select_here).astype(jnp.bfloat16)
    result_here = (middle_here + ffn_here + matmul(down_low_here, down_second_flattened)).astype(
        jnp.bfloat16
    )
    (result_rows,) = gather_rows((result_here,))
    layer_out = result_rows.reshape(layer_input.shape)
    grad_top_low = output_gradient.reshape(tok_rows, model_width)
    grad_top_here = tp_rows(grad_top_low, tp_count).astype(jnp.float32)
    down_back = (matmul_nt(grad_top_low, down_second_flattened) * select).astype(jnp.bfloat16)
    grad_down_in = matmul_tn(activated, down_back)
    grad_activated = matmul_nt(grad_top_low, down_full) + matmul_nt(down_back, down_first_flattened)
    grad_hidden = gelu_back(grad_activated)[0].astype(jnp.bfloat16)
    up_second_gradient = matmul_tn(up_low, grad_hidden)
    ffn_back_part = matmul_nt(grad_hidden, up_full)
    ffn_back_low = matmul_nt(grad_hidden, up_second_flattened)
    back_here, back_low_here = scatter_rows((ffn_back_part, ffn_back_low))
    up_back_here = (back_low_here * select_here).astype(jnp.bfloat16)
    grad_second = back_here + matmul_nt(up_back_here, up_first_flattened)
    grad_middle_here = grad_top_here + second_back(grad_second)[0]
    grad_middle_low_here = grad_middle_here.astype(jnp.bfloat16)
    heads_back_here = (matmul_nt(grad_middle_low_here, heads_second_flattened) * select_here).astype(
        jnp.bfloat16
    )
    low_rows = partner_gather_rows(
        jnp.concatenate([down_low_here, up_back_here, heads_back_here], axis=1), "tp"
    )
    down_low, up_back, heads_back = split_columns(low_rows, [rank_width * adapter_tables] * 3)
    down_second_gradient = matmul_tn(down_low, grad_top_low)
    grad_up_in = matmul_tn(second_act, up_back)
    grad_heads_in = matmul_tn(heads_act, heads_back)
    heads_second_gradient = matmul_tn(heads_low_here, grad_middle_low_here)
    early_terms = lax.psum(
        (
            unflat_in(grad_heads_in, adapter_tables),
            unflat_in(grad_up_in, adapter_tables),
            up_second_gradient.reshape(adapter_up_second.shape),
            unflat_in(grad_down_in, adapter_tables),
            down_second_gradient.reshape(adapter_down_second.shape),
        ),
        ("shard", "ctx"),
    )
    heads_second_total = lax.psum(
        heads_second_gradient.reshape(adapter_heads_second.shape), ("shard", "ctx", "tp")
    )
    grad_heads_here = (
        matmul_nt(grad_middle_low_here, heads_full)
        + matmul_nt(heads_back_here, heads_first_all_flattened)
    ).astype(jnp.bfloat16)
    grad_heads = lax.all_to_all(grad_heads_here, "tp", 1, 0, tiled=True)
    grad_heads_wide = grad_heads.reshape(seq_here, local_len, device_heads, head_width).astype(
        jnp.float32
    )
    scaled_grad = (grad_heads_wide / per_total).astype(jnp.bfloat16)
    row_delta = jnp.sum(grad_heads_wide * heads_raw, axis=-1) / per_total[..., 0]
    grad_queries, grad_keyrows, grad_valrows = block_grads(
        queries,
        scaled_grad,
        row_delta,
        piece_keys,
        piece_values,
        here_pos,
        key_pos,
        visible_mask,
        slopes,
    )
    grad_kv = jnp.concatenate(
        [
            grad_keyrows.reshape(seq_here, ctx_count, local_len, local_width),
            grad_valrows.reshape(seq_here, ctx_count, local_len, local_width),
        ],
        axis=3,
    )
    grad_kv_here = grad_kv[:, 0]
    for offset in range(1, ctx_count):
        pairs = [(index, index ^ offset) for index in range(ctx_count)]
        grad_kv_here = grad_kv_here + lax.ppermute(
            grad_kv[:, offset].astype(jnp.bfloat16), "ctx", pairs
        ).astype(jnp.float32)
    grad_keys_all = grad_kv_here[:, :, :local_width]
    grad_values_all = grad_kv_here[:, :, local_width:]
    grad_projected = jnp.concatenate(
        [
            grad_queries.reshape(tok_rows, local_width),
            grad_keys_all.reshape(tok_rows, local_width),
            grad_values_all.reshape(tok_rows, local_width),
        ],
        axis=1,
    ).astype(jnp.bfloat16)
    projection_second_gradient = matmul_tn(first_low, grad_projected)
    attn_back_part = matmul_nt(grad_projected, qkv_full)
    attn_back_low = matmul_nt(grad_projected, projection_second_flattened)
    low_blocks = jnp.stack(partner_swaps(attn_back_low, "tp", tp_count))
    low_owners = jnp.bitwise_xor(lax.axis_index("tp"), jnp.arange(tp_count, dtype=jnp.int32))
    low_total = jnp.sum(jnp.take(low_blocks, low_owners, axis=0), axis=0)
    select_late = lax.optimization_barrier(select)
    qkv_back = (low_total * select_late).astype(jnp.bfloat16)
    grad_qkv_in = matmul_tn(first_act, qkv_back)
    late_terms = butterfly_sum(
        (
            unflat_in(grad_qkv_in, adapter_tables),
            projection_second_gradient.reshape(adapter_projection_second.shape),
        ),
        ("shard", "ctx"),
    )
    first_here, first_low_here = scatter_rows((attn_back_part, attn_back_low))
    select_later = lax.optimization_barrier(select_here)
    qkv_back_here = (first_low_here * select_later).astype(jnp.bfloat16)
    grad_first = first_here + matmul_nt(qkv_back_here, projection_first_flattened)
    input_here = (grad_middle_here + first_back_full(grad_first)[0]).astype(jnp.bfloat16)
    (input_rows,) = gather_rows((input_here,))
    input_grad = input_rows.reshape(layer_input.shape)
    return (
        layer_out,
        input_grad,
        late_terms[0],
        late_terms[1],
        early_terms[0],
        heads_second_total,
        early_terms[1],
        early_terms[2],
        early_terms[3],
        early_terms[4],
    )


def solution(mesh):
    placed = (
        P("shard", "ctx", None),
        P("shard", "ctx", None),
        P("shard", None),
        P("shard"),
        P(),
        P(),
        P(),
        P(),
        P("shard", None, "tp"),
        P("tp", "shard"),
        P("shard", "tp"),
        P("tp", "shard"),
        P(),
        P(None, None, None, "tp"),
        P(None, "tp", None),
        P(),
        P(),
        P(None, None, "tp"),
        P(None, "tp", None),
        P(),
    )
    return jax.shard_map(
        layer_body,
        mesh=mesh,
        in_specs=placed,
        out_specs=(
            P("shard", "ctx", None),
            P("shard", "ctx", None),
            P(),
            P(None, None, None, "tp"),
            P(None, "tp", None),
            P(),
            P(),
            P(None, None, "tp"),
            P(None, "tp", None),
            P(),
        ),
        check_vma=False,
    )
```

```python
import jax
import jax.numpy as jnp
from jax import lax
from jax.sharding import PartitionSpec as P

HD = 128
PIC = 256


NORM_EPS = 1e-05


def layer_norm(inputs, gains, biases):
    average = jnp.mean(inputs, axis=-1, keepdims=True)
    centred = inputs - average
    spread = jnp.mean(centred * centred, axis=-1, keepdims=True)
    return centred * lax.rsqrt(spread + NORM_EPS) * gains + biases


def gelu_tanh(inputs):
    return (
        0.5
        * inputs
        * (1.0 + jnp.tanh(0.7978845608028654 * (inputs + 0.044715 * inputs * inputs * inputs)))
    )


def flattened_first(adapter_mat):
    adapter_tables, inner_dim, rank_width = adapter_mat.shape
    return jnp.transpose(adapter_mat, (1, 0, 2)).reshape(inner_dim, adapter_tables * rank_width)


def flattened_second(adapter_mat):
    return adapter_mat.reshape(adapter_mat.shape[0] * adapter_mat.shape[1], -1)


def unflat_in(grad_flat, adapter_tables):
    inner_dim = grad_flat.shape[0]
    return jnp.transpose(grad_flat.reshape(inner_dim, adapter_tables, -1), (1, 0, 2))


def matmul(left_mat, right_mat):
    return jnp.dot(left_mat, right_mat, preferred_element_type=jnp.float32)


def matmul_tn(left_mat, right_mat):
    return lax.dot_general(
        left_mat, right_mat, (((0,), (0,)), ((), ())), preferred_element_type=jnp.float32
    )


def matmul_nt(left_mat, right_mat):
    return lax.dot_general(
        left_mat, right_mat, (((1,), (1,)), ((), ())), preferred_element_type=jnp.float32
    )


def piece_labels(starts, positions):
    inside = (positions[None, None, :] >= starts[:, :, None]) & (
        positions[None, None, :] < starts[:, :, None] + PIC
    )
    labels = jnp.arange(1, starts.shape[1] + 1, dtype=jnp.int32)
    return jnp.sum(jnp.where(inside, labels[None, :, None], 0), axis=1)


def visible(query_pos, key_pos, query_labels, key_labels):
    causal = key_pos[None, None, :] <= query_pos[None, :, None]
    shared = (query_labels[:, :, None] == key_labels[:, None, :]) & (query_labels[:, :, None] > 0)
    return causal | shared


def exponents(queries, key_rows, query_pos, key_pos, visible_mask, slopes):
    score_scale = queries.shape[-1] ** (-0.5)
    logits = (
        jnp.einsum("sqhd,skhd->shqk", queries, key_rows, preferred_element_type=jnp.float32)
        * score_scale
    )
    distance = jnp.abs(query_pos[:, None] - key_pos[None, :]).astype(jnp.float32)
    logits = logits - slopes[None, :, None, None] * distance[None, None]
    return jnp.where(visible_mask[:, None], jnp.exp(logits), 0.0)


def block_grads(
    queries, scaled_grad, row_delta, key_rows, value_rows, query_pos, key_pos, visible_mask, slopes
):
    score_scale = queries.shape[-1] ** (-0.5)
    exponent = exponents(queries, key_rows, query_pos, key_pos, visible_mask, slopes)
    products_gv = jnp.einsum(
        "sqhd,skhd->shqk", scaled_grad, value_rows, preferred_element_type=jnp.float32
    )
    grad_logits = (
        exponent * (products_gv - jnp.transpose(row_delta, (0, 2, 1))[..., None])
    ).astype(jnp.bfloat16)
    grad_queries = (
        jnp.einsum("shqk,skhd->sqhd", grad_logits, key_rows, preferred_element_type=jnp.float32)
        * score_scale
    )
    grad_keyrows = (
        jnp.einsum("shqk,sqhd->skhd", grad_logits, queries, preferred_element_type=jnp.float32)
        * score_scale
    )
    grad_valrows = jnp.einsum(
        "shqk,sqhd->skhd",
        exponent.astype(jnp.bfloat16),
        scaled_grad,
        preferred_element_type=jnp.float32,
    )
    return (grad_queries, grad_keyrows, grad_valrows)


def partner_swaps(block, axis_name, axis_count):
    received = [block]
    for offset in range(1, axis_count):
        pairs = [(index, index ^ offset) for index in range(axis_count)]
        received.append(lax.ppermute(block, axis_name, pairs))
    return received


def pair_gather(block, axis_name, axis):
    if lax.axis_size(axis_name) != 2:
        return lax.all_gather(block, axis_name, axis=axis, tiled=True)
    other = lax.ppermute(block, axis_name, [(0, 1), (1, 0)])
    first = lax.axis_index(axis_name) == 0
    low = jnp.where(first, block, other)
    high = jnp.where(first, other, block)
    return jnp.concatenate([low, high], axis=axis)


def butterfly_sum(values, axis_names):
    leaves, tree = jax.tree.flatten(values)
    packed = jnp.concatenate([leaf.reshape(-1) for leaf in leaves])
    for axis_name in axis_names:
        axis_count = lax.axis_size(axis_name)
        step = 1
        while step < axis_count:
            pairs = [(index, index ^ step) for index in range(axis_count)]
            packed = packed + lax.ppermute(packed, axis_name, pairs)
            step *= 2
    parts, offset = [], 0
    for leaf in leaves:
        parts.append(packed[offset : offset + leaf.size].reshape(leaf.shape))
        offset += leaf.size
    return jax.tree.unflatten(tree, parts)


def partner_gather_rows(rows_here, axis_name):
    axis_count = lax.axis_size(axis_name)
    blocks = jnp.stack(partner_swaps(rows_here, axis_name, axis_count))
    owners = jnp.bitwise_xor(
        lax.axis_index(axis_name), jnp.arange(axis_count, dtype=jnp.int32)
    )
    ordered = jnp.take(blocks, owners, axis=0)
    return ordered.reshape(axis_count * rows_here.shape[0], *rows_here.shape[1:])


def narrow_psum(values, axis_names):
    summed = lax.psum(jax.tree.map(lambda value: value.astype(jnp.bfloat16), values), axis_names)
    return jax.tree.map(lambda value: value.astype(jnp.float32), summed)


def tp_rows(rows_array, tp_count):
    chunk = rows_array.shape[0] // tp_count
    return lax.dynamic_slice_in_dim(rows_array, lax.axis_index("tp") * chunk, chunk, axis=0)


def scatter_rows(partials):
    widths = [part.shape[1] for part in partials]
    joined = lax.psum_scatter(
        jnp.concatenate(partials, axis=1).astype(jnp.bfloat16),
        "tp",
        scatter_dimension=0,
        tiled=True,
    )
    return split_columns(joined.astype(jnp.float32), widths)


def gather_rows(rows_here):
    widths = [part.shape[1] for part in rows_here]
    joined = lax.all_gather(jnp.concatenate(rows_here, axis=1), "tp", axis=0, tiled=True)
    return split_columns(joined, widths)


def split_columns(joined, widths):
    parts, offset = [], 0
    for width in widths:
        parts.append(joined[:, offset : offset + width])
        offset += width
    return tuple(parts)


def layer_body(
    layer_input,
    output_gradient,
    picture_piece_starts,
    sequence_adapter_index,
    attention_norm_gain,
    attention_norm_bias,
    feedforward_norm_gain,
    feedforward_norm_bias,
    query_key_value_weight,
    attention_output_weight,
    up_projection_weight,
    down_projection_weight,
    adapter_projection_first,
    adapter_projection_second,
    adapter_heads_first,
    adapter_heads_second,
    adapter_up_first,
    adapter_up_second,
    adapter_down_first,
    adapter_down_second,
):
    seq_here, local_len, model_width = layer_input.shape
    tok_rows = seq_here * local_len
    tp_count = lax.axis_size("tp")
    adapter_tables = adapter_projection_first.shape[0]
    rank_width = adapter_projection_first.shape[2]
    head_width = HD
    device_heads = adapter_projection_second.shape[-1] // head_width
    local_width = device_heads * head_width
    columns = jnp.arange(adapter_tables * rank_width, dtype=jnp.int32) // rank_width
    chosen = (sequence_adapter_index[:, None] == columns[None, :]).astype(jnp.float32)
    select = jnp.broadcast_to(
        chosen[:, None, :], (seq_here, local_len, adapter_tables * rank_width)
    ).reshape(tok_rows, adapter_tables * rank_width)
    select_here = tp_rows(select, tp_count)
    head_ids = lax.axis_index("tp") * device_heads + jnp.arange(device_heads, dtype=jnp.int32)
    slopes = jnp.exp2(
        -8.0 * (head_ids.astype(jnp.float32) + 1.0) / (device_heads * tp_count)
    )
    here_pos = lax.axis_index("ctx") * local_len + jnp.arange(local_len, dtype=jnp.int32)
    here_labels = piece_labels(picture_piece_starts, here_pos)
    heads_first_local = flattened_first(adapter_heads_first)
    heads_pair = lax.all_gather(
        jnp.concatenate([attention_output_weight, heads_first_local], axis=1),
        "tp",
        axis=0,
        tiled=True,
    )
    out_cols = attention_output_weight.shape[1]
    heads_full = pair_gather(heads_pair[:, :out_cols], "shard", 1)
    heads_first_all_flattened = heads_pair[:, out_cols:]
    projection_first_flattened = flattened_first(adapter_projection_first)
    projection_second_flattened = flattened_second(adapter_projection_second)
    heads_first_flattened = flattened_first(adapter_heads_first)
    heads_second_flattened = flattened_second(adapter_heads_second)
    up_first_flattened = flattened_first(adapter_up_first)
    up_second_flattened = flattened_second(adapter_up_second)
    down_first_flattened = flattened_first(adapter_down_first)
    down_second_flattened = flattened_second(adapter_down_second)
    residual = layer_input.reshape(tok_rows, model_width).astype(jnp.float32)
    residual_here = tp_rows(residual, tp_count)
    first_norm = layer_norm(residual, attention_norm_gain, attention_norm_bias)
    first_act = first_norm.astype(jnp.bfloat16)
    _, first_back_full = jax.vjp(
        lambda inputs: layer_norm(inputs, attention_norm_gain, attention_norm_bias), residual_here
    )
    gathered_rows = (
        pair_gather(query_key_value_weight, "shard", 0),
        pair_gather(up_projection_weight, "shard", 0),
    )
    qkv_full = gathered_rows[0].reshape(model_width, 3 * local_width)
    up_full = gathered_rows[1]
    down_full = pair_gather(down_projection_weight, "shard", 1)
    first_low = (matmul(first_act, projection_first_flattened) * select).astype(jnp.bfloat16)
    projected = (
        matmul(first_act, qkv_full) + matmul(first_low, projection_second_flattened)
    ).astype(jnp.bfloat16)
    queries_flat = projected[:, :local_width].reshape(seq_here, local_len, local_width)
    queries = queries_flat.reshape(seq_here, local_len, device_heads, head_width)
    key_rows = projected[:, local_width : 2 * local_width].reshape(seq_here, local_len, local_width)
    value_rows = projected[:, 2 * local_width :].reshape(seq_here, local_len, local_width)
    ctx_count = lax.axis_size("ctx")
    ctx_here = lax.axis_index("ctx")
    blocks = partner_swaps(
        jnp.concatenate([key_rows, value_rows], axis=2), "ctx", ctx_count
    )
    pieces = jnp.concatenate(blocks, axis=1)
    piece_len = pieces.shape[1]
    key_pos = jnp.concatenate(
        [
            (ctx_here ^ offset) * local_len + jnp.arange(local_len, dtype=jnp.int32)
            for offset in range(ctx_count)
        ]
    )
    key_labels = piece_labels(picture_piece_starts, key_pos)
    visible_mask = visible(here_pos, key_pos, here_labels, key_labels)
    piece_keys = pieces[:, :, :local_width].reshape(seq_here, piece_len, device_heads, head_width)
    piece_values = pieces[:, :, local_width:].reshape(
        seq_here, piece_len, device_heads, head_width
    )
    exponent = exponents(queries, piece_keys, here_pos, key_pos, visible_mask, slopes)
    weighted = jnp.einsum(
        "shqk,skhd->sqhd",
        exponent.astype(jnp.bfloat16),
        piece_values,
        preferred_element_type=jnp.float32,
    )
    weighted, totals = (weighted, jnp.sum(exponent, axis=-1))
    per_total = jnp.transpose(totals, (0, 2, 1))[..., None]
    heads_raw = weighted / per_total
    heads_act = heads_raw.reshape(tok_rows, local_width).astype(jnp.bfloat16)
    heads_act_here = lax.all_to_all(heads_act, "tp", 0, 1, tiled=True)
    attn_here = matmul(heads_act_here, heads_full)
    heads_low_here = (matmul(heads_act_here, heads_first_all_flattened) * select_here).astype(
        jnp.bfloat16
    )
    middle_here = residual_here + attn_here + matmul(heads_low_here, heads_second_flattened)
    second_norm, second_back = jax.vjp(
        lambda inputs: layer_norm(inputs, feedforward_norm_gain, feedforward_norm_bias), middle_here
    )
    second_act_here = second_norm.astype(jnp.bfloat16)
    (second_act,) = gather_rows((second_act_here,))
    up_low = (matmul(second_act, up_first_flattened) * select).astype(jnp.bfloat16)
    hidden = matmul(second_act, up_full) + matmul(up_low, up_second_flattened)
    activated, gelu_back = jax.vjp(gelu_tanh, hidden)
    activated = activated.astype(jnp.bfloat16)
    down_part = matmul(activated, down_full)
    down_low_part = matmul(activated, down_first_flattened)
    ffn_here, ffn_low_here = scatter_rows((down_part, down_low_part))
    down_low_here = (ffn_low_here * select_here).astype(jnp.bfloat16)
    result_here = (middle_here + ffn_here + matmul(down_low_here, down_second_flattened)).astype(
        jnp.bfloat16
    )
    (result_rows,) = gather_rows((result_here,))
    layer_out = result_rows.reshape(layer_input.shape)
    grad_top_low = output_gradient.reshape(tok_rows, model_width)
    grad_top_here = tp_rows(grad_top_low, tp_count).astype(jnp.float32)
    down_back = (matmul_nt(grad_top_low, down_second_flattened) * select).astype(jnp.bfloat16)
    grad_down_in = matmul_tn(activated, down_back)
    grad_activated = matmul_nt(grad_top_low, down_full) + matmul_nt(down_back, down_first_flattened)
    grad_hidden = gelu_back(grad_activated)[0].astype(jnp.bfloat16)
    up_second_gradient = matmul_tn(up_low, grad_hidden)
    ffn_back_part = matmul_nt(grad_hidden, up_full)
    ffn_back_low = matmul_nt(grad_hidden, up_second_flattened)
    back_here, back_low_here = scatter_rows((ffn_back_part, ffn_back_low))
    up_back_here = (back_low_here * select_here).astype(jnp.bfloat16)
    grad_second = back_here + matmul_nt(up_back_here, up_first_flattened)
    grad_middle_here = grad_top_here + second_back(grad_second)[0]
    grad_middle_low_here = grad_middle_here.astype(jnp.bfloat16)
    heads_back_here = (matmul_nt(grad_middle_low_here, heads_second_flattened) * select_here).astype(
        jnp.bfloat16
    )
    low_rows = partner_gather_rows(
        jnp.concatenate([down_low_here, up_back_here, heads_back_here], axis=1), "tp"
    )
    down_low, up_back, heads_back = split_columns(low_rows, [rank_width * adapter_tables] * 3)
    down_second_gradient = matmul_tn(down_low, grad_top_low)
    grad_up_in = matmul_tn(second_act, up_back)
    grad_heads_in = matmul_tn(heads_act, heads_back)
    heads_second_gradient = matmul_tn(heads_low_here, grad_middle_low_here)
    early_terms = narrow_psum(
        (
            unflat_in(grad_heads_in, adapter_tables),
            unflat_in(grad_up_in, adapter_tables),
            up_second_gradient.reshape(adapter_up_second.shape),
            unflat_in(grad_down_in, adapter_tables),
            down_second_gradient.reshape(adapter_down_second.shape),
        ),
        ("shard", "ctx"),
    )
    heads_second_total = narrow_psum(
        heads_second_gradient.reshape(adapter_heads_second.shape), ("shard", "ctx", "tp")
    )
    grad_heads_here = (
        matmul_nt(grad_middle_low_here, heads_full)
        + matmul_nt(heads_back_here, heads_first_all_flattened)
    ).astype(jnp.bfloat16)
    grad_heads = lax.all_to_all(grad_heads_here, "tp", 1, 0, tiled=True)
    grad_heads_wide = grad_heads.reshape(seq_here, local_len, device_heads, head_width).astype(
        jnp.float32
    )
    scaled_grad = (grad_heads_wide / per_total).astype(jnp.bfloat16)
    row_delta = jnp.sum(grad_heads_wide * heads_raw, axis=-1) / per_total[..., 0]
    grad_queries, grad_keyrows, grad_valrows = block_grads(
        queries,
        scaled_grad,
        row_delta,
        piece_keys,
        piece_values,
        here_pos,
        key_pos,
        visible_mask,
        slopes,
    )
    grad_kv = jnp.concatenate(
        [
            grad_keyrows.reshape(seq_here, ctx_count, local_len, local_width),
            grad_valrows.reshape(seq_here, ctx_count, local_len, local_width),
        ],
        axis=3,
    )
    grad_kv_here = grad_kv[:, 0]
    for offset in range(1, ctx_count):
        pairs = [(index, index ^ offset) for index in range(ctx_count)]
        grad_kv_here = grad_kv_here + lax.ppermute(
            grad_kv[:, offset].astype(jnp.bfloat16), "ctx", pairs
        ).astype(jnp.float32)
    grad_keys_all = grad_kv_here[:, :, :local_width]
    grad_values_all = grad_kv_here[:, :, local_width:]
    grad_projected = jnp.concatenate(
        [
            grad_queries.reshape(tok_rows, local_width),
            grad_keys_all.reshape(tok_rows, local_width),
            grad_values_all.reshape(tok_rows, local_width),
        ],
        axis=1,
    ).astype(jnp.bfloat16)
    projection_second_gradient = matmul_tn(first_low, grad_projected)
    attn_back_part = matmul_nt(grad_projected, qkv_full)
    attn_back_low = matmul_nt(grad_projected, projection_second_flattened)
    low_blocks = jnp.stack(partner_swaps(attn_back_low, "tp", tp_count))
    low_owners = jnp.bitwise_xor(lax.axis_index("tp"), jnp.arange(tp_count, dtype=jnp.int32))
    low_total = jnp.sum(jnp.take(low_blocks, low_owners, axis=0), axis=0)
    select_late = lax.optimization_barrier(select)
    qkv_back = (low_total * select_late).astype(jnp.bfloat16)
    grad_qkv_in = matmul_tn(first_act, qkv_back)
    late_terms = butterfly_sum(
        (
            unflat_in(grad_qkv_in, adapter_tables),
            projection_second_gradient.reshape(adapter_projection_second.shape),
        ),
        ("shard", "ctx"),
    )
    first_here, first_low_here = scatter_rows((attn_back_part, attn_back_low))
    select_later = lax.optimization_barrier(select_here)
    qkv_back_here = (first_low_here * select_later).astype(jnp.bfloat16)
    grad_first = first_here + matmul_nt(qkv_back_here, projection_first_flattened)
    input_here = (grad_middle_here + first_back_full(grad_first)[0]).astype(jnp.bfloat16)
    (input_rows,) = gather_rows((input_here,))
    input_grad = input_rows.reshape(layer_input.shape)
    return (
        layer_out,
        input_grad,
        late_terms[0],
        late_terms[1],
        early_terms[0],
        heads_second_total,
        early_terms[1],
        early_terms[2],
        early_terms[3],
        early_terms[4],
    )


def solution(mesh):
    placed = (
        P("shard", "ctx", None),
        P("shard", "ctx", None),
        P("shard", None),
        P("shard"),
        P(),
        P(),
        P(),
        P(),
        P("shard", None, "tp"),
        P("tp", "shard"),
        P("shard", "tp"),
        P("tp", "shard"),
        P(),
        P(None, None, None, "tp"),
        P(None, "tp", None),
        P(),
        P(),
        P(None, None, "tp"),
        P(None, "tp", None),
        P(),
    )
    return jax.shard_map(
        layer_body,
        mesh=mesh,
        in_specs=placed,
        out_specs=(
            P("shard", "ctx", None),
            P("shard", "ctx", None),
            P(),
            P(None, None, None, "tp"),
            P(None, "tp", None),
            P(),
            P(),
            P(None, None, "tp"),
            P(None, "tp", None),
            P(),
        ),
        check_vma=False,
    )
```

```python
import jax
import jax.numpy as jnp
from jax import lax
from jax.sharding import PartitionSpec as P

HD = 128
PIC = 256


NORM_EPS = 1e-05


def layer_norm(inputs, gains, biases):
    average = jnp.mean(inputs, axis=-1, keepdims=True)
    centred = inputs - average
    spread = jnp.mean(centred * centred, axis=-1, keepdims=True)
    return centred * lax.rsqrt(spread + NORM_EPS) * gains + biases


def gelu_tanh(inputs):
    return (
        0.5
        * inputs
        * (1.0 + jnp.tanh(0.7978845608028654 * (inputs + 0.044715 * inputs * inputs * inputs)))
    )


def flattened_first(adapter_mat):
    adapter_tables, inner_dim, rank_width = adapter_mat.shape
    return jnp.transpose(adapter_mat, (1, 0, 2)).reshape(inner_dim, adapter_tables * rank_width)


def flattened_second(adapter_mat):
    return adapter_mat.reshape(adapter_mat.shape[0] * adapter_mat.shape[1], -1)


def unflat_in(grad_flat, adapter_tables):
    inner_dim = grad_flat.shape[0]
    return jnp.transpose(grad_flat.reshape(inner_dim, adapter_tables, -1), (1, 0, 2))


def matmul(left_mat, right_mat):
    return jnp.dot(left_mat, right_mat, preferred_element_type=jnp.float32)


def matmul_tn(left_mat, right_mat):
    return lax.dot_general(
        left_mat, right_mat, (((0,), (0,)), ((), ())), preferred_element_type=jnp.float32
    )


def matmul_nt(left_mat, right_mat):
    return lax.dot_general(
        left_mat, right_mat, (((1,), (1,)), ((), ())), preferred_element_type=jnp.float32
    )


def piece_labels(starts, positions):
    inside = (positions[None, None, :] >= starts[:, :, None]) & (
        positions[None, None, :] < starts[:, :, None] + PIC
    )
    labels = jnp.arange(1, starts.shape[1] + 1, dtype=jnp.int32)
    return jnp.sum(jnp.where(inside, labels[None, :, None], 0), axis=1)


def visible(query_pos, key_pos, query_labels, key_labels):
    causal = key_pos[None, None, :] <= query_pos[None, :, None]
    shared = (query_labels[:, :, None] == key_labels[:, None, :]) & (query_labels[:, :, None] > 0)
    return causal | shared


def exponents(queries, key_rows, query_pos, key_pos, visible_mask, slopes):
    score_scale = queries.shape[-1] ** (-0.5)
    logits = (
        jnp.einsum("sqhd,skhd->shqk", queries, key_rows, preferred_element_type=jnp.float32)
        * score_scale
    )
    distance = jnp.abs(query_pos[:, None] - key_pos[None, :]).astype(jnp.float32)
    logits = logits - slopes[None, :, None, None] * distance[None, None]
    return jnp.where(visible_mask[:, None], jnp.exp(logits), 0.0)


def block_grads(
    queries, scaled_grad, row_delta, key_rows, value_rows, query_pos, key_pos, visible_mask, slopes
):
    score_scale = queries.shape[-1] ** (-0.5)
    exponent = exponents(queries, key_rows, query_pos, key_pos, visible_mask, slopes)
    products_gv = jnp.einsum(
        "sqhd,skhd->shqk", scaled_grad, value_rows, preferred_element_type=jnp.float32
    )
    grad_logits = (
        exponent * (products_gv - jnp.transpose(row_delta, (0, 2, 1))[..., None])
    ).astype(jnp.bfloat16)
    grad_queries = (
        jnp.einsum("shqk,skhd->sqhd", grad_logits, key_rows, preferred_element_type=jnp.float32)
        * score_scale
    )
    grad_keyrows = (
        jnp.einsum("shqk,sqhd->skhd", grad_logits, queries, preferred_element_type=jnp.float32)
        * score_scale
    )
    grad_valrows = jnp.einsum(
        "shqk,sqhd->skhd",
        exponent.astype(jnp.bfloat16),
        scaled_grad,
        preferred_element_type=jnp.float32,
    )
    return (grad_queries, grad_keyrows, grad_valrows)


def partner_swaps(block, axis_name, axis_count):
    received = [block]
    for offset in range(1, axis_count):
        pairs = [(index, index ^ offset) for index in range(axis_count)]
        received.append(lax.ppermute(block, axis_name, pairs))
    return received


def pair_gather(block, axis_name, axis):
    if lax.axis_size(axis_name) != 2:
        return lax.all_gather(block, axis_name, axis=axis, tiled=True)
    other = lax.ppermute(block, axis_name, [(0, 1), (1, 0)])
    first = lax.axis_index(axis_name) == 0
    low = jnp.where(first, block, other)
    high = jnp.where(first, other, block)
    return jnp.concatenate([low, high], axis=axis)


def butterfly_sum(values, axis_names):
    leaves, tree = jax.tree.flatten(values)
    packed = jnp.concatenate([leaf.reshape(-1) for leaf in leaves])
    for axis_name in axis_names:
        axis_count = lax.axis_size(axis_name)
        step = 1
        while step < axis_count:
            pairs = [(index, index ^ step) for index in range(axis_count)]
            packed = packed + lax.ppermute(packed, axis_name, pairs)
            step *= 2
    parts, offset = [], 0
    for leaf in leaves:
        parts.append(packed[offset : offset + leaf.size].reshape(leaf.shape))
        offset += leaf.size
    return jax.tree.unflatten(tree, parts)


def partner_gather_rows(rows_here, axis_name):
    axis_count = lax.axis_size(axis_name)
    blocks = jnp.stack(partner_swaps(rows_here, axis_name, axis_count))
    owners = jnp.bitwise_xor(
        lax.axis_index(axis_name), jnp.arange(axis_count, dtype=jnp.int32)
    )
    ordered = jnp.take(blocks, owners, axis=0)
    return ordered.reshape(axis_count * rows_here.shape[0], *rows_here.shape[1:])


def narrow_psum(values, axis_names):
    summed = lax.psum(jax.tree.map(lambda value: value.astype(jnp.bfloat16), values), axis_names)
    return jax.tree.map(lambda value: value.astype(jnp.float32), summed)


def tp_rows(rows_array, tp_count):
    chunk = rows_array.shape[0] // tp_count
    return lax.dynamic_slice_in_dim(rows_array, lax.axis_index("tp") * chunk, chunk, axis=0)


def scatter_rows(partials):
    widths = [part.shape[1] for part in partials]
    joined = lax.psum_scatter(
        jnp.concatenate(partials, axis=1).astype(jnp.bfloat16),
        "tp",
        scatter_dimension=0,
        tiled=True,
    )
    return split_columns(joined.astype(jnp.float32), widths)


def gather_rows(rows_here):
    widths = [part.shape[1] for part in rows_here]
    joined = lax.all_gather(jnp.concatenate(rows_here, axis=1), "tp", axis=0, tiled=True)
    return split_columns(joined, widths)


def split_columns(joined, widths):
    parts, offset = [], 0
    for width in widths:
        parts.append(joined[:, offset : offset + width])
        offset += width
    return tuple(parts)


def layer_body(
    layer_input,
    output_gradient,
    picture_piece_starts,
    sequence_adapter_index,
    attention_norm_gain,
    attention_norm_bias,
    feedforward_norm_gain,
    feedforward_norm_bias,
    query_key_value_weight,
    attention_output_weight,
    up_projection_weight,
    down_projection_weight,
    adapter_projection_first,
    adapter_projection_second,
    adapter_heads_first,
    adapter_heads_second,
    adapter_up_first,
    adapter_up_second,
    adapter_down_first,
    adapter_down_second,
):
    seq_here, local_len, model_width = layer_input.shape
    tok_rows = seq_here * local_len
    tp_count = lax.axis_size("tp")
    adapter_tables = adapter_projection_first.shape[0]
    rank_width = adapter_projection_first.shape[2]
    head_width = HD
    device_heads = adapter_projection_second.shape[-1] // head_width
    local_width = device_heads * head_width
    columns = jnp.arange(adapter_tables * rank_width, dtype=jnp.int32) // rank_width
    chosen = (sequence_adapter_index[:, None] == columns[None, :]).astype(jnp.float32)
    select = jnp.broadcast_to(
        chosen[:, None, :], (seq_here, local_len, adapter_tables * rank_width)
    ).reshape(tok_rows, adapter_tables * rank_width)
    select_here = tp_rows(select, tp_count)
    head_ids = lax.axis_index("tp") * device_heads + jnp.arange(device_heads, dtype=jnp.int32)
    slopes = jnp.exp2(
        -8.0 * (head_ids.astype(jnp.float32) + 1.0) / (device_heads * tp_count)
    )
    here_pos = lax.axis_index("ctx") * local_len + jnp.arange(local_len, dtype=jnp.int32)
    here_labels = piece_labels(picture_piece_starts, here_pos)
    heads_first_local = flattened_first(adapter_heads_first)
    heads_pair = lax.all_gather(
        jnp.concatenate([attention_output_weight, heads_first_local], axis=1),
        "tp",
        axis=0,
        tiled=True,
    )
    out_cols = attention_output_weight.shape[1]
    heads_full = pair_gather(heads_pair[:, :out_cols], "shard", 1)
    heads_first_all_flattened = heads_pair[:, out_cols:]
    projection_first_flattened = flattened_first(adapter_projection_first)
    projection_second_flattened = flattened_second(adapter_projection_second)
    heads_first_flattened = flattened_first(adapter_heads_first)
    heads_second_flattened = flattened_second(adapter_heads_second)
    up_first_flattened = flattened_first(adapter_up_first)
    up_second_flattened = flattened_second(adapter_up_second)
    down_first_flattened = flattened_first(adapter_down_first)
    down_second_flattened = flattened_second(adapter_down_second)
    residual = layer_input.reshape(tok_rows, model_width).astype(jnp.float32)
    residual_here = tp_rows(residual, tp_count)
    first_norm = layer_norm(residual, attention_norm_gain, attention_norm_bias)
    first_act = first_norm.astype(jnp.bfloat16)
    _, first_back_full = jax.vjp(
        lambda inputs: layer_norm(inputs, attention_norm_gain, attention_norm_bias), residual_here
    )
    gathered_rows = (
        pair_gather(query_key_value_weight, "shard", 0),
        pair_gather(up_projection_weight, "shard", 0),
    )
    qkv_full = gathered_rows[0].reshape(model_width, 3 * local_width)
    up_full = gathered_rows[1]
    down_full = pair_gather(down_projection_weight, "shard", 1)
    first_low = (matmul(first_act, projection_first_flattened) * select).astype(jnp.bfloat16)
    projected = (
        matmul(first_act, qkv_full) + matmul(first_low, projection_second_flattened)
    ).astype(jnp.bfloat16)
    queries_flat = projected[:, :local_width].reshape(seq_here, local_len, local_width)
    queries = queries_flat.reshape(seq_here, local_len, device_heads, head_width)
    key_rows = projected[:, local_width : 2 * local_width].reshape(seq_here, local_len, local_width)
    value_rows = projected[:, 2 * local_width :].reshape(seq_here, local_len, local_width)
    ctx_count = lax.axis_size("ctx")
    ctx_here = lax.axis_index("ctx")
    blocks = partner_swaps(
        jnp.concatenate([key_rows, value_rows], axis=2), "ctx", ctx_count
    )
    pieces = jnp.concatenate(blocks, axis=1)
    piece_len = pieces.shape[1]
    key_pos = jnp.concatenate(
        [
            (ctx_here ^ offset) * local_len + jnp.arange(local_len, dtype=jnp.int32)
            for offset in range(ctx_count)
        ]
    )
    key_labels = piece_labels(picture_piece_starts, key_pos)
    visible_mask = visible(here_pos, key_pos, here_labels, key_labels)
    piece_keys = pieces[:, :, :local_width].reshape(seq_here, piece_len, device_heads, head_width)
    piece_values = pieces[:, :, local_width:].reshape(
        seq_here, piece_len, device_heads, head_width
    )
    exponent = exponents(queries, piece_keys, here_pos, key_pos, visible_mask, slopes)
    weighted = jnp.einsum(
        "shqk,skhd->sqhd",
        exponent.astype(jnp.bfloat16),
        piece_values,
        preferred_element_type=jnp.float32,
    )
    weighted, totals = (weighted, jnp.sum(exponent, axis=-1))
    per_total = jnp.transpose(totals, (0, 2, 1))[..., None]
    heads_raw = weighted / per_total
    heads_act = heads_raw.reshape(tok_rows, local_width).astype(jnp.bfloat16)
    heads_act_here = lax.all_to_all(heads_act, "tp", 0, 1, tiled=True)
    attn_here = matmul(heads_act_here, heads_full)
    heads_low_here = (matmul(heads_act_here, heads_first_all_flattened) * select_here).astype(
        jnp.bfloat16
    )
    middle_here = residual_here + attn_here + matmul(heads_low_here, heads_second_flattened)
    second_norm, second_back = jax.vjp(
        lambda inputs: layer_norm(inputs, feedforward_norm_gain, feedforward_norm_bias), middle_here
    )
    second_act_here = second_norm.astype(jnp.bfloat16)
    (second_act,) = gather_rows((second_act_here,))
    up_low = (matmul(second_act, up_first_flattened) * select).astype(jnp.bfloat16)
    hidden = matmul(second_act, up_full) + matmul(up_low, up_second_flattened)
    activated, gelu_back = jax.vjp(gelu_tanh, hidden)
    activated = activated.astype(jnp.bfloat16)
    down_part = matmul(activated, down_full)
    down_low_part = matmul(activated, down_first_flattened)
    ffn_here, ffn_low_here = scatter_rows((down_part, down_low_part))
    down_low_here = (ffn_low_here * select_here).astype(jnp.bfloat16)
    result_here = (middle_here + ffn_here + matmul(down_low_here, down_second_flattened)).astype(
        jnp.bfloat16
    )
    (result_rows,) = gather_rows((result_here,))
    layer_out = result_rows.reshape(layer_input.shape)
    grad_top_low = output_gradient.reshape(tok_rows, model_width)
    grad_top_here = tp_rows(grad_top_low, tp_count).astype(jnp.float32)
    down_back = (matmul_nt(grad_top_low, down_second_flattened) * select).astype(jnp.bfloat16)
    grad_down_in = matmul_tn(activated, down_back)
    grad_activated = matmul_nt(grad_top_low, down_full) + matmul_nt(down_back, down_first_flattened)
    grad_hidden = gelu_back(grad_activated)[0].astype(jnp.bfloat16)
    up_second_gradient = matmul_tn(up_low, grad_hidden)
    ffn_back_part = matmul_nt(grad_hidden, up_full)
    ffn_back_low = matmul_nt(grad_hidden, up_second_flattened)
    back_here, back_low_here = scatter_rows((ffn_back_part, ffn_back_low))
    up_back_here = (back_low_here * select_here).astype(jnp.bfloat16)
    grad_second = back_here + matmul_nt(up_back_here, up_first_flattened)
    grad_middle_here = grad_top_here + second_back(grad_second)[0]
    grad_middle_low_here = grad_middle_here.astype(jnp.bfloat16)
    heads_back_here = (matmul_nt(grad_middle_low_here, heads_second_flattened) * select_here).astype(
        jnp.bfloat16
    )
    low_rows = partner_gather_rows(
        jnp.concatenate([down_low_here, up_back_here, heads_back_here], axis=1), "tp"
    )
    down_low, up_back, heads_back = split_columns(low_rows, [rank_width * adapter_tables] * 3)
    down_second_gradient = matmul_tn(down_low, grad_top_low)
    grad_up_in = matmul_tn(second_act, up_back)
    grad_heads_in = matmul_tn(heads_act, heads_back)
    heads_second_gradient = matmul_tn(heads_low_here, grad_middle_low_here)
    early_terms = narrow_psum(
        (
            unflat_in(grad_heads_in, adapter_tables),
            unflat_in(grad_up_in, adapter_tables),
            up_second_gradient.reshape(adapter_up_second.shape),
            unflat_in(grad_down_in, adapter_tables),
            down_second_gradient.reshape(adapter_down_second.shape),
        ),
        ("shard", "ctx"),
    )
    heads_second_total = narrow_psum(
        heads_second_gradient.reshape(adapter_heads_second.shape), ("shard", "ctx", "tp")
    )
    grad_heads_here = (
        matmul_nt(grad_middle_low_here, heads_full)
        + matmul_nt(heads_back_here, heads_first_all_flattened)
    ).astype(jnp.bfloat16)
    grad_heads = lax.all_to_all(grad_heads_here, "tp", 1, 0, tiled=True)
    grad_heads_wide = grad_heads.reshape(seq_here, local_len, device_heads, head_width).astype(
        jnp.float32
    )
    scaled_grad = (grad_heads_wide / per_total).astype(jnp.bfloat16)
    row_delta = jnp.sum(grad_heads_wide * heads_raw, axis=-1) / per_total[..., 0]
    grad_queries, grad_keyrows, grad_valrows = block_grads(
        queries,
        scaled_grad,
        row_delta,
        piece_keys,
        piece_values,
        here_pos,
        key_pos,
        visible_mask,
        slopes,
    )
    grad_kv = jnp.concatenate(
        [
            grad_keyrows.reshape(seq_here, ctx_count, local_len, local_width),
            grad_valrows.reshape(seq_here, ctx_count, local_len, local_width),
        ],
        axis=3,
    )
    grad_kv_here = grad_kv[:, 0]
    for offset in range(1, ctx_count):
        pairs = [(index, index ^ offset) for index in range(ctx_count)]
        grad_kv_here = grad_kv_here + lax.ppermute(
            grad_kv[:, offset].astype(jnp.bfloat16), "ctx", pairs
        ).astype(jnp.float32)
    grad_keys_all = grad_kv_here[:, :, :local_width]
    grad_values_all = grad_kv_here[:, :, local_width:]
    grad_projected = jnp.concatenate(
        [
            grad_queries.reshape(tok_rows, local_width),
            grad_keys_all.reshape(tok_rows, local_width),
            grad_values_all.reshape(tok_rows, local_width),
        ],
        axis=1,
    ).astype(jnp.bfloat16)
    projection_second_gradient = matmul_tn(first_low, grad_projected)
    attn_back_part = matmul_nt(grad_projected, qkv_full)
    attn_back_low = matmul_nt(grad_projected, projection_second_flattened)

    first_here, first_low_here = scatter_rows((attn_back_part, attn_back_low))
    select_later = lax.optimization_barrier(select_here)
    qkv_back_here = (first_low_here * select_later).astype(jnp.bfloat16)
    grad_first = first_here + matmul_nt(qkv_back_here, projection_first_flattened)
    input_here = (grad_middle_here + first_back_full(grad_first)[0]).astype(jnp.bfloat16)
    qkv_back = partner_gather_rows(qkv_back_here, "tp")
    grad_qkv_in = matmul_tn(first_act, qkv_back)
    late_terms = butterfly_sum(
        (
            unflat_in(grad_qkv_in, adapter_tables),
            projection_second_gradient.reshape(adapter_projection_second.shape),
        ),
        ("shard", "ctx"),
    )
    (input_rows,) = gather_rows((input_here,))
    input_grad = input_rows.reshape(layer_input.shape)
    return (
        layer_out,
        input_grad,
        late_terms[0],
        late_terms[1],
        early_terms[0],
        heads_second_total,
        early_terms[1],
        early_terms[2],
        early_terms[3],
        early_terms[4],
    )


def solution(mesh):
    placed = (
        P("shard", "ctx", None),
        P("shard", "ctx", None),
        P("shard", None),
        P("shard"),
        P(),
        P(),
        P(),
        P(),
        P("shard", None, "tp"),
        P("tp", "shard"),
        P("shard", "tp"),
        P("tp", "shard"),
        P(),
        P(None, None, None, "tp"),
        P(None, "tp", None),
        P(),
        P(),
        P(None, None, "tp"),
        P(None, "tp", None),
        P(),
    )
    return jax.shard_map(
        layer_body,
        mesh=mesh,
        in_specs=placed,
        out_specs=(
            P("shard", "ctx", None),
            P("shard", "ctx", None),
            P(),
            P(None, None, None, "tp"),
            P(None, "tp", None),
            P(),
            P(),
            P(None, None, "tp"),
            P(None, "tp", None),
            P(),
        ),
        check_vma=False,
    )
```

```python
import jax
import jax.numpy as jnp
from jax import lax
from jax.sharding import PartitionSpec as P

HD = 128
PIC = 256


NORM_EPS = 1e-05


def layer_norm(inputs, gains, biases):
    average = jnp.mean(inputs, axis=-1, keepdims=True)
    centred = inputs - average
    spread = jnp.mean(centred * centred, axis=-1, keepdims=True)
    return centred * lax.rsqrt(spread + NORM_EPS) * gains + biases


def gelu_tanh(inputs):
    return (
        0.5
        * inputs
        * (1.0 + jnp.tanh(0.7978845608028654 * (inputs + 0.044715 * inputs * inputs * inputs)))
    )


def flattened_first(adapter_mat):
    adapter_tables, inner_dim, rank_width = adapter_mat.shape
    return jnp.transpose(adapter_mat, (1, 0, 2)).reshape(inner_dim, adapter_tables * rank_width)


def flattened_second(adapter_mat):
    return adapter_mat.reshape(adapter_mat.shape[0] * adapter_mat.shape[1], -1)


def unflat_in(grad_flat, adapter_tables):
    inner_dim = grad_flat.shape[0]
    return jnp.transpose(grad_flat.reshape(inner_dim, adapter_tables, -1), (1, 0, 2))


def matmul(left_mat, right_mat):
    return jnp.dot(left_mat, right_mat, preferred_element_type=jnp.float32)


def matmul_tn(left_mat, right_mat):
    return lax.dot_general(
        left_mat, right_mat, (((0,), (0,)), ((), ())), preferred_element_type=jnp.float32
    )


def matmul_nt(left_mat, right_mat):
    return lax.dot_general(
        left_mat, right_mat, (((1,), (1,)), ((), ())), preferred_element_type=jnp.float32
    )


def piece_labels(starts, positions):
    inside = (positions[None, None, :] >= starts[:, :, None]) & (
        positions[None, None, :] < starts[:, :, None] + PIC
    )
    labels = jnp.arange(1, starts.shape[1] + 1, dtype=jnp.int32)
    return jnp.sum(jnp.where(inside, labels[None, :, None], 0), axis=1)


def visible(query_pos, key_pos, query_labels, key_labels):
    causal = key_pos[None, None, :] <= query_pos[None, :, None]
    shared = (query_labels[:, :, None] == key_labels[:, None, :]) & (query_labels[:, :, None] > 0)
    return causal | shared


def exponents(queries, key_rows, query_pos, key_pos, visible_mask, slopes):
    score_scale = queries.shape[-1] ** (-0.5)
    logits = (
        jnp.einsum("sqhd,skhd->shqk", queries, key_rows, preferred_element_type=jnp.float32)
        * score_scale
    )
    distance = jnp.abs(query_pos[:, None] - key_pos[None, :]).astype(jnp.float32)
    logits = logits - slopes[None, :, None, None] * distance[None, None]
    return jnp.where(visible_mask[:, None], jnp.exp(logits), 0.0)


def block_grads(
    queries, scaled_grad, row_delta, key_rows, value_rows, query_pos, key_pos, visible_mask, slopes
):
    score_scale = queries.shape[-1] ** (-0.5)
    exponent = exponents(queries, key_rows, query_pos, key_pos, visible_mask, slopes)
    products_gv = jnp.einsum(
        "sqhd,skhd->shqk", scaled_grad, value_rows, preferred_element_type=jnp.float32
    )
    grad_logits = (
        exponent * (products_gv - jnp.transpose(row_delta, (0, 2, 1))[..., None])
    ).astype(jnp.bfloat16)
    grad_queries = (
        jnp.einsum("shqk,skhd->sqhd", grad_logits, key_rows, preferred_element_type=jnp.float32)
        * score_scale
    )
    grad_keyrows = (
        jnp.einsum("shqk,sqhd->skhd", grad_logits, queries, preferred_element_type=jnp.float32)
        * score_scale
    )
    grad_valrows = jnp.einsum(
        "shqk,sqhd->skhd",
        exponent.astype(jnp.bfloat16),
        scaled_grad,
        preferred_element_type=jnp.float32,
    )
    return (grad_queries, grad_keyrows, grad_valrows)


def partner_swaps(block, axis_name, axis_count):
    received = [block]
    for offset in range(1, axis_count):
        pairs = [(index, index ^ offset) for index in range(axis_count)]
        received.append(lax.ppermute(block, axis_name, pairs))
    return received


def pair_gather(block, axis_name, axis):
    if lax.axis_size(axis_name) != 2:
        return lax.all_gather(block, axis_name, axis=axis, tiled=True)
    other = lax.ppermute(block, axis_name, [(0, 1), (1, 0)])
    first = lax.axis_index(axis_name) == 0
    low = jnp.where(first, block, other)
    high = jnp.where(first, other, block)
    return jnp.concatenate([low, high], axis=axis)


def butterfly_sum(values, axis_names):
    leaves, tree = jax.tree.flatten(values)
    packed = jnp.concatenate([leaf.reshape(-1) for leaf in leaves])
    for axis_name in axis_names:
        axis_count = lax.axis_size(axis_name)
        step = 1
        while step < axis_count:
            pairs = [(index, index ^ step) for index in range(axis_count)]
            narrow = packed.astype(jnp.bfloat16)
            packed = narrow.astype(jnp.float32) + lax.ppermute(narrow, axis_name, pairs).astype(
                jnp.float32
            )
            step *= 2
    parts, offset = [], 0
    for leaf in leaves:
        parts.append(packed[offset : offset + leaf.size].reshape(leaf.shape))
        offset += leaf.size
    return jax.tree.unflatten(tree, parts)


def partner_gather_rows(rows_here, axis_name):
    axis_count = lax.axis_size(axis_name)
    blocks = jnp.stack(partner_swaps(rows_here, axis_name, axis_count))
    owners = jnp.bitwise_xor(
        lax.axis_index(axis_name), jnp.arange(axis_count, dtype=jnp.int32)
    )
    ordered = jnp.take(blocks, owners, axis=0)
    return ordered.reshape(axis_count * rows_here.shape[0], *rows_here.shape[1:])


def narrow_psum(values, axis_names):
    summed = lax.psum(jax.tree.map(lambda value: value.astype(jnp.bfloat16), values), axis_names)
    return jax.tree.map(lambda value: value.astype(jnp.float32), summed)


def tp_rows(rows_array, tp_count):
    chunk = rows_array.shape[0] // tp_count
    return lax.dynamic_slice_in_dim(rows_array, lax.axis_index("tp") * chunk, chunk, axis=0)


def scatter_rows(partials):
    widths = [part.shape[1] for part in partials]
    joined = lax.psum_scatter(
        jnp.concatenate(partials, axis=1).astype(jnp.bfloat16),
        "tp",
        scatter_dimension=0,
        tiled=True,
    )
    return split_columns(joined.astype(jnp.float32), widths)


def gather_rows(rows_here):
    widths = [part.shape[1] for part in rows_here]
    joined = lax.all_gather(jnp.concatenate(rows_here, axis=1), "tp", axis=0, tiled=True)
    return split_columns(joined, widths)


def split_columns(joined, widths):
    parts, offset = [], 0
    for width in widths:
        parts.append(joined[:, offset : offset + width])
        offset += width
    return tuple(parts)


def layer_body(
    layer_input,
    output_gradient,
    picture_piece_starts,
    sequence_adapter_index,
    attention_norm_gain,
    attention_norm_bias,
    feedforward_norm_gain,
    feedforward_norm_bias,
    query_key_value_weight,
    attention_output_weight,
    up_projection_weight,
    down_projection_weight,
    adapter_projection_first,
    adapter_projection_second,
    adapter_heads_first,
    adapter_heads_second,
    adapter_up_first,
    adapter_up_second,
    adapter_down_first,
    adapter_down_second,
):
    seq_here, local_len, model_width = layer_input.shape
    tok_rows = seq_here * local_len
    tp_count = lax.axis_size("tp")
    adapter_tables = adapter_projection_first.shape[0]
    rank_width = adapter_projection_first.shape[2]
    head_width = HD
    device_heads = adapter_projection_second.shape[-1] // head_width
    local_width = device_heads * head_width
    columns = jnp.arange(adapter_tables * rank_width, dtype=jnp.int32) // rank_width
    chosen = (sequence_adapter_index[:, None] == columns[None, :]).astype(jnp.float32)
    select = jnp.broadcast_to(
        chosen[:, None, :], (seq_here, local_len, adapter_tables * rank_width)
    ).reshape(tok_rows, adapter_tables * rank_width)
    select_here = tp_rows(select, tp_count)
    head_ids = lax.axis_index("tp") * device_heads + jnp.arange(device_heads, dtype=jnp.int32)
    slopes = jnp.exp2(
        -8.0 * (head_ids.astype(jnp.float32) + 1.0) / (device_heads * tp_count)
    )
    here_pos = lax.axis_index("ctx") * local_len + jnp.arange(local_len, dtype=jnp.int32)
    here_labels = piece_labels(picture_piece_starts, here_pos)
    heads_first_local = flattened_first(adapter_heads_first)
    heads_pair = lax.all_gather(
        jnp.concatenate([attention_output_weight, heads_first_local], axis=1),
        "tp",
        axis=0,
        tiled=True,
    )
    out_cols = attention_output_weight.shape[1]
    heads_full = pair_gather(heads_pair[:, :out_cols], "shard", 1)
    heads_first_all_flattened = heads_pair[:, out_cols:]
    projection_first_flattened = flattened_first(adapter_projection_first)
    projection_second_flattened = flattened_second(adapter_projection_second)
    heads_first_flattened = flattened_first(adapter_heads_first)
    heads_second_flattened = flattened_second(adapter_heads_second)
    up_first_flattened = flattened_first(adapter_up_first)
    up_second_flattened = flattened_second(adapter_up_second)
    down_first_flattened = flattened_first(adapter_down_first)
    down_second_flattened = flattened_second(adapter_down_second)
    residual = layer_input.reshape(tok_rows, model_width).astype(jnp.float32)
    residual_here = tp_rows(residual, tp_count)
    first_norm = layer_norm(residual, attention_norm_gain, attention_norm_bias)
    first_act = first_norm.astype(jnp.bfloat16)
    _, first_back_full = jax.vjp(
        lambda inputs: layer_norm(inputs, attention_norm_gain, attention_norm_bias), residual_here
    )
    gathered_rows = (
        pair_gather(query_key_value_weight, "shard", 0),
        pair_gather(up_projection_weight, "shard", 0),
    )
    qkv_full = gathered_rows[0].reshape(model_width, 3 * local_width)
    up_full = gathered_rows[1]
    down_full = pair_gather(down_projection_weight, "shard", 1)
    first_low = (matmul(first_act, projection_first_flattened) * select).astype(jnp.bfloat16)
    projected = (
        matmul(first_act, qkv_full) + matmul(first_low, projection_second_flattened)
    ).astype(jnp.bfloat16)
    queries_flat = projected[:, :local_width].reshape(seq_here, local_len, local_width)
    queries = queries_flat.reshape(seq_here, local_len, device_heads, head_width)
    key_rows = projected[:, local_width : 2 * local_width].reshape(seq_here, local_len, local_width)
    value_rows = projected[:, 2 * local_width :].reshape(seq_here, local_len, local_width)
    ctx_count = lax.axis_size("ctx")
    ctx_here = lax.axis_index("ctx")
    blocks = partner_swaps(
        jnp.concatenate([key_rows, value_rows], axis=2), "ctx", ctx_count
    )
    pieces = jnp.concatenate(blocks, axis=1)
    piece_len = pieces.shape[1]
    key_pos = jnp.concatenate(
        [
            (ctx_here ^ offset) * local_len + jnp.arange(local_len, dtype=jnp.int32)
            for offset in range(ctx_count)
        ]
    )
    key_labels = piece_labels(picture_piece_starts, key_pos)
    visible_mask = visible(here_pos, key_pos, here_labels, key_labels)
    piece_keys = pieces[:, :, :local_width].reshape(seq_here, piece_len, device_heads, head_width)
    piece_values = pieces[:, :, local_width:].reshape(
        seq_here, piece_len, device_heads, head_width
    )
    exponent = exponents(queries, piece_keys, here_pos, key_pos, visible_mask, slopes)
    weighted = jnp.einsum(
        "shqk,skhd->sqhd",
        exponent.astype(jnp.bfloat16),
        piece_values,
        preferred_element_type=jnp.float32,
    )
    weighted, totals = (weighted, jnp.sum(exponent, axis=-1))
    per_total = jnp.transpose(totals, (0, 2, 1))[..., None]
    heads_raw = weighted / per_total
    heads_act = heads_raw.reshape(tok_rows, local_width).astype(jnp.bfloat16)
    heads_act_here = lax.all_to_all(heads_act, "tp", 0, 1, tiled=True)
    attn_here = matmul(heads_act_here, heads_full)
    heads_low_here = (matmul(heads_act_here, heads_first_all_flattened) * select_here).astype(
        jnp.bfloat16
    )
    middle_here = residual_here + attn_here + matmul(heads_low_here, heads_second_flattened)
    second_norm, second_back = jax.vjp(
        lambda inputs: layer_norm(inputs, feedforward_norm_gain, feedforward_norm_bias), middle_here
    )
    second_act_here = second_norm.astype(jnp.bfloat16)
    (second_act,) = gather_rows((second_act_here,))
    up_low = (matmul(second_act, up_first_flattened) * select).astype(jnp.bfloat16)
    hidden = matmul(second_act, up_full) + matmul(up_low, up_second_flattened)
    activated, gelu_back = jax.vjp(gelu_tanh, hidden)
    activated = activated.astype(jnp.bfloat16)
    down_part = matmul(activated, down_full)
    down_low_part = matmul(activated, down_first_flattened)
    (ffn_here,) = scatter_rows((down_part,))
    grad_top_low = output_gradient.reshape(tok_rows, model_width)
    grad_top_here = tp_rows(grad_top_low, tp_count).astype(jnp.float32)
    down_back = (matmul_nt(grad_top_low, down_second_flattened) * select).astype(jnp.bfloat16)
    grad_down_in = matmul_tn(activated, down_back)
    grad_activated = matmul_nt(grad_top_low, down_full) + matmul_nt(down_back, down_first_flattened)
    grad_hidden = gelu_back(grad_activated)[0].astype(jnp.bfloat16)
    up_second_gradient = matmul_tn(up_low, grad_hidden)
    ffn_back_part = matmul_nt(grad_hidden, up_full)
    ffn_back_low = matmul_nt(grad_hidden, up_second_flattened)
    back_here, back_low_here, ffn_low_here = scatter_rows(
        (ffn_back_part, ffn_back_low, down_low_part)
    )
    up_back_here = (back_low_here * select_here).astype(jnp.bfloat16)
    down_low_here = (ffn_low_here * select_here).astype(jnp.bfloat16)
    result_here = (middle_here + ffn_here + matmul(down_low_here, down_second_flattened)).astype(
        jnp.bfloat16
    )
    (result_rows,) = gather_rows((result_here,))
    layer_out = result_rows.reshape(layer_input.shape)
    grad_second = back_here + matmul_nt(up_back_here, up_first_flattened)
    grad_middle_here = grad_top_here + second_back(grad_second)[0]
    grad_middle_low_here = grad_middle_here.astype(jnp.bfloat16)
    heads_back_here = (matmul_nt(grad_middle_low_here, heads_second_flattened) * select_here).astype(
        jnp.bfloat16
    )
    low_rows = partner_gather_rows(
        jnp.concatenate([down_low_here, up_back_here, heads_back_here], axis=1), "tp"
    )
    down_low, up_back, heads_back = split_columns(low_rows, [rank_width * adapter_tables] * 3)
    down_second_gradient = matmul_tn(down_low, grad_top_low)
    grad_up_in = matmul_tn(second_act, up_back)
    grad_heads_in = matmul_tn(heads_act, heads_back)
    heads_second_gradient = matmul_tn(heads_low_here, grad_middle_low_here)
    early_terms = narrow_psum(
        (
            unflat_in(grad_heads_in, adapter_tables),
            unflat_in(grad_up_in, adapter_tables),
            up_second_gradient.reshape(adapter_up_second.shape),
            unflat_in(grad_down_in, adapter_tables),
            down_second_gradient.reshape(adapter_down_second.shape),
        ),
        ("shard", "ctx"),
    )
    heads_second_total = narrow_psum(
        heads_second_gradient.reshape(adapter_heads_second.shape), ("shard", "ctx", "tp")
    )
    grad_heads_here = (
        matmul_nt(grad_middle_low_here, heads_full)
        + matmul_nt(heads_back_here, heads_first_all_flattened)
    ).astype(jnp.bfloat16)
    grad_heads = lax.all_to_all(grad_heads_here, "tp", 1, 0, tiled=True)
    grad_heads_wide = grad_heads.reshape(seq_here, local_len, device_heads, head_width).astype(
        jnp.float32
    )
    scaled_grad = (grad_heads_wide / per_total).astype(jnp.bfloat16)
    row_delta = jnp.sum(grad_heads_wide * heads_raw, axis=-1) / per_total[..., 0]
    grad_queries, grad_keyrows, grad_valrows = block_grads(
        queries,
        scaled_grad,
        row_delta,
        piece_keys,
        piece_values,
        here_pos,
        key_pos,
        visible_mask,
        slopes,
    )
    grad_kv = jnp.concatenate(
        [
            grad_keyrows.reshape(seq_here, ctx_count, local_len, local_width),
            grad_valrows.reshape(seq_here, ctx_count, local_len, local_width),
        ],
        axis=3,
    )
    grad_kv_here = grad_kv[:, 0]
    for offset in range(1, ctx_count):
        pairs = [(index, index ^ offset) for index in range(ctx_count)]
        grad_kv_here = grad_kv_here + lax.ppermute(
            grad_kv[:, offset].astype(jnp.bfloat16), "ctx", pairs
        ).astype(jnp.float32)
    grad_keys_all = grad_kv_here[:, :, :local_width]
    grad_values_all = grad_kv_here[:, :, local_width:]
    grad_projected = jnp.concatenate(
        [
            grad_queries.reshape(tok_rows, local_width),
            grad_keys_all.reshape(tok_rows, local_width),
            grad_values_all.reshape(tok_rows, local_width),
        ],
        axis=1,
    ).astype(jnp.bfloat16)
    projection_second_gradient = matmul_tn(first_low, grad_projected)
    attn_back_part = matmul_nt(grad_projected, qkv_full)
    attn_back_low = matmul_nt(grad_projected, projection_second_flattened)
    low_blocks = jnp.stack(partner_swaps(attn_back_low, "tp", tp_count))
    low_owners = jnp.bitwise_xor(lax.axis_index("tp"), jnp.arange(tp_count, dtype=jnp.int32))
    low_total = jnp.sum(jnp.take(low_blocks, low_owners, axis=0), axis=0)
    select_late = lax.optimization_barrier(select)
    qkv_back = (low_total * select_late).astype(jnp.bfloat16)
    grad_qkv_in = matmul_tn(first_act, qkv_back)
    late_terms = butterfly_sum(
        (
            unflat_in(grad_qkv_in, adapter_tables),
            projection_second_gradient.reshape(adapter_projection_second.shape),
        ),
        ("shard", "ctx"),
    )
    first_here, first_low_here = scatter_rows((attn_back_part, attn_back_low))
    select_later = lax.optimization_barrier(select_here)
    qkv_back_here = (first_low_here * select_later).astype(jnp.bfloat16)
    grad_first = first_here + matmul_nt(qkv_back_here, projection_first_flattened)
    input_here = (grad_middle_here + first_back_full(grad_first)[0]).astype(jnp.bfloat16)
    (input_rows,) = gather_rows((input_here,))
    input_grad = input_rows.reshape(layer_input.shape)
    return (
        layer_out,
        input_grad,
        late_terms[0],
        late_terms[1],
        early_terms[0],
        heads_second_total,
        early_terms[1],
        early_terms[2],
        early_terms[3],
        early_terms[4],
    )


def solution(mesh):
    placed = (
        P("shard", "ctx", None),
        P("shard", "ctx", None),
        P("shard", None),
        P("shard"),
        P(),
        P(),
        P(),
        P(),
        P("shard", None, "tp"),
        P("tp", "shard"),
        P("shard", "tp"),
        P("tp", "shard"),
        P(),
        P(None, None, None, "tp"),
        P(None, "tp", None),
        P(),
        P(),
        P(None, None, "tp"),
        P(None, "tp", None),
        P(),
    )
    return jax.shard_map(
        layer_body,
        mesh=mesh,
        in_specs=placed,
        out_specs=(
            P("shard", "ctx", None),
            P("shard", "ctx", None),
            P(),
            P(None, None, None, "tp"),
            P(None, "tp", None),
            P(),
            P(),
            P(None, None, "tp"),
            P(None, "tp", None),
            P(),
        ),
        check_vma=False,
    )
```

```python
import jax
import jax.numpy as jnp
from jax import lax
from jax.sharding import PartitionSpec as P

HD = 128
PIC = 256


NORM_EPS = 1e-05


def layer_norm(inputs, gains, biases):
    average = jnp.mean(inputs, axis=-1, keepdims=True)
    centred = inputs - average
    spread = jnp.mean(centred * centred, axis=-1, keepdims=True)
    return centred * lax.rsqrt(spread + NORM_EPS) * gains + biases


def gelu_tanh(inputs):
    return (
        0.5
        * inputs
        * (1.0 + jnp.tanh(0.7978845608028654 * (inputs + 0.044715 * inputs * inputs * inputs)))
    )


def flattened_first(adapter_mat):
    adapter_tables, inner_dim, rank_width = adapter_mat.shape
    return jnp.transpose(adapter_mat, (1, 0, 2)).reshape(inner_dim, adapter_tables * rank_width)


def flattened_second(adapter_mat):
    return adapter_mat.reshape(adapter_mat.shape[0] * adapter_mat.shape[1], -1)


def unflat_in(grad_flat, adapter_tables):
    inner_dim = grad_flat.shape[0]
    return jnp.transpose(grad_flat.reshape(inner_dim, adapter_tables, -1), (1, 0, 2))


def matmul(left_mat, right_mat):
    return jnp.dot(left_mat, right_mat, preferred_element_type=jnp.float32)


def matmul_tn(left_mat, right_mat):
    return lax.dot_general(
        left_mat, right_mat, (((0,), (0,)), ((), ())), preferred_element_type=jnp.float32
    )


def matmul_nt(left_mat, right_mat):
    return lax.dot_general(
        left_mat, right_mat, (((1,), (1,)), ((), ())), preferred_element_type=jnp.float32
    )


def piece_labels(starts, positions):
    inside = (positions[None, None, :] >= starts[:, :, None]) & (
        positions[None, None, :] < starts[:, :, None] + PIC
    )
    labels = jnp.arange(1, starts.shape[1] + 1, dtype=jnp.int32)
    return jnp.sum(jnp.where(inside, labels[None, :, None], 0), axis=1)


def visible(query_pos, key_pos, query_labels, key_labels):
    causal = key_pos[None, None, :] <= query_pos[None, :, None]
    shared = (query_labels[:, :, None] == key_labels[:, None, :]) & (query_labels[:, :, None] > 0)
    return causal | shared


def exponents(queries, key_rows, query_pos, key_pos, visible_mask, slopes):
    score_scale = queries.shape[-1] ** (-0.5)
    logits = (
        jnp.einsum("sqhd,skhd->shqk", queries, key_rows, preferred_element_type=jnp.float32)
        * score_scale
    )
    distance = jnp.abs(query_pos[:, None] - key_pos[None, :]).astype(jnp.float32)
    logits = logits - slopes[None, :, None, None] * distance[None, None]
    return jnp.where(visible_mask[:, None], jnp.exp(logits), 0.0)


def block_grads(
    queries, scaled_grad, row_delta, key_rows, value_rows, query_pos, key_pos, visible_mask, slopes
):
    score_scale = queries.shape[-1] ** (-0.5)
    exponent = exponents(queries, key_rows, query_pos, key_pos, visible_mask, slopes)
    products_gv = jnp.einsum(
        "sqhd,skhd->shqk", scaled_grad, value_rows, preferred_element_type=jnp.float32
    )
    grad_logits = (
        exponent * (products_gv - jnp.transpose(row_delta, (0, 2, 1))[..., None])
    ).astype(jnp.bfloat16)
    grad_queries = (
        jnp.einsum("shqk,skhd->sqhd", grad_logits, key_rows, preferred_element_type=jnp.float32)
        * score_scale
    )
    grad_keyrows = (
        jnp.einsum("shqk,sqhd->skhd", grad_logits, queries, preferred_element_type=jnp.float32)
        * score_scale
    )
    grad_valrows = jnp.einsum(
        "shqk,sqhd->skhd",
        exponent.astype(jnp.bfloat16),
        scaled_grad,
        preferred_element_type=jnp.float32,
    )
    return (grad_queries, grad_keyrows, grad_valrows)


def partner_swaps(block, axis_name, axis_count):
    received = [block]
    for offset in range(1, axis_count):
        pairs = [(index, index ^ offset) for index in range(axis_count)]
        received.append(lax.ppermute(block, axis_name, pairs))
    return received


def pair_gather(block, axis_name, axis):
    if lax.axis_size(axis_name) != 2:
        return lax.all_gather(block, axis_name, axis=axis, tiled=True)
    other = lax.ppermute(block, axis_name, [(0, 1), (1, 0)])
    first = lax.axis_index(axis_name) == 0
    low = jnp.where(first, block, other)
    high = jnp.where(first, other, block)
    return jnp.concatenate([low, high], axis=axis)


def butterfly_sum(values, axis_names):
    leaves, tree = jax.tree.flatten(values)
    packed = jnp.concatenate([leaf.reshape(-1) for leaf in leaves])
    for axis_name in axis_names:
        axis_count = lax.axis_size(axis_name)
        step = 1
        while step < axis_count:
            pairs = [(index, index ^ step) for index in range(axis_count)]
            narrow = packed.astype(jnp.bfloat16)
            packed = narrow.astype(jnp.float32) + lax.ppermute(narrow, axis_name, pairs).astype(
                jnp.float32
            )
            step *= 2
    parts, offset = [], 0
    for leaf in leaves:
        parts.append(packed[offset : offset + leaf.size].reshape(leaf.shape))
        offset += leaf.size
    return jax.tree.unflatten(tree, parts)


def partner_gather_rows(rows_here, axis_name):
    axis_count = lax.axis_size(axis_name)
    blocks = jnp.stack(partner_swaps(rows_here, axis_name, axis_count))
    owners = jnp.bitwise_xor(
        lax.axis_index(axis_name), jnp.arange(axis_count, dtype=jnp.int32)
    )
    ordered = jnp.take(blocks, owners, axis=0)
    return ordered.reshape(axis_count * rows_here.shape[0], *rows_here.shape[1:])


def narrow_psum(values, axis_names):
    summed = lax.psum(jax.tree.map(lambda value: value.astype(jnp.bfloat16), values), axis_names)
    return jax.tree.map(lambda value: value.astype(jnp.float32), summed)


def tp_rows(rows_array, tp_count):
    chunk = rows_array.shape[0] // tp_count
    return lax.dynamic_slice_in_dim(rows_array, lax.axis_index("tp") * chunk, chunk, axis=0)


def scatter_rows(partials):
    widths = [part.shape[1] for part in partials]
    joined = lax.psum_scatter(
        jnp.concatenate(partials, axis=1).astype(jnp.bfloat16),
        "tp",
        scatter_dimension=0,
        tiled=True,
    )
    return split_columns(joined.astype(jnp.float32), widths)


def gather_rows(rows_here):
    widths = [part.shape[1] for part in rows_here]
    joined = lax.all_gather(jnp.concatenate(rows_here, axis=1), "tp", axis=0, tiled=True)
    return split_columns(joined, widths)


def split_columns(joined, widths):
    parts, offset = [], 0
    for width in widths:
        parts.append(joined[:, offset : offset + width])
        offset += width
    return tuple(parts)


def layer_body(
    layer_input,
    output_gradient,
    picture_piece_starts,
    sequence_adapter_index,
    attention_norm_gain,
    attention_norm_bias,
    feedforward_norm_gain,
    feedforward_norm_bias,
    query_key_value_weight,
    attention_output_weight,
    up_projection_weight,
    down_projection_weight,
    adapter_projection_first,
    adapter_projection_second,
    adapter_heads_first,
    adapter_heads_second,
    adapter_up_first,
    adapter_up_second,
    adapter_down_first,
    adapter_down_second,
):
    seq_here, local_len, model_width = layer_input.shape
    tok_rows = seq_here * local_len
    tp_count = lax.axis_size("tp")
    adapter_tables = adapter_projection_first.shape[0]
    rank_width = adapter_projection_first.shape[2]
    head_width = HD
    device_heads = adapter_projection_second.shape[-1] // head_width
    local_width = device_heads * head_width
    columns = jnp.arange(adapter_tables * rank_width, dtype=jnp.int32) // rank_width
    chosen = (sequence_adapter_index[:, None] == columns[None, :]).astype(jnp.float32)
    select = jnp.broadcast_to(
        chosen[:, None, :], (seq_here, local_len, adapter_tables * rank_width)
    ).reshape(tok_rows, adapter_tables * rank_width)
    select_here = tp_rows(select, tp_count)
    head_ids = lax.axis_index("tp") * device_heads + jnp.arange(device_heads, dtype=jnp.int32)
    slopes = jnp.exp2(
        -8.0 * (head_ids.astype(jnp.float32) + 1.0) / (device_heads * tp_count)
    )
    here_pos = lax.axis_index("ctx") * local_len + jnp.arange(local_len, dtype=jnp.int32)
    here_labels = piece_labels(picture_piece_starts, here_pos)
    heads_first_local = flattened_first(adapter_heads_first)
    heads_pair = lax.all_gather(
        jnp.concatenate([attention_output_weight, heads_first_local], axis=1),
        "tp",
        axis=0,
        tiled=True,
    )
    out_cols = attention_output_weight.shape[1]
    heads_full = pair_gather(heads_pair[:, :out_cols], "shard", 1)
    heads_first_all_flattened = heads_pair[:, out_cols:]
    projection_first_flattened = flattened_first(adapter_projection_first)
    projection_second_flattened = flattened_second(adapter_projection_second)
    heads_first_flattened = flattened_first(adapter_heads_first)
    heads_second_flattened = flattened_second(adapter_heads_second)
    up_first_flattened = flattened_first(adapter_up_first)
    up_second_flattened = flattened_second(adapter_up_second)
    down_first_flattened = flattened_first(adapter_down_first)
    down_second_flattened = flattened_second(adapter_down_second)
    residual = layer_input.reshape(tok_rows, model_width).astype(jnp.float32)
    residual_here = tp_rows(residual, tp_count)
    first_norm = layer_norm(residual, attention_norm_gain, attention_norm_bias)
    first_act = first_norm.astype(jnp.bfloat16)
    _, first_back_full = jax.vjp(
        lambda inputs: layer_norm(inputs, attention_norm_gain, attention_norm_bias), residual_here
    )
    gathered_rows = (
        pair_gather(query_key_value_weight, "shard", 0),
        pair_gather(up_projection_weight, "shard", 0),
    )
    qkv_full = gathered_rows[0].reshape(model_width, 3 * local_width)
    up_full = gathered_rows[1]
    down_full = pair_gather(down_projection_weight, "shard", 1)
    first_low = (matmul(first_act, projection_first_flattened) * select).astype(jnp.bfloat16)
    projected = (
        matmul(first_act, qkv_full) + matmul(first_low, projection_second_flattened)
    ).astype(jnp.bfloat16)
    queries_flat = projected[:, :local_width].reshape(seq_here, local_len, local_width)
    queries = queries_flat.reshape(seq_here, local_len, device_heads, head_width)
    key_rows = projected[:, local_width : 2 * local_width].reshape(seq_here, local_len, local_width)
    value_rows = projected[:, 2 * local_width :].reshape(seq_here, local_len, local_width)
    ctx_count = lax.axis_size("ctx")
    ctx_here = lax.axis_index("ctx")
    blocks = partner_swaps(
        jnp.concatenate([key_rows, value_rows], axis=2), "ctx", ctx_count
    )
    pieces = jnp.concatenate(blocks, axis=1)
    piece_len = pieces.shape[1]
    key_pos = jnp.concatenate(
        [
            (ctx_here ^ offset) * local_len + jnp.arange(local_len, dtype=jnp.int32)
            for offset in range(ctx_count)
        ]
    )
    key_labels = piece_labels(picture_piece_starts, key_pos)
    visible_mask = visible(here_pos, key_pos, here_labels, key_labels)
    piece_keys = pieces[:, :, :local_width].reshape(seq_here, piece_len, device_heads, head_width)
    piece_values = pieces[:, :, local_width:].reshape(
        seq_here, piece_len, device_heads, head_width
    )
    exponent = exponents(queries, piece_keys, here_pos, key_pos, visible_mask, slopes)
    weighted = jnp.einsum(
        "shqk,skhd->sqhd",
        exponent.astype(jnp.bfloat16),
        piece_values,
        preferred_element_type=jnp.float32,
    )
    weighted, totals = (weighted, jnp.sum(exponent, axis=-1))
    per_total = jnp.transpose(totals, (0, 2, 1))[..., None]
    heads_raw = weighted / per_total
    heads_act = heads_raw.reshape(tok_rows, local_width).astype(jnp.bfloat16)
    heads_act_here = lax.all_to_all(heads_act, "tp", 0, 1, tiled=True)
    attn_here = matmul(heads_act_here, heads_full)
    heads_low_here = (matmul(heads_act_here, heads_first_all_flattened) * select_here).astype(
        jnp.bfloat16
    )
    middle_here = residual_here + attn_here + matmul(heads_low_here, heads_second_flattened)
    second_norm, second_back = jax.vjp(
        lambda inputs: layer_norm(inputs, feedforward_norm_gain, feedforward_norm_bias), middle_here
    )
    second_act_here = second_norm.astype(jnp.bfloat16)
    (second_act,) = gather_rows((second_act_here,))
    up_low = (matmul(second_act, up_first_flattened) * select).astype(jnp.bfloat16)
    hidden = matmul(second_act, up_full) + matmul(up_low, up_second_flattened)
    activated, gelu_back = jax.vjp(gelu_tanh, hidden)
    activated = activated.astype(jnp.bfloat16)
    down_part = matmul(activated, down_full)
    down_low_part = matmul(activated, down_first_flattened)
    (ffn_here,) = scatter_rows((down_part,))
    grad_top_low = output_gradient.reshape(tok_rows, model_width)
    grad_top_here = tp_rows(grad_top_low, tp_count).astype(jnp.float32)
    down_back = (matmul_nt(grad_top_low, down_second_flattened) * select).astype(jnp.bfloat16)
    grad_down_in = matmul_tn(activated, down_back)
    grad_activated = matmul_nt(grad_top_low, down_full) + matmul_nt(down_back, down_first_flattened)
    grad_hidden = gelu_back(grad_activated)[0].astype(jnp.bfloat16)
    up_second_gradient = matmul_tn(up_low, grad_hidden)
    ffn_back_part = matmul_nt(grad_hidden, up_full)
    ffn_back_low = matmul_nt(grad_hidden, up_second_flattened)
    back_here, back_low_here, ffn_low_here = scatter_rows(
        (ffn_back_part, ffn_back_low, down_low_part)
    )
    up_back_here = (back_low_here * select_here).astype(jnp.bfloat16)
    down_low_here = (ffn_low_here * select_here).astype(jnp.bfloat16)
    result_here = (middle_here + ffn_here + matmul(down_low_here, down_second_flattened)).astype(
        jnp.bfloat16
    )
    (result_rows,) = gather_rows((result_here,))
    layer_out = result_rows.reshape(layer_input.shape)
    grad_second = back_here + matmul_nt(up_back_here, up_first_flattened)
    grad_middle_here = grad_top_here + second_back(grad_second)[0]
    grad_middle_low_here = grad_middle_here.astype(jnp.bfloat16)
    heads_back_here = (matmul_nt(grad_middle_low_here, heads_second_flattened) * select_here).astype(
        jnp.bfloat16
    )
    low_rows = partner_gather_rows(
        jnp.concatenate([down_low_here, up_back_here, heads_back_here], axis=1), "tp"
    )
    down_low, up_back, heads_back = split_columns(low_rows, [rank_width * adapter_tables] * 3)
    down_second_gradient = matmul_tn(down_low, grad_top_low)
    grad_up_in = matmul_tn(second_act, up_back)
    grad_heads_in = matmul_tn(heads_act, heads_back)
    heads_second_gradient = matmul_tn(heads_low_here, grad_middle_low_here)
    heads_blocks = jnp.stack(
        partner_swaps(heads_second_gradient.astype(jnp.bfloat16), "tp", tp_count)
    )
    heads_owners = jnp.bitwise_xor(lax.axis_index("tp"), jnp.arange(tp_count, dtype=jnp.int32))
    heads_tp_total = jnp.sum(
        jnp.take(heads_blocks, heads_owners, axis=0).astype(jnp.float32), axis=0
    )
    early_terms = narrow_psum(
        (
            unflat_in(grad_heads_in, adapter_tables),
            unflat_in(grad_up_in, adapter_tables),
            up_second_gradient.reshape(adapter_up_second.shape),
            unflat_in(grad_down_in, adapter_tables),
            down_second_gradient.reshape(adapter_down_second.shape),
            heads_tp_total.reshape(adapter_heads_second.shape),
        ),
        ("shard", "ctx"),
    )
    heads_second_total = early_terms[5]
    grad_heads_here = (
        matmul_nt(grad_middle_low_here, heads_full)
        + matmul_nt(heads_back_here, heads_first_all_flattened)
    ).astype(jnp.bfloat16)
    grad_heads = lax.all_to_all(grad_heads_here, "tp", 1, 0, tiled=True)
    grad_heads_wide = grad_heads.reshape(seq_here, local_len, device_heads, head_width).astype(
        jnp.float32
    )
    scaled_grad = (grad_heads_wide / per_total).astype(jnp.bfloat16)
    row_delta = jnp.sum(grad_heads_wide * heads_raw, axis=-1) / per_total[..., 0]
    grad_queries, grad_keyrows, grad_valrows = block_grads(
        queries,
        scaled_grad,
        row_delta,
        piece_keys,
        piece_values,
        here_pos,
        key_pos,
        visible_mask,
        slopes,
    )
    grad_kv = jnp.concatenate(
        [
            grad_keyrows.reshape(seq_here, ctx_count, local_len, local_width),
            grad_valrows.reshape(seq_here, ctx_count, local_len, local_width),
        ],
        axis=3,
    )
    grad_kv_here = grad_kv[:, 0]
    for offset in range(1, ctx_count):
        pairs = [(index, index ^ offset) for index in range(ctx_count)]
        grad_kv_here = grad_kv_here + lax.ppermute(
            grad_kv[:, offset].astype(jnp.bfloat16), "ctx", pairs
        ).astype(jnp.float32)
    grad_keys_all = grad_kv_here[:, :, :local_width]
    grad_values_all = grad_kv_here[:, :, local_width:]
    grad_projected = jnp.concatenate(
        [
            grad_queries.reshape(tok_rows, local_width),
            grad_keys_all.reshape(tok_rows, local_width),
            grad_values_all.reshape(tok_rows, local_width),
        ],
        axis=1,
    ).astype(jnp.bfloat16)
    projection_second_gradient = matmul_tn(first_low, grad_projected)
    attn_back_part = matmul_nt(grad_projected, qkv_full)
    attn_back_low = matmul_nt(grad_projected, projection_second_flattened)
    low_blocks = jnp.stack(partner_swaps(attn_back_low, "tp", tp_count))
    low_owners = jnp.bitwise_xor(lax.axis_index("tp"), jnp.arange(tp_count, dtype=jnp.int32))
    low_total = jnp.sum(jnp.take(low_blocks, low_owners, axis=0), axis=0)
    select_late = lax.optimization_barrier(select)
    qkv_back = (low_total * select_late).astype(jnp.bfloat16)
    grad_qkv_in = matmul_tn(first_act, qkv_back)
    late_terms = butterfly_sum(
        (
            unflat_in(grad_qkv_in, adapter_tables),
            projection_second_gradient.reshape(adapter_projection_second.shape),
        ),
        ("shard", "ctx"),
    )
    first_here, first_low_here = scatter_rows((attn_back_part, attn_back_low))
    select_later = lax.optimization_barrier(select_here)
    qkv_back_here = (first_low_here * select_later).astype(jnp.bfloat16)
    grad_first = first_here + matmul_nt(qkv_back_here, projection_first_flattened)
    input_here = (grad_middle_here + first_back_full(grad_first)[0]).astype(jnp.bfloat16)
    (input_rows,) = gather_rows((input_here,))
    input_grad = input_rows.reshape(layer_input.shape)
    return (
        layer_out,
        input_grad,
        late_terms[0],
        late_terms[1],
        early_terms[0],
        heads_second_total,
        early_terms[1],
        early_terms[2],
        early_terms[3],
        early_terms[4],
    )


def solution(mesh):
    placed = (
        P("shard", "ctx", None),
        P("shard", "ctx", None),
        P("shard", None),
        P("shard"),
        P(),
        P(),
        P(),
        P(),
        P("shard", None, "tp"),
        P("tp", "shard"),
        P("shard", "tp"),
        P("tp", "shard"),
        P(),
        P(None, None, None, "tp"),
        P(None, "tp", None),
        P(),
        P(),
        P(None, None, "tp"),
        P(None, "tp", None),
        P(),
    )
    return jax.shard_map(
        layer_body,
        mesh=mesh,
        in_specs=placed,
        out_specs=(
            P("shard", "ctx", None),
            P("shard", "ctx", None),
            P(),
            P(None, None, None, "tp"),
            P(None, "tp", None),
            P(),
            P(),
            P(None, None, "tp"),
            P(None, "tp", None),
            P(),
        ),
        check_vma=False,
    )
```

```python
import jax
import jax.numpy as jnp
from jax import lax
from jax.sharding import PartitionSpec as P

HD = 128
PIC = 256


NORM_EPS = 1e-05


def layer_norm(inputs, gains, biases):
    average = jnp.mean(inputs, axis=-1, keepdims=True)
    centred = inputs - average
    spread = jnp.mean(centred * centred, axis=-1, keepdims=True)
    return centred * lax.rsqrt(spread + NORM_EPS) * gains + biases


def gelu_tanh(inputs):
    return (
        0.5
        * inputs
        * (1.0 + jnp.tanh(0.7978845608028654 * (inputs + 0.044715 * inputs * inputs * inputs)))
    )


def flattened_first(adapter_mat):
    adapter_tables, inner_dim, rank_width = adapter_mat.shape
    return jnp.transpose(adapter_mat, (1, 0, 2)).reshape(inner_dim, adapter_tables * rank_width)


def flattened_second(adapter_mat):
    return adapter_mat.reshape(adapter_mat.shape[0] * adapter_mat.shape[1], -1)


def unflat_in(grad_flat, adapter_tables):
    inner_dim = grad_flat.shape[0]
    return jnp.transpose(grad_flat.reshape(inner_dim, adapter_tables, -1), (1, 0, 2))


def matmul(left_mat, right_mat):
    return jnp.dot(left_mat, right_mat, preferred_element_type=jnp.float32)


def matmul_tn(left_mat, right_mat):
    return lax.dot_general(
        left_mat, right_mat, (((0,), (0,)), ((), ())), preferred_element_type=jnp.float32
    )


def matmul_nt(left_mat, right_mat):
    return lax.dot_general(
        left_mat, right_mat, (((1,), (1,)), ((), ())), preferred_element_type=jnp.float32
    )


def piece_labels(starts, positions):
    inside = (positions[None, None, :] >= starts[:, :, None]) & (
        positions[None, None, :] < starts[:, :, None] + PIC
    )
    labels = jnp.arange(1, starts.shape[1] + 1, dtype=jnp.int32)
    return jnp.sum(jnp.where(inside, labels[None, :, None], 0), axis=1)


def visible(query_pos, key_pos, query_labels, key_labels):
    causal = key_pos[None, None, :] <= query_pos[None, :, None]
    shared = (query_labels[:, :, None] == key_labels[:, None, :]) & (query_labels[:, :, None] > 0)
    return causal | shared


def exponents(queries, key_rows, query_pos, key_pos, visible_mask, slopes):
    score_scale = queries.shape[-1] ** (-0.5)
    logits = (
        jnp.einsum("sqhd,skhd->shqk", queries, key_rows, preferred_element_type=jnp.float32)
        * score_scale
    )
    distance = jnp.abs(query_pos[:, None] - key_pos[None, :]).astype(jnp.float32)
    logits = logits - slopes[None, :, None, None] * distance[None, None]
    return jnp.where(visible_mask[:, None], jnp.exp(logits), 0.0)


def block_grads(
    queries, scaled_grad, row_delta, key_rows, value_rows, query_pos, key_pos, visible_mask, slopes
):
    score_scale = queries.shape[-1] ** (-0.5)
    exponent = exponents(queries, key_rows, query_pos, key_pos, visible_mask, slopes)
    products_gv = jnp.einsum(
        "sqhd,skhd->shqk", scaled_grad, value_rows, preferred_element_type=jnp.float32
    )
    grad_logits = (
        exponent * (products_gv - jnp.transpose(row_delta, (0, 2, 1))[..., None])
    ).astype(jnp.bfloat16)
    grad_queries = (
        jnp.einsum("shqk,skhd->sqhd", grad_logits, key_rows, preferred_element_type=jnp.float32)
        * score_scale
    )
    grad_keyrows = (
        jnp.einsum("shqk,sqhd->skhd", grad_logits, queries, preferred_element_type=jnp.float32)
        * score_scale
    )
    grad_valrows = jnp.einsum(
        "shqk,sqhd->skhd",
        exponent.astype(jnp.bfloat16),
        scaled_grad,
        preferred_element_type=jnp.float32,
    )
    return (grad_queries, grad_keyrows, grad_valrows)


def partner_swaps(block, axis_name, axis_count):
    received = [block]
    for offset in range(1, axis_count):
        pairs = [(index, index ^ offset) for index in range(axis_count)]
        received.append(lax.ppermute(block, axis_name, pairs))
    return received


def pair_gather(block, axis_name, axis):
    if lax.axis_size(axis_name) != 2:
        return lax.all_gather(block, axis_name, axis=axis, tiled=True)
    other = lax.ppermute(block, axis_name, [(0, 1), (1, 0)])
    first = lax.axis_index(axis_name) == 0
    low = jnp.where(first, block, other)
    high = jnp.where(first, other, block)
    return jnp.concatenate([low, high], axis=axis)


def butterfly_sum(values, axis_names):
    leaves, tree = jax.tree.flatten(values)
    packed = jnp.concatenate([leaf.reshape(-1) for leaf in leaves])
    for axis_name in axis_names:
        axis_count = lax.axis_size(axis_name)
        step = 1
        while step < axis_count:
            pairs = [(index, index ^ step) for index in range(axis_count)]
            packed = packed + lax.ppermute(packed, axis_name, pairs)
            step *= 2
    parts, offset = [], 0
    for leaf in leaves:
        parts.append(packed[offset : offset + leaf.size].reshape(leaf.shape))
        offset += leaf.size
    return jax.tree.unflatten(tree, parts)


def partner_gather_rows(rows_here, axis_name):
    axis_count = lax.axis_size(axis_name)
    blocks = jnp.stack(partner_swaps(rows_here, axis_name, axis_count))
    owners = jnp.bitwise_xor(
        lax.axis_index(axis_name), jnp.arange(axis_count, dtype=jnp.int32)
    )
    ordered = jnp.take(blocks, owners, axis=0)
    return ordered.reshape(axis_count * rows_here.shape[0], *rows_here.shape[1:])


def narrow_psum(values, axis_names):
    summed = lax.psum(jax.tree.map(lambda value: value.astype(jnp.bfloat16), values), axis_names)
    return jax.tree.map(lambda value: value.astype(jnp.float32), summed)


def tp_rows(rows_array, tp_count):
    chunk = rows_array.shape[0] // tp_count
    return lax.dynamic_slice_in_dim(rows_array, lax.axis_index("tp") * chunk, chunk, axis=0)


def scatter_rows(partials):
    widths = [part.shape[1] for part in partials]
    joined = lax.psum_scatter(
        jnp.concatenate(partials, axis=1).astype(jnp.bfloat16),
        "tp",
        scatter_dimension=0,
        tiled=True,
    )
    return split_columns(joined.astype(jnp.float32), widths)


def gather_rows(rows_here):
    widths = [part.shape[1] for part in rows_here]
    joined = lax.all_gather(jnp.concatenate(rows_here, axis=1), "tp", axis=0, tiled=True)
    return split_columns(joined, widths)


def split_columns(joined, widths):
    parts, offset = [], 0
    for width in widths:
        parts.append(joined[:, offset : offset + width])
        offset += width
    return tuple(parts)


def layer_body(
    layer_input,
    output_gradient,
    picture_piece_starts,
    sequence_adapter_index,
    attention_norm_gain,
    attention_norm_bias,
    feedforward_norm_gain,
    feedforward_norm_bias,
    query_key_value_weight,
    attention_output_weight,
    up_projection_weight,
    down_projection_weight,
    adapter_projection_first,
    adapter_projection_second,
    adapter_heads_first,
    adapter_heads_second,
    adapter_up_first,
    adapter_up_second,
    adapter_down_first,
    adapter_down_second,
):
    seq_here, local_len, model_width = layer_input.shape
    tok_rows = seq_here * local_len
    tp_count = lax.axis_size("tp")
    adapter_tables = adapter_projection_first.shape[0]
    rank_width = adapter_projection_first.shape[2]
    head_width = HD
    device_heads = adapter_projection_second.shape[-1] // head_width
    local_width = device_heads * head_width
    columns = jnp.arange(adapter_tables * rank_width, dtype=jnp.int32) // rank_width
    chosen = (sequence_adapter_index[:, None] == columns[None, :]).astype(jnp.float32)
    select = jnp.broadcast_to(
        chosen[:, None, :], (seq_here, local_len, adapter_tables * rank_width)
    ).reshape(tok_rows, adapter_tables * rank_width)
    select_here = tp_rows(select, tp_count)
    head_ids = lax.axis_index("tp") * device_heads + jnp.arange(device_heads, dtype=jnp.int32)
    slopes = jnp.exp2(
        -8.0 * (head_ids.astype(jnp.float32) + 1.0) / (device_heads * tp_count)
    )
    here_pos = lax.axis_index("ctx") * local_len + jnp.arange(local_len, dtype=jnp.int32)
    here_labels = piece_labels(picture_piece_starts, here_pos)
    heads_first_local = flattened_first(adapter_heads_first)
    heads_pair = lax.all_gather(
        jnp.concatenate([attention_output_weight, heads_first_local], axis=1),
        "tp",
        axis=0,
        tiled=True,
    )
    out_cols = attention_output_weight.shape[1]
    heads_full = pair_gather(heads_pair[:, :out_cols], "shard", 1)
    heads_first_all_flattened = heads_pair[:, out_cols:]
    projection_first_flattened = flattened_first(adapter_projection_first)
    projection_second_flattened = flattened_second(adapter_projection_second)
    heads_first_flattened = flattened_first(adapter_heads_first)
    heads_second_flattened = flattened_second(adapter_heads_second)
    up_first_flattened = flattened_first(adapter_up_first)
    up_second_flattened = flattened_second(adapter_up_second)
    down_first_flattened = flattened_first(adapter_down_first)
    down_second_flattened = flattened_second(adapter_down_second)
    residual = layer_input.reshape(tok_rows, model_width).astype(jnp.float32)
    residual_here = tp_rows(residual, tp_count)
    first_norm = layer_norm(residual, attention_norm_gain, attention_norm_bias)
    first_act = first_norm.astype(jnp.bfloat16)
    _, first_back_full = jax.vjp(
        lambda inputs: layer_norm(inputs, attention_norm_gain, attention_norm_bias), residual_here
    )
    gathered_rows = (
        pair_gather(query_key_value_weight, "shard", 0),
        pair_gather(up_projection_weight, "shard", 0),
    )
    qkv_full = gathered_rows[0].reshape(model_width, 3 * local_width)
    up_full = gathered_rows[1]
    down_full = pair_gather(down_projection_weight, "shard", 1)
    first_low = (matmul(first_act, projection_first_flattened) * select).astype(jnp.bfloat16)
    projected = (
        matmul(first_act, qkv_full) + matmul(first_low, projection_second_flattened)
    ).astype(jnp.bfloat16)
    queries_flat = projected[:, :local_width].reshape(seq_here, local_len, local_width)
    queries = queries_flat.reshape(seq_here, local_len, device_heads, head_width)
    key_rows = projected[:, local_width : 2 * local_width].reshape(seq_here, local_len, local_width)
    value_rows = projected[:, 2 * local_width :].reshape(seq_here, local_len, local_width)
    ctx_count = lax.axis_size("ctx")
    ctx_here = lax.axis_index("ctx")
    pieces = lax.all_gather(
        jnp.concatenate([key_rows, value_rows], axis=2), "ctx", axis=1, tiled=True
    )
    piece_len = pieces.shape[1]
    key_pos = jnp.arange(piece_len, dtype=jnp.int32)
    key_labels = piece_labels(picture_piece_starts, key_pos)
    visible_mask = visible(here_pos, key_pos, here_labels, key_labels)
    piece_keys = pieces[:, :, :local_width].reshape(seq_here, piece_len, device_heads, head_width)
    piece_values = pieces[:, :, local_width:].reshape(
        seq_here, piece_len, device_heads, head_width
    )
    exponent = exponents(queries, piece_keys, here_pos, key_pos, visible_mask, slopes)
    weighted = jnp.einsum(
        "shqk,skhd->sqhd",
        exponent.astype(jnp.bfloat16),
        piece_values,
        preferred_element_type=jnp.float32,
    )
    weighted, totals = (weighted, jnp.sum(exponent, axis=-1))
    per_total = jnp.transpose(totals, (0, 2, 1))[..., None]
    heads_raw = weighted / per_total
    heads_act = heads_raw.reshape(tok_rows, local_width).astype(jnp.bfloat16)
    heads_act_here = lax.all_to_all(heads_act, "tp", 0, 1, tiled=True)
    attn_here = matmul(heads_act_here, heads_full)
    heads_low_here = (matmul(heads_act_here, heads_first_all_flattened) * select_here).astype(
        jnp.bfloat16
    )
    middle_here = residual_here + attn_here + matmul(heads_low_here, heads_second_flattened)
    second_norm, second_back = jax.vjp(
        lambda inputs: layer_norm(inputs, feedforward_norm_gain, feedforward_norm_bias), middle_here
    )
    second_act_here = second_norm.astype(jnp.bfloat16)
    (second_act,) = gather_rows((second_act_here,))
    up_low = (matmul(second_act, up_first_flattened) * select).astype(jnp.bfloat16)
    hidden = matmul(second_act, up_full) + matmul(up_low, up_second_flattened)
    activated, gelu_back = jax.vjp(gelu_tanh, hidden)
    activated = activated.astype(jnp.bfloat16)
    down_part = matmul(activated, down_full)
    down_low_part = matmul(activated, down_first_flattened)
    ffn_here, ffn_low_here = scatter_rows((down_part, down_low_part))
    down_low_here = (ffn_low_here * select_here).astype(jnp.bfloat16)
    result_here = (middle_here + ffn_here + matmul(down_low_here, down_second_flattened)).astype(
        jnp.bfloat16
    )
    (result_rows,) = gather_rows((result_here,))
    layer_out = result_rows.reshape(layer_input.shape)
    grad_top_low = output_gradient.reshape(tok_rows, model_width)
    grad_top_here = tp_rows(grad_top_low, tp_count).astype(jnp.float32)
    down_back = (matmul_nt(grad_top_low, down_second_flattened) * select).astype(jnp.bfloat16)
    grad_down_in = matmul_tn(activated, down_back)
    grad_activated = matmul_nt(grad_top_low, down_full) + matmul_nt(down_back, down_first_flattened)
    grad_hidden = gelu_back(grad_activated)[0].astype(jnp.bfloat16)
    up_second_gradient = matmul_tn(up_low, grad_hidden)
    ffn_back_part = matmul_nt(grad_hidden, up_full)
    ffn_back_low = matmul_nt(grad_hidden, up_second_flattened)
    back_here, back_low_here = scatter_rows((ffn_back_part, ffn_back_low))
    up_back_here = (back_low_here * select_here).astype(jnp.bfloat16)
    grad_second = back_here + matmul_nt(up_back_here, up_first_flattened)
    grad_middle_here = grad_top_here + second_back(grad_second)[0]
    grad_middle_low_here = grad_middle_here.astype(jnp.bfloat16)
    heads_back_here = (matmul_nt(grad_middle_low_here, heads_second_flattened) * select_here).astype(
        jnp.bfloat16
    )
    low_rows = partner_gather_rows(
        jnp.concatenate([down_low_here, up_back_here, heads_back_here], axis=1), "tp"
    )
    down_low, up_back, heads_back = split_columns(low_rows, [rank_width * adapter_tables] * 3)
    down_second_gradient = matmul_tn(down_low, grad_top_low)
    grad_up_in = matmul_tn(second_act, up_back)
    grad_heads_in = matmul_tn(heads_act, heads_back)
    heads_second_gradient = matmul_tn(heads_low_here, grad_middle_low_here)
    early_terms = narrow_psum(
        (
            unflat_in(grad_heads_in, adapter_tables),
            unflat_in(grad_up_in, adapter_tables),
            up_second_gradient.reshape(adapter_up_second.shape),
            unflat_in(grad_down_in, adapter_tables),
            down_second_gradient.reshape(adapter_down_second.shape),
        ),
        ("shard", "ctx"),
    )
    heads_second_total = narrow_psum(
        heads_second_gradient.reshape(adapter_heads_second.shape), ("shard", "ctx", "tp")
    )
    grad_heads_here = (
        matmul_nt(grad_middle_low_here, heads_full)
        + matmul_nt(heads_back_here, heads_first_all_flattened)
    ).astype(jnp.bfloat16)
    grad_heads = lax.all_to_all(grad_heads_here, "tp", 1, 0, tiled=True)
    grad_heads_wide = grad_heads.reshape(seq_here, local_len, device_heads, head_width).astype(
        jnp.float32
    )
    scaled_grad = (grad_heads_wide / per_total).astype(jnp.bfloat16)
    row_delta = jnp.sum(grad_heads_wide * heads_raw, axis=-1) / per_total[..., 0]
    grad_queries, grad_keyrows, grad_valrows = block_grads(
        queries,
        scaled_grad,
        row_delta,
        piece_keys,
        piece_values,
        here_pos,
        key_pos,
        visible_mask,
        slopes,
    )
    grad_kv = jnp.concatenate(
        [
            grad_keyrows.reshape(seq_here, ctx_count, local_len, local_width),
            grad_valrows.reshape(seq_here, ctx_count, local_len, local_width),
        ],
        axis=3,
    )
    grad_kv_here = lax.dynamic_index_in_dim(grad_kv, ctx_here, axis=1, keepdims=False)
    for offset in range(1, ctx_count):
        pairs = [(index, index ^ offset) for index in range(ctx_count)]
        block = lax.dynamic_index_in_dim(grad_kv, ctx_here ^ offset, axis=1, keepdims=False)
        grad_kv_here = grad_kv_here + lax.ppermute(
            block.astype(jnp.bfloat16), "ctx", pairs
        ).astype(jnp.float32)
    grad_keys_all = grad_kv_here[:, :, :local_width]
    grad_values_all = grad_kv_here[:, :, local_width:]
    grad_projected = jnp.concatenate(
        [
            grad_queries.reshape(tok_rows, local_width),
            grad_keys_all.reshape(tok_rows, local_width),
            grad_values_all.reshape(tok_rows, local_width),
        ],
        axis=1,
    ).astype(jnp.bfloat16)
    projection_second_gradient = matmul_tn(first_low, grad_projected)
    attn_back_part = matmul_nt(grad_projected, qkv_full)
    attn_back_low = matmul_nt(grad_projected, projection_second_flattened)
    low_blocks = jnp.stack(partner_swaps(attn_back_low, "tp", tp_count))
    low_owners = jnp.bitwise_xor(lax.axis_index("tp"), jnp.arange(tp_count, dtype=jnp.int32))
    low_total = jnp.sum(jnp.take(low_blocks, low_owners, axis=0), axis=0)
    select_late = lax.optimization_barrier(select)
    qkv_back = (low_total * select_late).astype(jnp.bfloat16)
    grad_qkv_in = matmul_tn(first_act, qkv_back)
    late_terms = butterfly_sum(
        (
            unflat_in(grad_qkv_in, adapter_tables),
            projection_second_gradient.reshape(adapter_projection_second.shape),
        ),
        ("shard", "ctx"),
    )
    first_here, first_low_here = scatter_rows((attn_back_part, attn_back_low))
    select_later = lax.optimization_barrier(select_here)
    qkv_back_here = (first_low_here * select_later).astype(jnp.bfloat16)
    grad_first = first_here + matmul_nt(qkv_back_here, projection_first_flattened)
    input_here = (grad_middle_here + first_back_full(grad_first)[0]).astype(jnp.bfloat16)
    (input_rows,) = gather_rows((input_here,))
    input_grad = input_rows.reshape(layer_input.shape)
    return (
        layer_out,
        input_grad,
        late_terms[0],
        late_terms[1],
        early_terms[0],
        heads_second_total,
        early_terms[1],
        early_terms[2],
        early_terms[3],
        early_terms[4],
    )


def solution(mesh):
    placed = (
        P("shard", "ctx", None),
        P("shard", "ctx", None),
        P("shard", None),
        P("shard"),
        P(),
        P(),
        P(),
        P(),
        P("shard", None, "tp"),
        P("tp", "shard"),
        P("shard", "tp"),
        P("tp", "shard"),
        P(),
        P(None, None, None, "tp"),
        P(None, "tp", None),
        P(),
        P(),
        P(None, None, "tp"),
        P(None, "tp", None),
        P(),
    )
    return jax.shard_map(
        layer_body,
        mesh=mesh,
        in_specs=placed,
        out_specs=(
            P("shard", "ctx", None),
            P("shard", "ctx", None),
            P(),
            P(None, None, None, "tp"),
            P(None, "tp", None),
            P(),
            P(),
            P(None, None, "tp"),
            P(None, "tp", None),
            P(),
        ),
        check_vma=False,
    )
```

```python
import jax
import jax.numpy as jnp
from jax import lax
from jax.sharding import PartitionSpec as P

HD = 128
PIC = 256


NORM_EPS = 1e-05


def layer_norm(inputs, gains, biases):
    average = jnp.mean(inputs, axis=-1, keepdims=True)
    centred = inputs - average
    spread = jnp.mean(centred * centred, axis=-1, keepdims=True)
    return centred * lax.rsqrt(spread + NORM_EPS) * gains + biases


def gelu_tanh(inputs):
    return (
        0.5
        * inputs
        * (1.0 + jnp.tanh(0.7978845608028654 * (inputs + 0.044715 * inputs * inputs * inputs)))
    )


def flattened_first(adapter_mat):
    adapter_tables, inner_dim, rank_width = adapter_mat.shape
    return jnp.transpose(adapter_mat, (1, 0, 2)).reshape(inner_dim, adapter_tables * rank_width)


def flattened_second(adapter_mat):
    return adapter_mat.reshape(adapter_mat.shape[0] * adapter_mat.shape[1], -1)


def unflat_in(grad_flat, adapter_tables):
    inner_dim = grad_flat.shape[0]
    return jnp.transpose(grad_flat.reshape(inner_dim, adapter_tables, -1), (1, 0, 2))


def matmul(left_mat, right_mat):
    return jnp.dot(left_mat, right_mat, preferred_element_type=jnp.float32)


def matmul_tn(left_mat, right_mat):
    return lax.dot_general(
        left_mat, right_mat, (((0,), (0,)), ((), ())), preferred_element_type=jnp.float32
    )


def matmul_nt(left_mat, right_mat):
    return lax.dot_general(
        left_mat, right_mat, (((1,), (1,)), ((), ())), preferred_element_type=jnp.float32
    )


def piece_labels(starts, positions):
    inside = (positions[None, None, :] >= starts[:, :, None]) & (
        positions[None, None, :] < starts[:, :, None] + PIC
    )
    labels = jnp.arange(1, starts.shape[1] + 1, dtype=jnp.int32)
    return jnp.sum(jnp.where(inside, labels[None, :, None], 0), axis=1)


def visible(query_pos, key_pos, query_labels, key_labels):
    causal = key_pos[None, None, :] <= query_pos[None, :, None]
    shared = (query_labels[:, :, None] == key_labels[:, None, :]) & (query_labels[:, :, None] > 0)
    return causal | shared


def exponents(queries, key_rows, query_pos, key_pos, visible_mask, slopes):
    score_scale = queries.shape[-1] ** (-0.5)
    logits = (
        jnp.einsum("sqhd,skhd->shqk", queries, key_rows, preferred_element_type=jnp.float32)
        * score_scale
    )
    distance = jnp.abs(query_pos[:, None] - key_pos[None, :]).astype(jnp.float32)
    logits = logits - slopes[None, :, None, None] * distance[None, None]
    return jnp.where(visible_mask[:, None], jnp.exp(logits), 0.0)


def block_grads(
    queries, scaled_grad, row_delta, key_rows, value_rows, query_pos, key_pos, visible_mask, slopes
):
    score_scale = queries.shape[-1] ** (-0.5)
    exponent = exponents(queries, key_rows, query_pos, key_pos, visible_mask, slopes)
    products_gv = jnp.einsum(
        "sqhd,skhd->shqk", scaled_grad, value_rows, preferred_element_type=jnp.float32
    )
    grad_logits = (
        exponent * (products_gv - jnp.transpose(row_delta, (0, 2, 1))[..., None])
    ).astype(jnp.bfloat16)
    grad_queries = (
        jnp.einsum("shqk,skhd->sqhd", grad_logits, key_rows, preferred_element_type=jnp.float32)
        * score_scale
    )
    grad_keyrows = (
        jnp.einsum("shqk,sqhd->skhd", grad_logits, queries, preferred_element_type=jnp.float32)
        * score_scale
    )
    grad_valrows = jnp.einsum(
        "shqk,sqhd->skhd",
        exponent.astype(jnp.bfloat16),
        scaled_grad,
        preferred_element_type=jnp.float32,
    )
    return (grad_queries, grad_keyrows, grad_valrows)


def partner_swaps(block, axis_name, axis_count):
    received = [block]
    for offset in range(1, axis_count):
        pairs = [(index, index ^ offset) for index in range(axis_count)]
        received.append(lax.ppermute(block, axis_name, pairs))
    return received


def pair_gather(block, axis_name, axis):
    if lax.axis_size(axis_name) != 2:
        return lax.all_gather(block, axis_name, axis=axis, tiled=True)
    other = lax.ppermute(block, axis_name, [(0, 1), (1, 0)])
    first = lax.axis_index(axis_name) == 0
    low = jnp.where(first, block, other)
    high = jnp.where(first, other, block)
    return jnp.concatenate([low, high], axis=axis)


def butterfly_sum(values, axis_names):
    leaves, tree = jax.tree.flatten(values)
    packed = jnp.concatenate([leaf.reshape(-1) for leaf in leaves])
    for axis_name in axis_names:
        axis_count = lax.axis_size(axis_name)
        step = 1
        while step < axis_count:
            pairs = [(index, index ^ step) for index in range(axis_count)]
            narrow = packed.astype(jnp.bfloat16)
            packed = narrow.astype(jnp.float32) + lax.ppermute(narrow, axis_name, pairs).astype(
                jnp.float32
            )
            step *= 2
    parts, offset = [], 0
    for leaf in leaves:
        parts.append(packed[offset : offset + leaf.size].reshape(leaf.shape))
        offset += leaf.size
    return jax.tree.unflatten(tree, parts)


def partner_gather_rows(rows_here, axis_name):
    axis_count = lax.axis_size(axis_name)
    blocks = jnp.stack(partner_swaps(rows_here, axis_name, axis_count))
    owners = jnp.bitwise_xor(
        lax.axis_index(axis_name), jnp.arange(axis_count, dtype=jnp.int32)
    )
    ordered = jnp.take(blocks, owners, axis=0)
    return ordered.reshape(axis_count * rows_here.shape[0], *rows_here.shape[1:])


def narrow_psum(values, axis_names):
    summed = lax.psum(jax.tree.map(lambda value: value.astype(jnp.bfloat16), values), axis_names)
    return jax.tree.map(lambda value: value.astype(jnp.float32), summed)


def tp_rows(rows_array, tp_count):
    chunk = rows_array.shape[0] // tp_count
    return lax.dynamic_slice_in_dim(rows_array, lax.axis_index("tp") * chunk, chunk, axis=0)


def scatter_rows(partials):
    widths = [part.shape[1] for part in partials]
    joined = lax.psum_scatter(
        jnp.concatenate(partials, axis=1).astype(jnp.bfloat16),
        "tp",
        scatter_dimension=0,
        tiled=True,
    )
    return split_columns(joined.astype(jnp.float32), widths)


def gather_rows(rows_here):
    widths = [part.shape[1] for part in rows_here]
    joined = lax.all_gather(jnp.concatenate(rows_here, axis=1), "tp", axis=0, tiled=True)
    return split_columns(joined, widths)


def split_columns(joined, widths):
    parts, offset = [], 0
    for width in widths:
        parts.append(joined[:, offset : offset + width])
        offset += width
    return tuple(parts)


def layer_body(
    layer_input,
    output_gradient,
    picture_piece_starts,
    sequence_adapter_index,
    attention_norm_gain,
    attention_norm_bias,
    feedforward_norm_gain,
    feedforward_norm_bias,
    query_key_value_weight,
    attention_output_weight,
    up_projection_weight,
    down_projection_weight,
    adapter_projection_first,
    adapter_projection_second,
    adapter_heads_first,
    adapter_heads_second,
    adapter_up_first,
    adapter_up_second,
    adapter_down_first,
    adapter_down_second,
):
    seq_here, local_len, model_width = layer_input.shape
    tok_rows = seq_here * local_len
    tp_count = lax.axis_size("tp")
    adapter_tables = adapter_projection_first.shape[0]
    rank_width = adapter_projection_first.shape[2]
    head_width = HD
    device_heads = adapter_projection_second.shape[-1] // head_width
    local_width = device_heads * head_width
    columns = jnp.arange(adapter_tables * rank_width, dtype=jnp.int32) // rank_width
    chosen = (sequence_adapter_index[:, None] == columns[None, :]).astype(jnp.float32)
    select = jnp.broadcast_to(
        chosen[:, None, :], (seq_here, local_len, adapter_tables * rank_width)
    ).reshape(tok_rows, adapter_tables * rank_width)
    select_here = tp_rows(select, tp_count)
    head_ids = lax.axis_index("tp") * device_heads + jnp.arange(device_heads, dtype=jnp.int32)
    slopes = jnp.exp2(
        -8.0 * (head_ids.astype(jnp.float32) + 1.0) / (device_heads * tp_count)
    )
    here_pos = lax.axis_index("ctx") * local_len + jnp.arange(local_len, dtype=jnp.int32)
    here_labels = piece_labels(picture_piece_starts, here_pos)
    heads_first_local = flattened_first(adapter_heads_first)
    heads_pair = lax.all_gather(
        jnp.concatenate([attention_output_weight, heads_first_local], axis=1),
        "tp",
        axis=0,
        tiled=True,
    )
    out_cols = attention_output_weight.shape[1]
    heads_full = pair_gather(heads_pair[:, :out_cols], "shard", 1)
    heads_first_all_flattened = heads_pair[:, out_cols:]
    projection_first_flattened = flattened_first(adapter_projection_first)
    projection_second_flattened = flattened_second(adapter_projection_second)
    heads_first_flattened = flattened_first(adapter_heads_first)
    heads_second_flattened = flattened_second(adapter_heads_second)
    up_first_flattened = flattened_first(adapter_up_first)
    up_second_flattened = flattened_second(adapter_up_second)
    down_first_flattened = flattened_first(adapter_down_first)
    down_second_flattened = flattened_second(adapter_down_second)
    residual = layer_input.reshape(tok_rows, model_width).astype(jnp.float32)
    residual_here = tp_rows(residual, tp_count)
    first_norm = layer_norm(residual, attention_norm_gain, attention_norm_bias)
    first_act = first_norm.astype(jnp.bfloat16)
    _, first_back_full = jax.vjp(
        lambda inputs: layer_norm(inputs, attention_norm_gain, attention_norm_bias), residual_here
    )
    gathered_rows = (
        pair_gather(query_key_value_weight, "shard", 0),
        pair_gather(up_projection_weight, "shard", 0),
    )
    qkv_full = gathered_rows[0].reshape(model_width, 3 * local_width)
    up_full = gathered_rows[1]
    down_full = pair_gather(down_projection_weight, "shard", 1)
    first_low = (matmul(first_act, projection_first_flattened) * select).astype(jnp.bfloat16)
    projected = (
        matmul(first_act, qkv_full) + matmul(first_low, projection_second_flattened)
    ).astype(jnp.bfloat16)
    queries_flat = projected[:, :local_width].reshape(seq_here, local_len, local_width)
    queries = queries_flat.reshape(seq_here, local_len, device_heads, head_width)
    key_rows = projected[:, local_width : 2 * local_width].reshape(seq_here, local_len, local_width)
    value_rows = projected[:, 2 * local_width :].reshape(seq_here, local_len, local_width)
    ctx_count = lax.axis_size("ctx")
    ctx_here = lax.axis_index("ctx")
    blocks = partner_swaps(
        jnp.concatenate([key_rows, value_rows], axis=2), "ctx", ctx_count
    )
    pieces = jnp.concatenate(blocks, axis=1)
    piece_len = pieces.shape[1]
    key_pos = jnp.concatenate(
        [
            (ctx_here ^ offset) * local_len + jnp.arange(local_len, dtype=jnp.int32)
            for offset in range(ctx_count)
        ]
    )
    key_labels = piece_labels(picture_piece_starts, key_pos)
    visible_mask = visible(here_pos, key_pos, here_labels, key_labels)
    piece_keys = pieces[:, :, :local_width].reshape(seq_here, piece_len, device_heads, head_width)
    piece_values = pieces[:, :, local_width:].reshape(
        seq_here, piece_len, device_heads, head_width
    )
    exponent = exponents(queries, piece_keys, here_pos, key_pos, visible_mask, slopes)
    weighted = jnp.einsum(
        "shqk,skhd->sqhd",
        exponent.astype(jnp.bfloat16),
        piece_values,
        preferred_element_type=jnp.float32,
    )
    weighted, totals = (weighted, jnp.sum(exponent, axis=-1))
    per_total = jnp.transpose(totals, (0, 2, 1))[..., None]
    heads_raw = weighted / per_total
    heads_act = heads_raw.reshape(tok_rows, local_width).astype(jnp.bfloat16)
    heads_act_here = lax.all_to_all(heads_act, "tp", 0, 1, tiled=True)
    attn_here = matmul(heads_act_here, heads_full)
    heads_low_here = (matmul(heads_act_here, heads_first_all_flattened) * select_here).astype(
        jnp.bfloat16
    )
    middle_here = residual_here + attn_here + matmul(heads_low_here, heads_second_flattened)
    second_norm, second_back = jax.vjp(
        lambda inputs: layer_norm(inputs, feedforward_norm_gain, feedforward_norm_bias), middle_here
    )
    second_act_here = second_norm.astype(jnp.bfloat16)
    (second_act,) = gather_rows((second_act_here,))
    up_low = (matmul(second_act, up_first_flattened) * select).astype(jnp.bfloat16)
    hidden = matmul(second_act, up_full) + matmul(up_low, up_second_flattened)
    activated, gelu_back = jax.vjp(gelu_tanh, hidden)
    activated = activated.astype(jnp.bfloat16)
    down_part = matmul(activated, down_full)
    down_low_part = matmul(activated, down_first_flattened)
    ffn_here, ffn_low_here = scatter_rows((down_part, down_low_part))
    down_low_here = (ffn_low_here * select_here).astype(jnp.bfloat16)
    result_here = (middle_here + ffn_here + matmul(down_low_here, down_second_flattened)).astype(
        jnp.bfloat16
    )
    (result_rows,) = gather_rows((result_here,))
    layer_out = result_rows.reshape(layer_input.shape)
    grad_top_low = output_gradient.reshape(tok_rows, model_width)
    grad_top_here = tp_rows(grad_top_low, tp_count).astype(jnp.float32)
    down_back = (matmul_nt(grad_top_low, down_second_flattened) * select).astype(jnp.bfloat16)
    grad_down_in = matmul_tn(activated, down_back)
    grad_activated = matmul_nt(grad_top_low, down_full) + matmul_nt(down_back, down_first_flattened)
    grad_hidden = gelu_back(grad_activated)[0].astype(jnp.bfloat16)
    up_second_gradient = matmul_tn(up_low, grad_hidden)
    ffn_back_part = matmul_nt(grad_hidden, up_full)
    ffn_back_low = matmul_nt(grad_hidden, up_second_flattened)
    back_here, back_low_here = scatter_rows((ffn_back_part, ffn_back_low))
    up_back_here = (back_low_here * select_here).astype(jnp.bfloat16)
    grad_second = back_here + matmul_nt(up_back_here, up_first_flattened)
    grad_middle_here = grad_top_here + second_back(grad_second)[0]
    grad_middle_low_here = grad_middle_here.astype(jnp.bfloat16)
    heads_back_here = (matmul_nt(grad_middle_low_here, heads_second_flattened) * select_here).astype(
        jnp.bfloat16
    )
    low_rows = partner_gather_rows(
        jnp.concatenate([down_low_here, up_back_here, heads_back_here], axis=1), "tp"
    )
    down_low, up_back, heads_back = split_columns(low_rows, [rank_width * adapter_tables] * 3)
    down_second_gradient = matmul_tn(down_low, grad_top_low)
    grad_up_in = matmul_tn(second_act, up_back)
    grad_heads_in = matmul_tn(heads_act, heads_back)
    heads_second_gradient = matmul_tn(heads_low_here, grad_middle_low_here)
    early_terms = narrow_psum(
        (
            unflat_in(grad_heads_in, adapter_tables),
            unflat_in(grad_up_in, adapter_tables),
            up_second_gradient.reshape(adapter_up_second.shape),
            unflat_in(grad_down_in, adapter_tables),
            down_second_gradient.reshape(adapter_down_second.shape),
        ),
        ("shard", "ctx"),
    )
    heads_tp_total = narrow_psum(heads_second_gradient.reshape(adapter_heads_second.shape), ("tp",))
    grad_heads_here = (
        matmul_nt(grad_middle_low_here, heads_full)
        + matmul_nt(heads_back_here, heads_first_all_flattened)
    ).astype(jnp.bfloat16)
    grad_heads = lax.all_to_all(grad_heads_here, "tp", 1, 0, tiled=True)
    grad_heads_wide = grad_heads.reshape(seq_here, local_len, device_heads, head_width).astype(
        jnp.float32
    )
    scaled_grad = (grad_heads_wide / per_total).astype(jnp.bfloat16)
    row_delta = jnp.sum(grad_heads_wide * heads_raw, axis=-1) / per_total[..., 0]
    grad_queries, grad_keyrows, grad_valrows = block_grads(
        queries,
        scaled_grad,
        row_delta,
        piece_keys,
        piece_values,
        here_pos,
        key_pos,
        visible_mask,
        slopes,
    )
    grad_kv = jnp.concatenate(
        [
            grad_keyrows.reshape(seq_here, ctx_count, local_len, local_width),
            grad_valrows.reshape(seq_here, ctx_count, local_len, local_width),
        ],
        axis=3,
    )
    grad_kv_here = grad_kv[:, 0]
    for offset in range(1, ctx_count):
        pairs = [(index, index ^ offset) for index in range(ctx_count)]
        grad_kv_here = grad_kv_here + lax.ppermute(
            grad_kv[:, offset].astype(jnp.bfloat16), "ctx", pairs
        ).astype(jnp.float32)
    grad_keys_all = grad_kv_here[:, :, :local_width]
    grad_values_all = grad_kv_here[:, :, local_width:]
    grad_projected = jnp.concatenate(
        [
            grad_queries.reshape(tok_rows, local_width),
            grad_keys_all.reshape(tok_rows, local_width),
            grad_values_all.reshape(tok_rows, local_width),
        ],
        axis=1,
    ).astype(jnp.bfloat16)
    projection_second_gradient = matmul_tn(first_low, grad_projected)
    attn_back_part = matmul_nt(grad_projected, qkv_full)
    attn_back_low = matmul_nt(grad_projected, projection_second_flattened)
    low_blocks = jnp.stack(partner_swaps(attn_back_low.astype(jnp.bfloat16), "tp", tp_count))
    low_owners = jnp.bitwise_xor(lax.axis_index("tp"), jnp.arange(tp_count, dtype=jnp.int32))
    low_total = jnp.sum(jnp.take(low_blocks, low_owners, axis=0).astype(jnp.float32), axis=0)
    select_late = lax.optimization_barrier(select)
    qkv_back = (low_total * select_late).astype(jnp.bfloat16)
    grad_qkv_in = matmul_tn(first_act, qkv_back)
    late_terms = butterfly_sum(
        (
            unflat_in(grad_qkv_in, adapter_tables),
            projection_second_gradient.reshape(adapter_projection_second.shape),
            heads_tp_total,
        ),
        ("shard", "ctx"),
    )
    heads_second_total = late_terms[2]
    first_here, first_low_here = scatter_rows((attn_back_part, attn_back_low))
    select_later = lax.optimization_barrier(select_here)
    qkv_back_here = (first_low_here * select_later).astype(jnp.bfloat16)
    grad_first = first_here + matmul_nt(qkv_back_here, projection_first_flattened)
    input_here = (grad_middle_here + first_back_full(grad_first)[0]).astype(jnp.bfloat16)
    (input_rows,) = gather_rows((input_here,))
    input_grad = input_rows.reshape(layer_input.shape)
    return (
        layer_out,
        input_grad,
        late_terms[0],
        late_terms[1],
        early_terms[0],
        heads_second_total,
        early_terms[1],
        early_terms[2],
        early_terms[3],
        early_terms[4],
    )


def solution(mesh):
    placed = (
        P("shard", "ctx", None),
        P("shard", "ctx", None),
        P("shard", None),
        P("shard"),
        P(),
        P(),
        P(),
        P(),
        P("shard", None, "tp"),
        P("tp", "shard"),
        P("shard", "tp"),
        P("tp", "shard"),
        P(),
        P(None, None, None, "tp"),
        P(None, "tp", None),
        P(),
        P(),
        P(None, None, "tp"),
        P(None, "tp", None),
        P(),
    )
    return jax.shard_map(
        layer_body,
        mesh=mesh,
        in_specs=placed,
        out_specs=(
            P("shard", "ctx", None),
            P("shard", "ctx", None),
            P(),
            P(None, None, None, "tp"),
            P(None, "tp", None),
            P(),
            P(),
            P(None, None, "tp"),
            P(None, "tp", None),
            P(),
        ),
        check_vma=False,
    )
```

```python
import jax
import jax.numpy as jnp
from jax import lax
from jax.sharding import PartitionSpec as P

HD = 128
PIC = 256


NORM_EPS = 1e-05


def layer_norm(inputs, gains, biases):
    average = jnp.mean(inputs, axis=-1, keepdims=True)
    centred = inputs - average
    spread = jnp.mean(centred * centred, axis=-1, keepdims=True)
    return centred * lax.rsqrt(spread + NORM_EPS) * gains + biases


def gelu_tanh(inputs):
    return (
        0.5
        * inputs
        * (1.0 + jnp.tanh(0.7978845608028654 * (inputs + 0.044715 * inputs * inputs * inputs)))
    )


def flattened_first(adapter_mat):
    adapter_tables, inner_dim, rank_width = adapter_mat.shape
    return jnp.transpose(adapter_mat, (1, 0, 2)).reshape(inner_dim, adapter_tables * rank_width)


def flattened_second(adapter_mat):
    return adapter_mat.reshape(adapter_mat.shape[0] * adapter_mat.shape[1], -1)


def unflat_in(grad_flat, adapter_tables):
    inner_dim = grad_flat.shape[0]
    return jnp.transpose(grad_flat.reshape(inner_dim, adapter_tables, -1), (1, 0, 2))


def matmul(left_mat, right_mat):
    return jnp.dot(left_mat, right_mat, preferred_element_type=jnp.float32)


def matmul_tn(left_mat, right_mat):
    return lax.dot_general(
        left_mat, right_mat, (((0,), (0,)), ((), ())), preferred_element_type=jnp.float32
    )


def matmul_nt(left_mat, right_mat):
    return lax.dot_general(
        left_mat, right_mat, (((1,), (1,)), ((), ())), preferred_element_type=jnp.float32
    )


def piece_labels(starts, positions):
    inside = (positions[None, None, :] >= starts[:, :, None]) & (
        positions[None, None, :] < starts[:, :, None] + PIC
    )
    labels = jnp.arange(1, starts.shape[1] + 1, dtype=jnp.int32)
    return jnp.sum(jnp.where(inside, labels[None, :, None], 0), axis=1)


def visible(query_pos, key_pos, query_labels, key_labels):
    causal = key_pos[None, None, :] <= query_pos[None, :, None]
    shared = (query_labels[:, :, None] == key_labels[:, None, :]) & (query_labels[:, :, None] > 0)
    return causal | shared


def exponents(queries, key_rows, query_pos, key_pos, visible_mask, slopes):
    score_scale = queries.shape[-1] ** (-0.5)
    logits = (
        jnp.einsum("sqhd,skhd->shqk", queries, key_rows, preferred_element_type=jnp.float32)
        * score_scale
    )
    distance = jnp.abs(query_pos[:, None] - key_pos[None, :]).astype(jnp.float32)
    logits = logits - slopes[None, :, None, None] * distance[None, None]
    return jnp.where(visible_mask[:, None], jnp.exp(logits), 0.0)


def block_grads(
    queries, scaled_grad, row_delta, key_rows, value_rows, query_pos, key_pos, visible_mask, slopes
):
    score_scale = queries.shape[-1] ** (-0.5)
    exponent = exponents(queries, key_rows, query_pos, key_pos, visible_mask, slopes)
    products_gv = jnp.einsum(
        "sqhd,skhd->shqk", scaled_grad, value_rows, preferred_element_type=jnp.float32
    )
    grad_logits = (
        exponent * (products_gv - jnp.transpose(row_delta, (0, 2, 1))[..., None])
    ).astype(jnp.bfloat16)
    grad_queries = (
        jnp.einsum("shqk,skhd->sqhd", grad_logits, key_rows, preferred_element_type=jnp.float32)
        * score_scale
    )
    grad_keyrows = (
        jnp.einsum("shqk,sqhd->skhd", grad_logits, queries, preferred_element_type=jnp.float32)
        * score_scale
    )
    grad_valrows = jnp.einsum(
        "shqk,sqhd->skhd",
        exponent.astype(jnp.bfloat16),
        scaled_grad,
        preferred_element_type=jnp.float32,
    )
    return (grad_queries, grad_keyrows, grad_valrows)


def partner_swaps(block, axis_name, axis_count):
    received = [block]
    for offset in range(1, axis_count):
        pairs = [(index, index ^ offset) for index in range(axis_count)]
        received.append(lax.ppermute(block, axis_name, pairs))
    return received


def pair_gather(block, axis_name, axis):
    if lax.axis_size(axis_name) != 2:
        return lax.all_gather(block, axis_name, axis=axis, tiled=True)
    other = lax.ppermute(block, axis_name, [(0, 1), (1, 0)])
    first = lax.axis_index(axis_name) == 0
    low = jnp.where(first, block, other)
    high = jnp.where(first, other, block)
    return jnp.concatenate([low, high], axis=axis)


def butterfly_sum(values, axis_names):
    leaves, tree = jax.tree.flatten(values)
    packed = jnp.concatenate([leaf.reshape(-1) for leaf in leaves])
    for axis_name in axis_names:
        axis_count = lax.axis_size(axis_name)
        step = 1
        while step < axis_count:
            pairs = [(index, index ^ step) for index in range(axis_count)]
            narrow = packed.astype(jnp.bfloat16)
            packed = narrow.astype(jnp.float32) + lax.ppermute(narrow, axis_name, pairs).astype(
                jnp.float32
            )
            step *= 2
    parts, offset = [], 0
    for leaf in leaves:
        parts.append(packed[offset : offset + leaf.size].reshape(leaf.shape))
        offset += leaf.size
    return jax.tree.unflatten(tree, parts)


def partner_gather_rows(rows_here, axis_name):
    axis_count = lax.axis_size(axis_name)
    blocks = jnp.stack(partner_swaps(rows_here, axis_name, axis_count))
    owners = jnp.bitwise_xor(
        lax.axis_index(axis_name), jnp.arange(axis_count, dtype=jnp.int32)
    )
    ordered = jnp.take(blocks, owners, axis=0)
    return ordered.reshape(axis_count * rows_here.shape[0], *rows_here.shape[1:])


def narrow_psum(values, axis_names):
    summed = lax.psum(jax.tree.map(lambda value: value.astype(jnp.bfloat16), values), axis_names)
    return jax.tree.map(lambda value: value.astype(jnp.float32), summed)


def tp_rows(rows_array, tp_count):
    chunk = rows_array.shape[0] // tp_count
    return lax.dynamic_slice_in_dim(rows_array, lax.axis_index("tp") * chunk, chunk, axis=0)


def scatter_rows(partials):
    widths = [part.shape[1] for part in partials]
    joined = lax.psum_scatter(
        jnp.concatenate(partials, axis=1).astype(jnp.bfloat16),
        "tp",
        scatter_dimension=0,
        tiled=True,
    )
    return split_columns(joined.astype(jnp.float32), widths)


def gather_rows(rows_here):
    widths = [part.shape[1] for part in rows_here]
    joined = lax.all_gather(jnp.concatenate(rows_here, axis=1), "tp", axis=0, tiled=True)
    return split_columns(joined, widths)


def split_columns(joined, widths):
    parts, offset = [], 0
    for width in widths:
        parts.append(joined[:, offset : offset + width])
        offset += width
    return tuple(parts)


def layer_body(
    layer_input,
    output_gradient,
    picture_piece_starts,
    sequence_adapter_index,
    attention_norm_gain,
    attention_norm_bias,
    feedforward_norm_gain,
    feedforward_norm_bias,
    query_key_value_weight,
    attention_output_weight,
    up_projection_weight,
    down_projection_weight,
    adapter_projection_first,
    adapter_projection_second,
    adapter_heads_first,
    adapter_heads_second,
    adapter_up_first,
    adapter_up_second,
    adapter_down_first,
    adapter_down_second,
):
    seq_here, local_len, model_width = layer_input.shape
    tok_rows = seq_here * local_len
    tp_count = lax.axis_size("tp")
    adapter_tables = adapter_projection_first.shape[0]
    rank_width = adapter_projection_first.shape[2]
    head_width = HD
    device_heads = adapter_projection_second.shape[-1] // head_width
    local_width = device_heads * head_width
    columns = jnp.arange(adapter_tables * rank_width, dtype=jnp.int32) // rank_width
    chosen = (sequence_adapter_index[:, None] == columns[None, :]).astype(jnp.float32)
    select = jnp.broadcast_to(
        chosen[:, None, :], (seq_here, local_len, adapter_tables * rank_width)
    ).reshape(tok_rows, adapter_tables * rank_width)
    select_here = tp_rows(select, tp_count)
    head_ids = lax.axis_index("tp") * device_heads + jnp.arange(device_heads, dtype=jnp.int32)
    slopes = jnp.exp2(
        -8.0 * (head_ids.astype(jnp.float32) + 1.0) / (device_heads * tp_count)
    )
    here_pos = lax.axis_index("ctx") * local_len + jnp.arange(local_len, dtype=jnp.int32)
    here_labels = piece_labels(picture_piece_starts, here_pos)
    heads_first_local = flattened_first(adapter_heads_first)
    heads_pair = lax.all_gather(
        jnp.concatenate([attention_output_weight, heads_first_local], axis=1),
        "tp",
        axis=0,
        tiled=True,
    )
    out_cols = attention_output_weight.shape[1]
    heads_full = pair_gather(heads_pair[:, :out_cols], "shard", 1)
    heads_first_all_flattened = heads_pair[:, out_cols:]
    projection_first_flattened = flattened_first(adapter_projection_first)
    projection_second_flattened = flattened_second(adapter_projection_second)
    heads_first_flattened = flattened_first(adapter_heads_first)
    heads_second_flattened = flattened_second(adapter_heads_second)
    up_first_flattened = flattened_first(adapter_up_first)
    up_second_flattened = flattened_second(adapter_up_second)
    down_first_flattened = flattened_first(adapter_down_first)
    down_second_flattened = flattened_second(adapter_down_second)
    residual = layer_input.reshape(tok_rows, model_width).astype(jnp.float32)
    residual_here = tp_rows(residual, tp_count)
    first_norm = layer_norm(residual, attention_norm_gain, attention_norm_bias)
    first_act = first_norm.astype(jnp.bfloat16)
    _, first_back_full = jax.vjp(
        lambda inputs: layer_norm(inputs, attention_norm_gain, attention_norm_bias), residual_here
    )
    gathered_rows = (
        pair_gather(query_key_value_weight, "shard", 0),
        pair_gather(up_projection_weight, "shard", 0),
    )
    qkv_full = gathered_rows[0].reshape(model_width, 3 * local_width)
    up_full = gathered_rows[1]
    down_full = pair_gather(down_projection_weight, "shard", 1)
    first_low = (matmul(first_act, projection_first_flattened) * select).astype(jnp.bfloat16)
    projected = (
        matmul(first_act, qkv_full) + matmul(first_low, projection_second_flattened)
    ).astype(jnp.bfloat16)
    queries_flat = projected[:, :local_width].reshape(seq_here, local_len, local_width)
    queries = queries_flat.reshape(seq_here, local_len, device_heads, head_width)
    key_rows = projected[:, local_width : 2 * local_width].reshape(seq_here, local_len, local_width)
    value_rows = projected[:, 2 * local_width :].reshape(seq_here, local_len, local_width)
    ctx_count = lax.axis_size("ctx")
    ctx_here = lax.axis_index("ctx")
    blocks = partner_swaps(
        jnp.concatenate([key_rows, value_rows], axis=2), "ctx", ctx_count
    )
    pieces = jnp.concatenate(blocks, axis=1)
    piece_len = pieces.shape[1]
    key_pos = jnp.concatenate(
        [
            (ctx_here ^ offset) * local_len + jnp.arange(local_len, dtype=jnp.int32)
            for offset in range(ctx_count)
        ]
    )
    key_labels = piece_labels(picture_piece_starts, key_pos)
    visible_mask = visible(here_pos, key_pos, here_labels, key_labels)
    piece_keys = pieces[:, :, :local_width].reshape(seq_here, piece_len, device_heads, head_width)
    piece_values = pieces[:, :, local_width:].reshape(
        seq_here, piece_len, device_heads, head_width
    )
    exponent = exponents(queries, piece_keys, here_pos, key_pos, visible_mask, slopes)
    weighted = jnp.einsum(
        "shqk,skhd->sqhd",
        exponent.astype(jnp.bfloat16),
        piece_values,
        preferred_element_type=jnp.float32,
    )
    weighted, totals = (weighted, jnp.sum(exponent, axis=-1))
    per_total = jnp.transpose(totals, (0, 2, 1))[..., None]
    heads_raw = weighted / per_total
    heads_act = heads_raw.reshape(tok_rows, local_width).astype(jnp.bfloat16)
    heads_act_here = lax.all_to_all(heads_act, "tp", 0, 1, tiled=True)
    attn_here = matmul(heads_act_here, heads_full)
    heads_low_here = (matmul(heads_act_here, heads_first_all_flattened) * select_here).astype(
        jnp.bfloat16
    )
    middle_here = residual_here + attn_here + matmul(heads_low_here, heads_second_flattened)
    second_norm, second_back = jax.vjp(
        lambda inputs: layer_norm(inputs, feedforward_norm_gain, feedforward_norm_bias), middle_here
    )
    second_act_here = second_norm.astype(jnp.bfloat16)
    (second_act,) = gather_rows((second_act_here,))
    up_low = (matmul(second_act, up_first_flattened) * select).astype(jnp.bfloat16)
    hidden = matmul(second_act, up_full) + matmul(up_low, up_second_flattened)
    activated, gelu_back = jax.vjp(gelu_tanh, hidden)
    activated = activated.astype(jnp.bfloat16)
    down_part = matmul(activated, down_full)
    down_low_part = matmul(activated, down_first_flattened)
    ffn_here, ffn_low_here = scatter_rows((down_part, down_low_part))
    down_low_here = (ffn_low_here * select_here).astype(jnp.bfloat16)
    result_here = (middle_here + ffn_here + matmul(down_low_here, down_second_flattened)).astype(
        jnp.bfloat16
    )
    (result_rows,) = gather_rows((result_here,))
    layer_out = result_rows.reshape(layer_input.shape)
    grad_top_low = output_gradient.reshape(tok_rows, model_width)
    grad_top_here = tp_rows(grad_top_low, tp_count).astype(jnp.float32)
    down_back = (matmul_nt(grad_top_low, down_second_flattened) * select).astype(jnp.bfloat16)
    grad_down_in = matmul_tn(activated, down_back)
    grad_activated = matmul_nt(grad_top_low, down_full) + matmul_nt(down_back, down_first_flattened)
    grad_hidden = gelu_back(grad_activated)[0].astype(jnp.bfloat16)
    up_second_gradient = matmul_tn(up_low, grad_hidden)
    ffn_back_part = matmul_nt(grad_hidden, up_full)
    ffn_back_low = matmul_nt(grad_hidden, up_second_flattened)
    back_here, back_low_here = scatter_rows((ffn_back_part, ffn_back_low))
    up_back_here = (back_low_here * select_here).astype(jnp.bfloat16)
    grad_second = back_here + matmul_nt(up_back_here, up_first_flattened)
    grad_middle_here = grad_top_here + second_back(grad_second)[0]
    grad_middle_low_here = grad_middle_here.astype(jnp.bfloat16)
    heads_back_here = (matmul_nt(grad_middle_low_here, heads_second_flattened) * select_here).astype(
        jnp.bfloat16
    )
    low_rows = partner_gather_rows(
        jnp.concatenate([down_low_here, up_back_here, heads_back_here], axis=1), "tp"
    )
    down_low, up_back, heads_back = split_columns(low_rows, [rank_width * adapter_tables] * 3)
    down_second_gradient = matmul_tn(down_low, grad_top_low)
    grad_up_in = matmul_tn(second_act, up_back)
    grad_heads_in = matmul_tn(heads_act, heads_back)
    heads_second_gradient = matmul_tn(heads_low_here, grad_middle_low_here)
    early_terms = narrow_psum(
        (
            unflat_in(grad_heads_in, adapter_tables),
            unflat_in(grad_up_in, adapter_tables),
            up_second_gradient.reshape(adapter_up_second.shape),
            unflat_in(grad_down_in, adapter_tables),
            down_second_gradient.reshape(adapter_down_second.shape),
        ),
        ("shard", "ctx"),
    )
    heads_second_total = narrow_psum(
        heads_second_gradient.reshape(adapter_heads_second.shape), ("shard", "ctx", "tp")
    )
    grad_heads_here = (
        matmul_nt(grad_middle_low_here, heads_full)
        + matmul_nt(heads_back_here, heads_first_all_flattened)
    ).astype(jnp.bfloat16)
    grad_heads = lax.all_to_all(grad_heads_here, "tp", 1, 0, tiled=True)
    grad_heads_wide = grad_heads.reshape(seq_here, local_len, device_heads, head_width).astype(
        jnp.float32
    )
    scaled_grad = (grad_heads_wide / per_total).astype(jnp.bfloat16)
    row_delta = jnp.sum(grad_heads_wide * heads_raw, axis=-1) / per_total[..., 0]
    grad_queries, grad_keyrows, grad_valrows = block_grads(
        queries,
        scaled_grad,
        row_delta,
        piece_keys,
        piece_values,
        here_pos,
        key_pos,
        visible_mask,
        slopes,
    )
    grad_kv = jnp.concatenate(
        [
            grad_keyrows.reshape(seq_here, ctx_count, local_len, local_width),
            grad_valrows.reshape(seq_here, ctx_count, local_len, local_width),
        ],
        axis=3,
    )
    grad_kv_here = grad_kv[:, 0]
    for offset in range(1, ctx_count):
        pairs = [(index, index ^ offset) for index in range(ctx_count)]
        grad_kv_here = grad_kv_here + lax.ppermute(
            grad_kv[:, offset].astype(jnp.bfloat16), "ctx", pairs
        ).astype(jnp.float32)
    grad_keys_all = grad_kv_here[:, :, :local_width]
    grad_values_all = grad_kv_here[:, :, local_width:]
    grad_projected = jnp.concatenate(
        [
            grad_queries.reshape(tok_rows, local_width),
            grad_keys_all.reshape(tok_rows, local_width),
            grad_values_all.reshape(tok_rows, local_width),
        ],
        axis=1,
    ).astype(jnp.bfloat16)
    projection_second_gradient = matmul_tn(first_low, grad_projected)
    attn_back_part = matmul_nt(grad_projected, qkv_full)
    attn_back_low = matmul_nt(grad_projected, projection_second_flattened)
    low_blocks = jnp.stack(partner_swaps(attn_back_low.astype(jnp.bfloat16), "tp", tp_count))
    low_owners = jnp.bitwise_xor(lax.axis_index("tp"), jnp.arange(tp_count, dtype=jnp.int32))
    low_total = jnp.sum(jnp.take(low_blocks, low_owners, axis=0).astype(jnp.float32), axis=0)
    select_late = lax.optimization_barrier(select)
    qkv_back = (low_total * select_late).astype(jnp.bfloat16)
    grad_qkv_in = matmul_tn(first_act, qkv_back)
    late_terms = butterfly_sum(
        (
            unflat_in(grad_qkv_in, adapter_tables),
            projection_second_gradient.reshape(adapter_projection_second.shape),
        ),
        ("shard", "ctx"),
    )
    first_here, first_low_here = scatter_rows((attn_back_part, attn_back_low))
    select_later = lax.optimization_barrier(select_here)
    qkv_back_here = (first_low_here * select_later).astype(jnp.bfloat16)
    grad_first = first_here + matmul_nt(qkv_back_here, projection_first_flattened)
    input_here = (grad_middle_here + first_back_full(grad_first)[0]).astype(jnp.bfloat16)
    (input_rows,) = gather_rows((input_here,))
    input_grad = input_rows.reshape(layer_input.shape)
    return (
        layer_out,
        input_grad,
        late_terms[0],
        late_terms[1],
        early_terms[0],
        heads_second_total,
        early_terms[1],
        early_terms[2],
        early_terms[3],
        early_terms[4],
    )


def solution(mesh):
    placed = (
        P("shard", "ctx", None),
        P("shard", "ctx", None),
        P("shard", None),
        P("shard"),
        P(),
        P(),
        P(),
        P(),
        P("shard", None, "tp"),
        P("tp", "shard"),
        P("shard", "tp"),
        P("tp", "shard"),
        P(),
        P(None, None, None, "tp"),
        P(None, "tp", None),
        P(),
        P(),
        P(None, None, "tp"),
        P(None, "tp", None),
        P(),
    )
    return jax.shard_map(
        layer_body,
        mesh=mesh,
        in_specs=placed,
        out_specs=(
            P("shard", "ctx", None),
            P("shard", "ctx", None),
            P(),
            P(None, None, None, "tp"),
            P(None, "tp", None),
            P(),
            P(),
            P(None, None, "tp"),
            P(None, "tp", None),
            P(),
        ),
        check_vma=False,
    )
```

```python
import jax
import jax.numpy as jnp
from jax import lax
from jax.sharding import PartitionSpec as P

HD = 128
PIC = 256


NORM_EPS = 1e-05


def layer_norm(inputs, gains, biases):
    average = jnp.mean(inputs, axis=-1, keepdims=True)
    centred = inputs - average
    spread = jnp.mean(centred * centred, axis=-1, keepdims=True)
    return centred * lax.rsqrt(spread + NORM_EPS) * gains + biases


def gelu_tanh(inputs):
    return (
        0.5
        * inputs
        * (1.0 + jnp.tanh(0.7978845608028654 * (inputs + 0.044715 * inputs * inputs * inputs)))
    )


def flattened_first(adapter_mat):
    adapter_tables, inner_dim, rank_width = adapter_mat.shape
    return jnp.transpose(adapter_mat, (1, 0, 2)).reshape(inner_dim, adapter_tables * rank_width)


def flattened_second(adapter_mat):
    return adapter_mat.reshape(adapter_mat.shape[0] * adapter_mat.shape[1], -1)


def unflat_in(grad_flat, adapter_tables):
    inner_dim = grad_flat.shape[0]
    return jnp.transpose(grad_flat.reshape(inner_dim, adapter_tables, -1), (1, 0, 2))


def matmul(left_mat, right_mat):
    return jnp.dot(left_mat, right_mat, preferred_element_type=jnp.float32)


def matmul_tn(left_mat, right_mat):
    return lax.dot_general(
        left_mat, right_mat, (((0,), (0,)), ((), ())), preferred_element_type=jnp.float32
    )


def matmul_nt(left_mat, right_mat):
    return lax.dot_general(
        left_mat, right_mat, (((1,), (1,)), ((), ())), preferred_element_type=jnp.float32
    )


def piece_labels(starts, positions):
    inside = (positions[None, None, :] >= starts[:, :, None]) & (
        positions[None, None, :] < starts[:, :, None] + PIC
    )
    labels = jnp.arange(1, starts.shape[1] + 1, dtype=jnp.int32)
    return jnp.sum(jnp.where(inside, labels[None, :, None], 0), axis=1)


def visible(query_pos, key_pos, query_labels, key_labels):
    causal = key_pos[None, None, :] <= query_pos[None, :, None]
    shared = (query_labels[:, :, None] == key_labels[:, None, :]) & (query_labels[:, :, None] > 0)
    return causal | shared


def exponents(queries, key_rows, query_pos, key_pos, visible_mask, slopes):
    score_scale = queries.shape[-1] ** (-0.5)
    logits = (
        jnp.einsum("sqhd,skhd->shqk", queries, key_rows, preferred_element_type=jnp.float32)
        * score_scale
    )
    distance = jnp.abs(query_pos[:, None] - key_pos[None, :]).astype(jnp.float32)
    logits = logits - slopes[None, :, None, None] * distance[None, None]
    return jnp.where(visible_mask[:, None], jnp.exp(logits), 0.0)


def block_grads(
    queries, scaled_grad, row_delta, key_rows, value_rows, query_pos, key_pos, visible_mask, slopes
):
    score_scale = queries.shape[-1] ** (-0.5)
    exponent = exponents(queries, key_rows, query_pos, key_pos, visible_mask, slopes)
    products_gv = jnp.einsum(
        "sqhd,skhd->shqk", scaled_grad, value_rows, preferred_element_type=jnp.float32
    )
    grad_logits = (
        exponent * (products_gv - jnp.transpose(row_delta, (0, 2, 1))[..., None])
    ).astype(jnp.bfloat16)
    grad_queries = (
        jnp.einsum("shqk,skhd->sqhd", grad_logits, key_rows, preferred_element_type=jnp.float32)
        * score_scale
    )
    grad_keyrows = (
        jnp.einsum("shqk,sqhd->skhd", grad_logits, queries, preferred_element_type=jnp.float32)
        * score_scale
    )
    grad_valrows = jnp.einsum(
        "shqk,sqhd->skhd",
        exponent.astype(jnp.bfloat16),
        scaled_grad,
        preferred_element_type=jnp.float32,
    )
    return (grad_queries, grad_keyrows, grad_valrows)


def partner_swaps(block, axis_name, axis_count):
    received = [block]
    for offset in range(1, axis_count):
        pairs = [(index, index ^ offset) for index in range(axis_count)]
        received.append(lax.ppermute(block, axis_name, pairs))
    return received


def pair_gather(block, axis_name, axis):
    if lax.axis_size(axis_name) != 2:
        return lax.all_gather(block, axis_name, axis=axis, tiled=True)
    other = lax.ppermute(block, axis_name, [(0, 1), (1, 0)])
    first = lax.axis_index(axis_name) == 0
    low = jnp.where(first, block, other)
    high = jnp.where(first, other, block)
    return jnp.concatenate([low, high], axis=axis)


def butterfly_sum(values, axis_names):
    leaves, tree = jax.tree.flatten(values)
    packed = jnp.concatenate([leaf.reshape(-1) for leaf in leaves])
    for axis_name in axis_names:
        axis_count = lax.axis_size(axis_name)
        step = 1
        while step < axis_count:
            pairs = [(index, index ^ step) for index in range(axis_count)]
            narrow = packed.astype(jnp.bfloat16)
            packed = narrow.astype(jnp.float32) + lax.ppermute(narrow, axis_name, pairs).astype(
                jnp.float32
            )
            step *= 2
    parts, offset = [], 0
    for leaf in leaves:
        parts.append(packed[offset : offset + leaf.size].reshape(leaf.shape))
        offset += leaf.size
    return jax.tree.unflatten(tree, parts)


def partner_gather_rows(rows_here, axis_name):
    axis_count = lax.axis_size(axis_name)
    blocks = jnp.stack(partner_swaps(rows_here, axis_name, axis_count))
    owners = jnp.bitwise_xor(
        lax.axis_index(axis_name), jnp.arange(axis_count, dtype=jnp.int32)
    )
    ordered = jnp.take(blocks, owners, axis=0)
    return ordered.reshape(axis_count * rows_here.shape[0], *rows_here.shape[1:])


def narrow_psum(values, axis_names):
    summed = lax.psum(jax.tree.map(lambda value: value.astype(jnp.bfloat16), values), axis_names)
    return jax.tree.map(lambda value: value.astype(jnp.float32), summed)


def tp_rows(rows_array, tp_count):
    chunk = rows_array.shape[0] // tp_count
    return lax.dynamic_slice_in_dim(rows_array, lax.axis_index("tp") * chunk, chunk, axis=0)


def scatter_rows(partials):
    widths = [part.shape[1] for part in partials]
    joined = lax.psum_scatter(
        jnp.concatenate(partials, axis=1).astype(jnp.bfloat16),
        "tp",
        scatter_dimension=0,
        tiled=True,
    )
    return split_columns(joined.astype(jnp.float32), widths)


def gather_rows(rows_here):
    widths = [part.shape[1] for part in rows_here]
    joined = lax.all_gather(jnp.concatenate(rows_here, axis=1), "tp", axis=0, tiled=True)
    return split_columns(joined, widths)


def split_columns(joined, widths):
    parts, offset = [], 0
    for width in widths:
        parts.append(joined[:, offset : offset + width])
        offset += width
    return tuple(parts)


def layer_body(
    layer_input,
    output_gradient,
    picture_piece_starts,
    sequence_adapter_index,
    attention_norm_gain,
    attention_norm_bias,
    feedforward_norm_gain,
    feedforward_norm_bias,
    query_key_value_weight,
    attention_output_weight,
    up_projection_weight,
    down_projection_weight,
    adapter_projection_first,
    adapter_projection_second,
    adapter_heads_first,
    adapter_heads_second,
    adapter_up_first,
    adapter_up_second,
    adapter_down_first,
    adapter_down_second,
):
    seq_here, local_len, model_width = layer_input.shape
    tok_rows = seq_here * local_len
    tp_count = lax.axis_size("tp")
    adapter_tables = adapter_projection_first.shape[0]
    rank_width = adapter_projection_first.shape[2]
    head_width = HD
    device_heads = adapter_projection_second.shape[-1] // head_width
    local_width = device_heads * head_width
    columns = jnp.arange(adapter_tables * rank_width, dtype=jnp.int32) // rank_width
    chosen = (sequence_adapter_index[:, None] == columns[None, :]).astype(jnp.float32)
    select = jnp.broadcast_to(
        chosen[:, None, :], (seq_here, local_len, adapter_tables * rank_width)
    ).reshape(tok_rows, adapter_tables * rank_width)
    select_here = tp_rows(select, tp_count)
    head_ids = lax.axis_index("tp") * device_heads + jnp.arange(device_heads, dtype=jnp.int32)
    slopes = jnp.exp2(
        -8.0 * (head_ids.astype(jnp.float32) + 1.0) / (device_heads * tp_count)
    )
    here_pos = lax.axis_index("ctx") * local_len + jnp.arange(local_len, dtype=jnp.int32)
    here_labels = piece_labels(picture_piece_starts, here_pos)
    heads_first_local = flattened_first(adapter_heads_first)
    heads_pair = lax.all_gather(
        jnp.concatenate([attention_output_weight, heads_first_local], axis=1),
        "tp",
        axis=0,
        tiled=True,
    )
    out_cols = attention_output_weight.shape[1]
    heads_full = pair_gather(heads_pair[:, :out_cols], "shard", 1)
    heads_first_all_flattened = heads_pair[:, out_cols:]
    projection_first_flattened = flattened_first(adapter_projection_first)
    projection_second_flattened = flattened_second(adapter_projection_second)
    heads_first_flattened = flattened_first(adapter_heads_first)
    heads_second_flattened = flattened_second(adapter_heads_second)
    up_first_flattened = flattened_first(adapter_up_first)
    up_second_flattened = flattened_second(adapter_up_second)
    down_first_flattened = flattened_first(adapter_down_first)
    down_second_flattened = flattened_second(adapter_down_second)
    residual = layer_input.reshape(tok_rows, model_width).astype(jnp.float32)
    residual_here = tp_rows(residual, tp_count)
    first_norm = layer_norm(residual, attention_norm_gain, attention_norm_bias)
    first_act = first_norm.astype(jnp.bfloat16)
    _, first_back_full = jax.vjp(
        lambda inputs: layer_norm(inputs, attention_norm_gain, attention_norm_bias), residual_here
    )
    gathered_rows = (
        pair_gather(query_key_value_weight, "shard", 0),
        pair_gather(up_projection_weight, "shard", 0),
    )
    qkv_full = gathered_rows[0].reshape(model_width, 3 * local_width)
    up_full = gathered_rows[1]
    down_full = pair_gather(down_projection_weight, "shard", 1)
    first_low = (matmul(first_act, projection_first_flattened) * select).astype(jnp.bfloat16)
    projected = (
        matmul(first_act, qkv_full) + matmul(first_low, projection_second_flattened)
    ).astype(jnp.bfloat16)
    queries_flat = projected[:, :local_width].reshape(seq_here, local_len, local_width)
    queries = queries_flat.reshape(seq_here, local_len, device_heads, head_width)
    key_rows = projected[:, local_width : 2 * local_width].reshape(seq_here, local_len, local_width)
    value_rows = projected[:, 2 * local_width :].reshape(seq_here, local_len, local_width)
    ctx_count = lax.axis_size("ctx")
    ctx_here = lax.axis_index("ctx")
    blocks = partner_swaps(
        jnp.concatenate([key_rows, value_rows], axis=2), "ctx", ctx_count
    )
    pieces = jnp.concatenate(blocks, axis=1)
    piece_len = pieces.shape[1]
    key_pos = jnp.concatenate(
        [
            (ctx_here ^ offset) * local_len + jnp.arange(local_len, dtype=jnp.int32)
            for offset in range(ctx_count)
        ]
    )
    key_labels = piece_labels(picture_piece_starts, key_pos)
    visible_mask = visible(here_pos, key_pos, here_labels, key_labels)
    piece_keys = pieces[:, :, :local_width].reshape(seq_here, piece_len, device_heads, head_width)
    piece_values = pieces[:, :, local_width:].reshape(
        seq_here, piece_len, device_heads, head_width
    )
    exponent = exponents(queries, piece_keys, here_pos, key_pos, visible_mask, slopes)
    weighted = jnp.einsum(
        "shqk,skhd->sqhd",
        exponent.astype(jnp.bfloat16),
        piece_values,
        preferred_element_type=jnp.float32,
    )
    weighted, totals = (weighted, jnp.sum(exponent, axis=-1))
    per_total = jnp.transpose(totals, (0, 2, 1))[..., None]
    heads_raw = weighted / per_total
    heads_act = heads_raw.reshape(tok_rows, local_width).astype(jnp.bfloat16)
    heads_act_here = lax.all_to_all(heads_act, "tp", 0, 1, tiled=True)
    attn_here = matmul(heads_act_here, heads_full)
    heads_low_here = (matmul(heads_act_here, heads_first_all_flattened) * select_here).astype(
        jnp.bfloat16
    )
    middle_here = residual_here + attn_here + matmul(heads_low_here, heads_second_flattened)
    second_norm, second_back = jax.vjp(
        lambda inputs: layer_norm(inputs, feedforward_norm_gain, feedforward_norm_bias), middle_here
    )
    second_act_here = second_norm.astype(jnp.bfloat16)
    (second_act,) = gather_rows((second_act_here,))
    up_low = (matmul(second_act, up_first_flattened) * select).astype(jnp.bfloat16)
    hidden = matmul(second_act, up_full) + matmul(up_low, up_second_flattened)
    activated, gelu_back = jax.vjp(gelu_tanh, hidden)
    activated = activated.astype(jnp.bfloat16)
    down_part = matmul(activated, down_full)
    down_low_part = matmul(activated, down_first_flattened)
    ffn_here, ffn_low_here = scatter_rows((down_part, down_low_part))
    down_low_here = (ffn_low_here * select_here).astype(jnp.bfloat16)
    result_here = (middle_here + ffn_here + matmul(down_low_here, down_second_flattened)).astype(
        jnp.bfloat16
    )
    (result_rows,) = gather_rows((result_here,))
    layer_out = result_rows.reshape(layer_input.shape)
    grad_top_low = output_gradient.reshape(tok_rows, model_width)
    grad_top_here = tp_rows(grad_top_low, tp_count).astype(jnp.float32)
    down_back = (matmul_nt(grad_top_low, down_second_flattened) * select).astype(jnp.bfloat16)
    grad_down_in = matmul_tn(activated, down_back)
    grad_activated = matmul_nt(grad_top_low, down_full) + matmul_nt(down_back, down_first_flattened)
    grad_hidden = gelu_back(grad_activated)[0].astype(jnp.bfloat16)
    up_second_gradient = matmul_tn(up_low, grad_hidden)
    ffn_back_part = matmul_nt(grad_hidden, up_full)
    ffn_back_low = matmul_nt(grad_hidden, up_second_flattened)
    back_here, back_low_here = scatter_rows((ffn_back_part, ffn_back_low))
    up_back_here = (back_low_here * select_here).astype(jnp.bfloat16)
    grad_second = back_here + matmul_nt(up_back_here, up_first_flattened)
    grad_middle_here = grad_top_here + second_back(grad_second)[0]
    grad_middle_low_here = grad_middle_here.astype(jnp.bfloat16)
    heads_back_here = (matmul_nt(grad_middle_low_here, heads_second_flattened) * select_here).astype(
        jnp.bfloat16
    )
    low_rows = partner_gather_rows(
        jnp.concatenate([down_low_here, up_back_here, heads_back_here], axis=1), "tp"
    )
    down_low, up_back, heads_back = split_columns(low_rows, [rank_width * adapter_tables] * 3)
    down_second_gradient = matmul_tn(down_low, grad_top_low)
    grad_up_in = matmul_tn(second_act, up_back)
    grad_heads_in = matmul_tn(heads_act, heads_back)
    heads_second_gradient = matmul_tn(heads_low_here, grad_middle_low_here)
    early_terms = narrow_psum(
        (
            unflat_in(grad_heads_in, adapter_tables),
            unflat_in(grad_up_in, adapter_tables),
            up_second_gradient.reshape(adapter_up_second.shape),
            unflat_in(grad_down_in, adapter_tables),
            down_second_gradient.reshape(adapter_down_second.shape),
        ),
        ("shard", "ctx"),
    )
    heads_second_total = narrow_psum(
        heads_second_gradient.reshape(adapter_heads_second.shape), ("shard", "ctx", "tp")
    )
    grad_heads_here = (
        matmul_nt(grad_middle_low_here, heads_full)
        + matmul_nt(heads_back_here, heads_first_all_flattened)
    ).astype(jnp.bfloat16)
    grad_heads = lax.all_to_all(grad_heads_here, "tp", 1, 0, tiled=True)
    grad_heads_wide = grad_heads.reshape(seq_here, local_len, device_heads, head_width).astype(
        jnp.float32
    )
    scaled_grad = (grad_heads_wide / per_total).astype(jnp.bfloat16)
    row_delta = jnp.sum(grad_heads_wide * heads_raw, axis=-1) / per_total[..., 0]
    grad_queries = None
    grad_kv_here = None
    for offset in list(range(1, ctx_count)) + [0]:
        keys_slice = slice(offset * local_len, (offset + 1) * local_len)
        query_part, key_part, value_part = block_grads(
            queries,
            scaled_grad,
            row_delta,
            piece_keys[:, keys_slice],
            piece_values[:, keys_slice],
            here_pos,
            key_pos[keys_slice],
            visible_mask[:, :, keys_slice],
            slopes,
        )
        grad_queries = query_part if grad_queries is None else grad_queries + query_part
        block_kv = jnp.concatenate(
            [
                key_part.reshape(seq_here, local_len, local_width),
                value_part.reshape(seq_here, local_len, local_width),
            ],
            axis=2,
        )
        if offset:
            pairs = [(index, index ^ offset) for index in range(ctx_count)]
            block_kv = lax.ppermute(block_kv.astype(jnp.bfloat16), "ctx", pairs).astype(
                jnp.float32
            )
        grad_kv_here = block_kv if grad_kv_here is None else grad_kv_here + block_kv
    grad_keys_all = grad_kv_here[:, :, :local_width]
    grad_values_all = grad_kv_here[:, :, local_width:]
    grad_projected = jnp.concatenate(
        [
            grad_queries.reshape(tok_rows, local_width),
            grad_keys_all.reshape(tok_rows, local_width),
            grad_values_all.reshape(tok_rows, local_width),
        ],
        axis=1,
    ).astype(jnp.bfloat16)
    projection_second_gradient = matmul_tn(first_low, grad_projected)
    attn_back_part = matmul_nt(grad_projected, qkv_full)
    attn_back_low = matmul_nt(grad_projected, projection_second_flattened)
    low_blocks = jnp.stack(partner_swaps(attn_back_low.astype(jnp.bfloat16), "tp", tp_count))
    low_owners = jnp.bitwise_xor(lax.axis_index("tp"), jnp.arange(tp_count, dtype=jnp.int32))
    low_total = jnp.sum(jnp.take(low_blocks, low_owners, axis=0).astype(jnp.float32), axis=0)
    select_late = lax.optimization_barrier(select)
    qkv_back = (low_total * select_late).astype(jnp.bfloat16)
    grad_qkv_in = matmul_tn(first_act, qkv_back)
    late_terms = butterfly_sum(
        (
            unflat_in(grad_qkv_in, adapter_tables),
            projection_second_gradient.reshape(adapter_projection_second.shape),
        ),
        ("shard", "ctx"),
    )
    first_here, first_low_here = scatter_rows((attn_back_part, attn_back_low))
    select_later = lax.optimization_barrier(select_here)
    qkv_back_here = (first_low_here * select_later).astype(jnp.bfloat16)
    grad_first = first_here + matmul_nt(qkv_back_here, projection_first_flattened)
    input_here = (grad_middle_here + first_back_full(grad_first)[0]).astype(jnp.bfloat16)
    (input_rows,) = gather_rows((input_here,))
    input_grad = input_rows.reshape(layer_input.shape)
    return (
        layer_out,
        input_grad,
        late_terms[0],
        late_terms[1],
        early_terms[0],
        heads_second_total,
        early_terms[1],
        early_terms[2],
        early_terms[3],
        early_terms[4],
    )


def solution(mesh):
    placed = (
        P("shard", "ctx", None),
        P("shard", "ctx", None),
        P("shard", None),
        P("shard"),
        P(),
        P(),
        P(),
        P(),
        P("shard", None, "tp"),
        P("tp", "shard"),
        P("shard", "tp"),
        P("tp", "shard"),
        P(),
        P(None, None, None, "tp"),
        P(None, "tp", None),
        P(),
        P(),
        P(None, None, "tp"),
        P(None, "tp", None),
        P(),
    )
    return jax.shard_map(
        layer_body,
        mesh=mesh,
        in_specs=placed,
        out_specs=(
            P("shard", "ctx", None),
            P("shard", "ctx", None),
            P(),
            P(None, None, None, "tp"),
            P(None, "tp", None),
            P(),
            P(),
            P(None, None, "tp"),
            P(None, "tp", None),
            P(),
        ),
        check_vma=False,
    )
```

```python
import jax
import jax.numpy as jnp
from jax import lax
from jax.sharding import PartitionSpec as P

HD = 128
PIC = 256


NORM_EPS = 1e-05


def layer_norm(inputs, gains, biases):
    average = jnp.mean(inputs, axis=-1, keepdims=True)
    centred = inputs - average
    spread = jnp.mean(centred * centred, axis=-1, keepdims=True)
    return centred * lax.rsqrt(spread + NORM_EPS) * gains + biases


def gelu_tanh(inputs):
    return (
        0.5
        * inputs
        * (1.0 + jnp.tanh(0.7978845608028654 * (inputs + 0.044715 * inputs * inputs * inputs)))
    )


def flattened_first(adapter_mat):
    adapter_tables, inner_dim, rank_width = adapter_mat.shape
    return jnp.transpose(adapter_mat, (1, 0, 2)).reshape(inner_dim, adapter_tables * rank_width)


def flattened_second(adapter_mat):
    return adapter_mat.reshape(adapter_mat.shape[0] * adapter_mat.shape[1], -1)


def unflat_in(grad_flat, adapter_tables):
    inner_dim = grad_flat.shape[0]
    return jnp.transpose(grad_flat.reshape(inner_dim, adapter_tables, -1), (1, 0, 2))


def matmul(left_mat, right_mat):
    return jnp.dot(left_mat, right_mat, preferred_element_type=jnp.float32)


def matmul_tn(left_mat, right_mat):
    return lax.dot_general(
        left_mat, right_mat, (((0,), (0,)), ((), ())), preferred_element_type=jnp.float32
    )


def matmul_nt(left_mat, right_mat):
    return lax.dot_general(
        left_mat, right_mat, (((1,), (1,)), ((), ())), preferred_element_type=jnp.float32
    )


def piece_labels(starts, positions):
    inside = (positions[None, None, :] >= starts[:, :, None]) & (
        positions[None, None, :] < starts[:, :, None] + PIC
    )
    labels = jnp.arange(1, starts.shape[1] + 1, dtype=jnp.int32)
    return jnp.sum(jnp.where(inside, labels[None, :, None], 0), axis=1)


def visible(query_pos, key_pos, query_labels, key_labels):
    causal = key_pos[None, None, :] <= query_pos[None, :, None]
    shared = (query_labels[:, :, None] == key_labels[:, None, :]) & (query_labels[:, :, None] > 0)
    return causal | shared


def exponents(queries, key_rows, query_pos, key_pos, visible_mask, slopes):
    score_scale = queries.shape[-1] ** (-0.5)
    logits = (
        jnp.einsum("sqhd,skhd->shqk", queries, key_rows, preferred_element_type=jnp.float32)
        * score_scale
    )
    distance = jnp.abs(query_pos[:, None] - key_pos[None, :]).astype(jnp.float32)
    logits = logits - slopes[None, :, None, None] * distance[None, None]
    return jnp.where(visible_mask[:, None], jnp.exp(logits), 0.0)


def block_grads(
    queries, scaled_grad, row_delta, key_rows, value_rows, query_pos, key_pos, visible_mask, slopes
):
    score_scale = queries.shape[-1] ** (-0.5)
    exponent = exponents(queries, key_rows, query_pos, key_pos, visible_mask, slopes)
    products_gv = jnp.einsum(
        "sqhd,skhd->shqk", scaled_grad, value_rows, preferred_element_type=jnp.float32
    )
    grad_logits = (
        exponent * (products_gv - jnp.transpose(row_delta, (0, 2, 1))[..., None])
    ).astype(jnp.bfloat16)
    grad_queries = (
        jnp.einsum("shqk,skhd->sqhd", grad_logits, key_rows, preferred_element_type=jnp.float32)
        * score_scale
    )
    grad_keyrows = (
        jnp.einsum("shqk,sqhd->skhd", grad_logits, queries, preferred_element_type=jnp.float32)
        * score_scale
    )
    grad_valrows = jnp.einsum(
        "shqk,sqhd->skhd",
        exponent.astype(jnp.bfloat16),
        scaled_grad,
        preferred_element_type=jnp.float32,
    )
    return (grad_queries, grad_keyrows, grad_valrows)


def partner_swaps(block, axis_name, axis_count):
    received = [block]
    for offset in range(1, axis_count):
        pairs = [(index, index ^ offset) for index in range(axis_count)]
        received.append(lax.ppermute(block, axis_name, pairs))
    return received


def pair_gather(block, axis_name, axis):
    if lax.axis_size(axis_name) != 2:
        return lax.all_gather(block, axis_name, axis=axis, tiled=True)
    other = lax.ppermute(block, axis_name, [(0, 1), (1, 0)])
    first = lax.axis_index(axis_name) == 0
    low = jnp.where(first, block, other)
    high = jnp.where(first, other, block)
    return jnp.concatenate([low, high], axis=axis)


def butterfly_sum(values, axis_names):
    leaves, tree = jax.tree.flatten(values)
    packed = jnp.concatenate([leaf.reshape(-1) for leaf in leaves])
    for axis_name in axis_names:
        axis_count = lax.axis_size(axis_name)
        step = 1
        while step < axis_count:
            pairs = [(index, index ^ step) for index in range(axis_count)]
            narrow = packed.astype(jnp.bfloat16)
            packed = narrow.astype(jnp.float32) + lax.ppermute(narrow, axis_name, pairs).astype(
                jnp.float32
            )
            step *= 2
    parts, offset = [], 0
    for leaf in leaves:
        parts.append(packed[offset : offset + leaf.size].reshape(leaf.shape))
        offset += leaf.size
    return jax.tree.unflatten(tree, parts)


def partner_gather_rows(rows_here, axis_name):
    axis_count = lax.axis_size(axis_name)
    blocks = jnp.stack(partner_swaps(rows_here, axis_name, axis_count))
    owners = jnp.bitwise_xor(
        lax.axis_index(axis_name), jnp.arange(axis_count, dtype=jnp.int32)
    )
    ordered = jnp.take(blocks, owners, axis=0)
    return ordered.reshape(axis_count * rows_here.shape[0], *rows_here.shape[1:])


def narrow_psum(values, axis_names):
    summed = lax.psum(jax.tree.map(lambda value: value.astype(jnp.bfloat16), values), axis_names)
    return jax.tree.map(lambda value: value.astype(jnp.float32), summed)


def tp_rows(rows_array, tp_count):
    chunk = rows_array.shape[0] // tp_count
    return lax.dynamic_slice_in_dim(rows_array, lax.axis_index("tp") * chunk, chunk, axis=0)


def scatter_rows(partials):
    widths = [part.shape[1] for part in partials]
    joined = lax.psum_scatter(
        jnp.concatenate(partials, axis=1).astype(jnp.bfloat16),
        "tp",
        scatter_dimension=0,
        tiled=True,
    )
    return split_columns(joined.astype(jnp.float32), widths)


def gather_rows(rows_here):
    widths = [part.shape[1] for part in rows_here]
    joined = lax.all_gather(jnp.concatenate(rows_here, axis=1), "tp", axis=0, tiled=True)
    return split_columns(joined, widths)


def split_columns(joined, widths):
    parts, offset = [], 0
    for width in widths:
        parts.append(joined[:, offset : offset + width])
        offset += width
    return tuple(parts)


def layer_body(
    layer_input,
    output_gradient,
    picture_piece_starts,
    sequence_adapter_index,
    attention_norm_gain,
    attention_norm_bias,
    feedforward_norm_gain,
    feedforward_norm_bias,
    query_key_value_weight,
    attention_output_weight,
    up_projection_weight,
    down_projection_weight,
    adapter_projection_first,
    adapter_projection_second,
    adapter_heads_first,
    adapter_heads_second,
    adapter_up_first,
    adapter_up_second,
    adapter_down_first,
    adapter_down_second,
):
    seq_here, local_len, model_width = layer_input.shape
    tok_rows = seq_here * local_len
    tp_count = lax.axis_size("tp")
    adapter_tables = adapter_projection_first.shape[0]
    rank_width = adapter_projection_first.shape[2]
    head_width = HD
    device_heads = adapter_projection_second.shape[-1] // head_width
    local_width = device_heads * head_width
    columns = jnp.arange(adapter_tables * rank_width, dtype=jnp.int32) // rank_width
    chosen = (sequence_adapter_index[:, None] == columns[None, :]).astype(jnp.float32)
    select = jnp.broadcast_to(
        chosen[:, None, :], (seq_here, local_len, adapter_tables * rank_width)
    ).reshape(tok_rows, adapter_tables * rank_width)
    select_here = tp_rows(select, tp_count)
    head_ids = lax.axis_index("tp") * device_heads + jnp.arange(device_heads, dtype=jnp.int32)
    slopes = jnp.exp2(
        -8.0 * (head_ids.astype(jnp.float32) + 1.0) / (device_heads * tp_count)
    )
    here_pos = lax.axis_index("ctx") * local_len + jnp.arange(local_len, dtype=jnp.int32)
    here_labels = piece_labels(picture_piece_starts, here_pos)
    heads_first_local = flattened_first(adapter_heads_first)
    heads_pair = lax.all_gather(
        jnp.concatenate([attention_output_weight, heads_first_local], axis=1),
        "tp",
        axis=0,
        tiled=True,
    )
    out_cols = attention_output_weight.shape[1]
    heads_full = pair_gather(heads_pair[:, :out_cols], "shard", 1)
    heads_first_all_flattened = heads_pair[:, out_cols:]
    projection_first_flattened = flattened_first(adapter_projection_first)
    projection_second_flattened = flattened_second(adapter_projection_second)
    heads_first_flattened = flattened_first(adapter_heads_first)
    heads_second_flattened = flattened_second(adapter_heads_second)
    up_first_flattened = flattened_first(adapter_up_first)
    up_second_flattened = flattened_second(adapter_up_second)
    down_first_flattened = flattened_first(adapter_down_first)
    down_second_flattened = flattened_second(adapter_down_second)
    residual = layer_input.reshape(tok_rows, model_width).astype(jnp.float32)
    residual_here = tp_rows(residual, tp_count)
    first_norm = layer_norm(residual, attention_norm_gain, attention_norm_bias)
    first_act = first_norm.astype(jnp.bfloat16)
    _, first_back_full = jax.vjp(
        lambda inputs: layer_norm(inputs, attention_norm_gain, attention_norm_bias), residual_here
    )
    gathered_rows = (
        pair_gather(query_key_value_weight, "shard", 0),
        pair_gather(up_projection_weight, "shard", 0),
    )
    qkv_full = gathered_rows[0].reshape(model_width, 3 * local_width)
    up_full = gathered_rows[1]
    down_full = pair_gather(down_projection_weight, "shard", 1)
    first_low = (matmul(first_act, projection_first_flattened) * select).astype(jnp.bfloat16)
    projected = (
        matmul(first_act, qkv_full) + matmul(first_low, projection_second_flattened)
    ).astype(jnp.bfloat16)
    queries_flat = projected[:, :local_width].reshape(seq_here, local_len, local_width)
    queries = queries_flat.reshape(seq_here, local_len, device_heads, head_width)
    key_rows = projected[:, local_width : 2 * local_width].reshape(seq_here, local_len, local_width)
    value_rows = projected[:, 2 * local_width :].reshape(seq_here, local_len, local_width)
    ctx_count = lax.axis_size("ctx")
    ctx_here = lax.axis_index("ctx")
    blocks = partner_swaps(
        jnp.concatenate([key_rows, value_rows], axis=2), "ctx", ctx_count
    )
    pieces = jnp.concatenate(blocks, axis=1)
    piece_len = pieces.shape[1]
    key_pos = jnp.concatenate(
        [
            (ctx_here ^ offset) * local_len + jnp.arange(local_len, dtype=jnp.int32)
            for offset in range(ctx_count)
        ]
    )
    key_labels = piece_labels(picture_piece_starts, key_pos)
    visible_mask = visible(here_pos, key_pos, here_labels, key_labels)
    piece_keys = pieces[:, :, :local_width].reshape(seq_here, piece_len, device_heads, head_width)
    piece_values = pieces[:, :, local_width:].reshape(
        seq_here, piece_len, device_heads, head_width
    )
    weighted, totals = None, None
    for offset in range(ctx_count):
        keys_slice = slice(offset * local_len, (offset + 1) * local_len)
        block_keys = blocks[offset][:, :, :local_width].reshape(
            seq_here, local_len, device_heads, head_width
        )
        block_values = blocks[offset][:, :, local_width:].reshape(
            seq_here, local_len, device_heads, head_width
        )
        block_exponent = exponents(
            queries,
            block_keys,
            here_pos,
            key_pos[keys_slice],
            visible_mask[:, :, keys_slice],
            slopes,
        )
        block_weighted = jnp.einsum(
            "shqk,skhd->sqhd",
            block_exponent.astype(jnp.bfloat16),
            block_values,
            preferred_element_type=jnp.float32,
        )
        block_totals = jnp.sum(block_exponent, axis=-1)
        weighted = block_weighted if weighted is None else weighted + block_weighted
        totals = block_totals if totals is None else totals + block_totals
    per_total = jnp.transpose(totals, (0, 2, 1))[..., None]
    heads_raw = weighted / per_total
    heads_act = heads_raw.reshape(tok_rows, local_width).astype(jnp.bfloat16)
    heads_act_here = lax.all_to_all(heads_act, "tp", 0, 1, tiled=True)
    attn_here = matmul(heads_act_here, heads_full)
    heads_low_here = (matmul(heads_act_here, heads_first_all_flattened) * select_here).astype(
        jnp.bfloat16
    )
    middle_here = residual_here + attn_here + matmul(heads_low_here, heads_second_flattened)
    second_norm, second_back = jax.vjp(
        lambda inputs: layer_norm(inputs, feedforward_norm_gain, feedforward_norm_bias), middle_here
    )
    second_act_here = second_norm.astype(jnp.bfloat16)
    (second_act,) = gather_rows((second_act_here,))
    up_low = (matmul(second_act, up_first_flattened) * select).astype(jnp.bfloat16)
    hidden = matmul(second_act, up_full) + matmul(up_low, up_second_flattened)
    activated, gelu_back = jax.vjp(gelu_tanh, hidden)
    activated = activated.astype(jnp.bfloat16)
    down_part = matmul(activated, down_full)
    down_low_part = matmul(activated, down_first_flattened)
    ffn_here, ffn_low_here = scatter_rows((down_part, down_low_part))
    down_low_here = (ffn_low_here * select_here).astype(jnp.bfloat16)
    result_here = (middle_here + ffn_here + matmul(down_low_here, down_second_flattened)).astype(
        jnp.bfloat16
    )
    (result_rows,) = gather_rows((result_here,))
    layer_out = result_rows.reshape(layer_input.shape)
    grad_top_low = output_gradient.reshape(tok_rows, model_width)
    grad_top_here = tp_rows(grad_top_low, tp_count).astype(jnp.float32)
    down_back = (matmul_nt(grad_top_low, down_second_flattened) * select).astype(jnp.bfloat16)
    grad_down_in = matmul_tn(activated, down_back)
    grad_activated = matmul_nt(grad_top_low, down_full) + matmul_nt(down_back, down_first_flattened)
    grad_hidden = gelu_back(grad_activated)[0].astype(jnp.bfloat16)
    up_second_gradient = matmul_tn(up_low, grad_hidden)
    ffn_back_part = matmul_nt(grad_hidden, up_full)
    ffn_back_low = matmul_nt(grad_hidden, up_second_flattened)
    back_here, back_low_here = scatter_rows((ffn_back_part, ffn_back_low))
    up_back_here = (back_low_here * select_here).astype(jnp.bfloat16)
    grad_second = back_here + matmul_nt(up_back_here, up_first_flattened)
    grad_middle_here = grad_top_here + second_back(grad_second)[0]
    grad_middle_low_here = grad_middle_here.astype(jnp.bfloat16)
    heads_back_here = (matmul_nt(grad_middle_low_here, heads_second_flattened) * select_here).astype(
        jnp.bfloat16
    )
    low_rows = partner_gather_rows(
        jnp.concatenate([down_low_here, up_back_here, heads_back_here], axis=1), "tp"
    )
    down_low, up_back, heads_back = split_columns(low_rows, [rank_width * adapter_tables] * 3)
    down_second_gradient = matmul_tn(down_low, grad_top_low)
    grad_up_in = matmul_tn(second_act, up_back)
    grad_heads_in = matmul_tn(heads_act, heads_back)
    heads_second_gradient = matmul_tn(heads_low_here, grad_middle_low_here)
    early_terms = narrow_psum(
        (
            unflat_in(grad_heads_in, adapter_tables),
            unflat_in(grad_up_in, adapter_tables),
            up_second_gradient.reshape(adapter_up_second.shape),
            unflat_in(grad_down_in, adapter_tables),
            down_second_gradient.reshape(adapter_down_second.shape),
        ),
        ("shard", "ctx"),
    )
    heads_second_total = narrow_psum(
        heads_second_gradient.reshape(adapter_heads_second.shape), ("shard", "ctx", "tp")
    )
    grad_heads_here = (
        matmul_nt(grad_middle_low_here, heads_full)
        + matmul_nt(heads_back_here, heads_first_all_flattened)
    ).astype(jnp.bfloat16)
    grad_heads = lax.all_to_all(grad_heads_here, "tp", 1, 0, tiled=True)
    grad_heads_wide = grad_heads.reshape(seq_here, local_len, device_heads, head_width).astype(
        jnp.float32
    )
    scaled_grad = (grad_heads_wide / per_total).astype(jnp.bfloat16)
    row_delta = jnp.sum(grad_heads_wide * heads_raw, axis=-1) / per_total[..., 0]
    grad_queries = None
    grad_kv_here = None
    for offset in list(range(ctx_count - 1, 0, -1)) + [0]:
        keys_slice = slice(offset * local_len, (offset + 1) * local_len)
        query_part, key_part, value_part = block_grads(
            queries,
            scaled_grad,
            row_delta,
            piece_keys[:, keys_slice],
            piece_values[:, keys_slice],
            here_pos,
            key_pos[keys_slice],
            visible_mask[:, :, keys_slice],
            slopes,
        )
        grad_queries = query_part if grad_queries is None else grad_queries + query_part
        block_kv = jnp.concatenate(
            [
                key_part.reshape(seq_here, local_len, local_width),
                value_part.reshape(seq_here, local_len, local_width),
            ],
            axis=2,
        )
        if offset:
            pairs = [(index, index ^ offset) for index in range(ctx_count)]
            block_kv = lax.ppermute(block_kv.astype(jnp.bfloat16), "ctx", pairs).astype(
                jnp.float32
            )
        grad_kv_here = block_kv if grad_kv_here is None else grad_kv_here + block_kv
    grad_keys_all = grad_kv_here[:, :, :local_width]
    grad_values_all = grad_kv_here[:, :, local_width:]
    grad_projected = jnp.concatenate(
        [
            grad_queries.reshape(tok_rows, local_width),
            grad_keys_all.reshape(tok_rows, local_width),
            grad_values_all.reshape(tok_rows, local_width),
        ],
        axis=1,
    ).astype(jnp.bfloat16)
    projection_second_gradient = matmul_tn(first_low, grad_projected)
    attn_back_part = matmul_nt(grad_projected, qkv_full)
    attn_back_low = matmul_nt(grad_projected, projection_second_flattened)
    low_blocks = jnp.stack(partner_swaps(attn_back_low.astype(jnp.bfloat16), "tp", tp_count))
    low_owners = jnp.bitwise_xor(lax.axis_index("tp"), jnp.arange(tp_count, dtype=jnp.int32))
    low_total = jnp.sum(jnp.take(low_blocks, low_owners, axis=0).astype(jnp.float32), axis=0)
    select_late = lax.optimization_barrier(select)
    qkv_back = (low_total * select_late).astype(jnp.bfloat16)
    grad_qkv_in = matmul_tn(first_act, qkv_back)
    late_terms = butterfly_sum(
        (
            unflat_in(grad_qkv_in, adapter_tables),
            projection_second_gradient.reshape(adapter_projection_second.shape),
        ),
        ("shard", "ctx"),
    )
    first_here, first_low_here = scatter_rows((attn_back_part, attn_back_low))
    select_later = lax.optimization_barrier(select_here)
    qkv_back_here = (first_low_here * select_later).astype(jnp.bfloat16)
    grad_first = first_here + matmul_nt(qkv_back_here, projection_first_flattened)
    input_here = (grad_middle_here + first_back_full(grad_first)[0]).astype(jnp.bfloat16)
    (input_rows,) = gather_rows((input_here,))
    input_grad = input_rows.reshape(layer_input.shape)
    return (
        layer_out,
        input_grad,
        late_terms[0],
        late_terms[1],
        early_terms[0],
        heads_second_total,
        early_terms[1],
        early_terms[2],
        early_terms[3],
        early_terms[4],
    )


def solution(mesh):
    placed = (
        P("shard", "ctx", None),
        P("shard", "ctx", None),
        P("shard", None),
        P("shard"),
        P(),
        P(),
        P(),
        P(),
        P("shard", None, "tp"),
        P("tp", "shard"),
        P("shard", "tp"),
        P("tp", "shard"),
        P(),
        P(None, None, None, "tp"),
        P(None, "tp", None),
        P(),
        P(),
        P(None, None, "tp"),
        P(None, "tp", None),
        P(),
    )
    return jax.shard_map(
        layer_body,
        mesh=mesh,
        in_specs=placed,
        out_specs=(
            P("shard", "ctx", None),
            P("shard", "ctx", None),
            P(),
            P(None, None, None, "tp"),
            P(None, "tp", None),
            P(),
            P(),
            P(None, None, "tp"),
            P(None, "tp", None),
            P(),
        ),
        check_vma=False,
    )
```
